32 devices in a mesh: groups: 2 (over x), seq: 16 (over z, y, core).
Axes of the slice: x: 2, y: 2, z: 4, core: 2. Of those that a mesh axis runs over, the one named last changes fastest.
Arguments:
- attn_query: bfloat16 [8192, 2048], P(('groups', 'seq')), parts along dimension 0, may hold values from -16 to 16
- attn_key: bfloat16 [8192, 2048], P(('groups', 'seq')), parts along dimension 0, may hold values from -16 to 16
- attn_value: bfloat16 [8192, 2048], P(('groups', 'seq')), parts along dimension 0, may hold values from -6 to 6
- mesa_query: bfloat16 [8192, 2048], P(('groups', 'seq')), parts along dimension 0, may hold values from -6 to 6
- mesa_key: bfloat16 [8192, 2048], P(('groups', 'seq')), parts along dimension 0, may hold values from -16 to 16
- log_decay: float32 [8192, 16], P(('groups', 'seq')), parts along dimension 0, may hold values from -1 to 0
- input_gate: float32 [8192, 16], P(('groups', 'seq')), parts along dimension 0, may hold values from 0.2 to 1
- regularizer: float32 [16, 128], replicated, may hold values from 0.5 to 4
Outputs:
- attention: bfloat16 [8192, 2048], P(('groups', 'seq')), parts along dimension 0
- mesa_out: bfloat16 [8192, 2048], P(('groups', 'seq')), parts along dimension 0
The draws below stay inside these ranges and needn't reach their ends.
There are 2 independent parts, one for each index of `groups`. The reference program is written for one: setup_inputs(seed, part) draws one part's arguments, and reference() takes and returns one part's arrays. A program takes and returns all parts, laid end to end along the dimension named above; an argument that names none is the same for every part. Nothing has to cross between parts.
All inputs are finite; a program needn't handle non-finite values.
Results may differ from the reference program's by a relative error of at most 0.017.
Values may be sent and summed in bfloat16 or wider, within the bound.
A program may use at most 128 MiB of HBM per device.

```python
import math
import jax
import jax.numpy as jnp
from jax import lax

HEAD_GROUP = 16
DK = 128
FEATURES = 2048
WINDOW = 2048
SPAN = 64
CG_ITERS = 8
TOK_DEV = 256
TOKEN_LENGTH = 4096


def drawn_pair(key):
    random_seeds = jax.random.split(jax.random.fold_in(key, 11), 2)
    base_query = jnp.clip(jax.random.normal(random_seeds[0], (TOKEN_LENGTH, FEATURES), jnp.float32), -4.0, 4.0)
    base_key = jnp.clip(jax.random.normal(random_seeds[1], (TOKEN_LENGTH, FEATURES), jnp.float32), -4.0, 4.0)
    return (base_query, base_key)


def draw_attn_query(key, part):
    return drawn_pair(key)[0].astype(jnp.bfloat16)


def draw_attn_key(key, part):
    return drawn_pair(key)[1].astype(jnp.bfloat16)


def draw_mesa_key(key, part):
    random_seeds = jax.random.split(jax.random.fold_in(key, 29), 3)
    overall = math.sqrt(32.0 / TOKEN_LENGTH)
    entries = jnp.clip(jax.random.normal(random_seeds[0], (TOKEN_LENGTH, FEATURES), jnp.float32), -4.0, 4.0)
    column = jnp.exp(jax.random.uniform(random_seeds[1], (1, FEATURES), jnp.float32, math.log(0.3), math.log(1.5)))
    coarse_result = jax.random.uniform(random_seeds[2], (TOKEN_LENGTH, 1), jnp.float32, 0.5, 1.5)
    return (entries * column * coarse_result * overall).astype(jnp.bfloat16)


def draw_log_decay(key, part):
    random_seeds = jax.random.split(jax.random.fold_in(key, 37), 7)
    share = 0.5
    slow = jax.random.uniform(random_seeds[0], (HEAD_GROUP,), jnp.float32) < share
    slow_rate = jax.random.uniform(random_seeds[1], (HEAD_GROUP,), jnp.float32, 0.1, 0.25) * math.log(10.0) / TOKEN_LENGTH
    fast_rate = math.log(10.0) / jax.random.uniform(random_seeds[2], (HEAD_GROUP,), jnp.float32, 30.0, 50.0)
    head_decay_rate = jnp.where(slow, slow_rate, fast_rate)
    slab_factor = jnp.exp(jax.random.uniform(random_seeds[3], (TOKEN_LENGTH // TOK_DEV, HEAD_GROUP), jnp.float32, math.log(0.5), math.log(2.0)))
    piece_rows = jnp.repeat(slab_factor, TOK_DEV, axis=0)
    coarse_result = jax.random.uniform(random_seeds[4], (TOKEN_LENGTH, HEAD_GROUP), jnp.float32, 0.5, 1.5)
    segment_list = jax.random.randint(random_seeds[5], (2,), 0, TOKEN_LENGTH)
    segment_rows = jnp.any(jnp.arange(TOKEN_LENGTH)[:, None] == segment_list[None, :], axis=1)[:, None]
    segment_loss = jnp.log(jax.random.uniform(random_seeds[6], (1, HEAD_GROUP), jnp.float32, 0.5, 0.8))
    return -(head_decay_rate[None, :] * piece_rows * coarse_result) + jnp.where(segment_rows, segment_loss, 0.0)


def block_scale(rng, shape, cuts, smallest, largest):
    loudness, own = 1.0, jax.random.fold_in(rng, 6)
    for position, shards_of in cuts:
        draws = jnp.exp(jax.random.uniform(jax.random.fold_in(own, position), (shards_of,), jnp.float32, smallest / len(cuts), largest / len(cuts)))
        loudness = loudness * jnp.repeat(draws, shape[position] // shards_of).reshape([-1 if axis == position else 1 for axis in range(len(shape))])
    return loudness


def scatter_about(rng, extent, deviation, bound, cuts=(), kind=jnp.bfloat16):
    level = block_scale(rng, extent, cuts, -0.22, 0.18) if cuts else 1.0
    values = jax.random.normal(rng, extent, jnp.float32) * deviation * level
    return jnp.minimum(jnp.maximum(values, -bound), bound).astype(kind)


def setup_inputs(seed: int = 0, part: int = 0) -> dict:
    arg_keys = jax.random.split(jax.random.key(seed), 9)
    part_splits = jax.random.split(jax.random.fold_in(arg_keys[8], part), 9)
    attn_query = draw_attn_query(jax.random.fold_in(jax.random.fold_in(arg_keys[8], part), 71), part)
    attn_key = draw_attn_key(jax.random.fold_in(jax.random.fold_in(arg_keys[8], part), 71), part)
    attn_value = scatter_about(part_splits[2], (TOKEN_LENGTH, FEATURES), 1.0, 6.0, ((0, 16),))
    mesa_query = scatter_about(part_splits[3], (TOKEN_LENGTH, FEATURES), 1.0, 6.0, ((0, 16),))
    mesa_key = draw_mesa_key(jax.random.fold_in(jax.random.fold_in(arg_keys[8], part), 71), part)
    log_decay = draw_log_decay(jax.random.fold_in(jax.random.fold_in(arg_keys[8], part), 71), part)
    input_gate = jnp.clip(0.2 + 0.8 * jax.random.uniform(part_splits[6], (TOKEN_LENGTH, HEAD_GROUP), jnp.float32) ** block_scale(part_splits[6], (TOKEN_LENGTH, HEAD_GROUP), ((0, 16),), -0.2, 0.2), 0.2, 1.0)
    regularizer = jnp.clip(jnp.exp(jax.random.uniform(arg_keys[7], (HEAD_GROUP, DK), jnp.float32, math.log(0.5), math.log(4.0))), 0.5, 4.0)
    return {"attn_query": attn_query, "attn_key": attn_key, "attn_value": attn_value, "mesa_query": mesa_query, "mesa_key": mesa_key, "log_decay": log_decay, "input_gate": input_gate, "regularizer": regularizer}


exact_mode = lax.Precision.HIGHEST
masked_score = -1e30


def span_update(states, inputs, ridge_diag):
    gram_start, cross_start = states
    queries, key_rows, value_rows, log_rates, gate_rows = inputs
    q_heads = jnp.transpose(queries, (1, 0, 2))
    k_heads = jnp.transpose(key_rows, (1, 0, 2))
    v_heads = jnp.transpose(value_rows, (1, 0, 2))
    cumulative = jnp.transpose(jnp.cumsum(log_rates, axis=0))
    length = cumulative.shape[1]
    causal = (jnp.arange(length)[:, None] >= jnp.arange(length)[None, :])[None]
    distance = cumulative[:, :, None] - cumulative[:, None, :]
    decay_mix = jnp.where(causal, jnp.exp(jnp.where(causal, distance, 0.0)), 0.0) * jnp.transpose(gate_rows)[:, None, :]
    start_scale = jnp.exp(cumulative)[:, :, None]

    def operator_apply(search):
        carried = start_scale * jnp.einsum('hcd,hed->hce', search, gram_start, precision=exact_mode)
        products = jnp.einsum('hjd,hid->hji', search, k_heads, precision=exact_mode)
        local_part = jnp.einsum('hji,hid->hjd', decay_mix * products, k_heads, precision=exact_mode)
        return carried + local_part + ridge_diag[:, None, :] * search

    iterate = jnp.zeros_like(q_heads)
    remain = q_heads
    search = q_heads
    norm_now = jnp.sum(remain * remain, axis=-1, keepdims=True)
    for sweep_index in range(CG_ITERS):
        image_vec = operator_apply(search)
        step_size = norm_now / (jnp.sum(search * image_vec, axis=-1, keepdims=True) + 1e-6)
        iterate = iterate + step_size * search
        remain = remain - step_size * image_vec
        norm_next = jnp.sum(remain * remain, axis=-1, keepdims=True)
        search = remain + (norm_next / (norm_now + 1e-6)) * search
        norm_now = norm_next
    products = jnp.einsum('hjd,hid->hji', iterate, k_heads, precision=exact_mode)
    mesa_rows = start_scale * jnp.einsum('hje,hde->hjd', iterate, cross_start, precision=exact_mode)
    mesa_rows = mesa_rows + jnp.einsum('hji,hid->hjd', decay_mix * products, v_heads, precision=exact_mode)
    tail_weight = (jnp.exp(cumulative[:, -1:] - cumulative) * jnp.transpose(gate_rows))[:, :, None]
    end_scale = jnp.exp(cumulative[:, -1])[:, None, None]
    gram_end = end_scale * gram_start + jnp.einsum('hid,hie->hde', k_heads * tail_weight, k_heads, precision=exact_mode)
    cross_end = end_scale * cross_start + jnp.einsum('hid,hie->hde', v_heads * tail_weight, k_heads, precision=exact_mode)
    return (gram_end, cross_end), jnp.transpose(mesa_rows, (1, 0, 2))


def mesa_pass(queries, key_rows, value_rows, log_rates, gate_rows, ridge_diag, gram_start, cross_start):
    row_total = queries.shape[0]
    span_count = row_total // SPAN

    def shaped(array_in):
        return array_in.reshape((span_count, SPAN) + array_in.shape[1:])

    def advance(states, inputs):
        return span_update(states, inputs, ridge_diag)

    finished, outputs = lax.scan(advance, (gram_start, cross_start),
                                 (shaped(queries), shaped(key_rows), shaped(value_rows), shaped(log_rates), shaped(gate_rows)))
    return outputs.reshape(row_total, -1)


def reference(attn_query, attn_key, attn_value, mesa_query, mesa_key, log_decay, input_gate, regularizer):
    head_count, head_size = regularizer.shape
    total_rows = attn_query.shape[0]
    block_rows = TOK_DEV
    block_count = total_rows // block_rows
    queries = attn_query.reshape(block_count, block_rows, head_count, head_size)
    padded_keys = jnp.pad(attn_key, ((WINDOW, 0), (0, 0)))
    padded_values = jnp.pad(attn_value, ((WINDOW, 0), (0, 0)))
    scale_factor = head_size ** -0.5

    def attend(inputs):
        block_index, block_queries = inputs
        first_row = (block_index * block_rows).astype(jnp.int32)
        key_rows = lax.dynamic_slice_in_dim(padded_keys, first_row, WINDOW + block_rows, 0).reshape(-1, head_count, head_size)
        value_rows = lax.dynamic_slice_in_dim(padded_values, first_row, WINDOW + block_rows, 0).reshape(-1, head_count, head_size)
        scores = jnp.einsum('qhd,khd->hqk', block_queries.astype(jnp.float32), key_rows.astype(jnp.float32)) * scale_factor
        query_pos = first_row + jnp.arange(block_rows, dtype=jnp.int32)[:, None]
        key_pos = first_row - WINDOW + jnp.arange(WINDOW + block_rows, dtype=jnp.int32)[None, :]
        distance = query_pos - key_pos
        inside = ((distance >= 0) & (distance < WINDOW) & (key_pos >= 0))[None]
        scores = jnp.where(inside, scores, masked_score)
        row_max = jnp.max(scores, axis=-1, keepdims=True)
        weights = jnp.exp(scores - row_max) * inside.astype(jnp.float32)
        rounded = weights.astype(jnp.bfloat16)
        summed = jnp.einsum('hqk,khd->hqd', rounded.astype(jnp.float32), value_rows.astype(jnp.float32))
        normed = summed / jnp.sum(weights, axis=-1, keepdims=True)
        return jnp.transpose(normed, (1, 0, 2)).reshape(block_rows, -1).astype(jnp.bfloat16)

    attention = lax.map(attend, (jnp.arange(block_count, dtype=jnp.int32), queries)).reshape(total_rows, -1)
    shape3 = (total_rows, head_count, head_size)
    gram_zero = jnp.zeros((head_count, head_size, head_size), jnp.float32)
    mesa_out = mesa_pass(mesa_query.astype(jnp.float32).reshape(shape3), mesa_key.astype(jnp.float32).reshape(shape3),
                         attention.astype(jnp.float32).reshape(shape3), log_decay, input_gate, regularizer,
                         gram_zero, gram_zero)
    return attention, mesa_out.astype(jnp.bfloat16)
```

```python
import jax
import jax.numpy as jnp
from jax import lax
from jax.experimental import pallas as pl
from jax.experimental.pallas import tpu as pltpu
from jax.sharding import PartitionSpec as P
import functools
import math

WINDOW = 2048
SPAN = 64
CG_ITERS = 8


exact_mode = lax.Precision.HIGHEST
masked_score = -1e30


def prefix(shard, axis, join, neutral):
    place = lax.axis_index(axis)
    gathered = jax.tree.map(
        lambda a, kind: lax.all_gather(a.astype(kind), axis), shard, (jnp.bfloat16, jnp.bfloat16)
    )
    state = jax.tree.map(lambda a, e: jnp.zeros_like(a) + jnp.asarray(e, a.dtype), shard, neutral)

    def one(lap, state):
        return join(
            state,
            jax.tree.map(
                lambda a, own: lax.dynamic_index_in_dim(a, lap, 0, False).astype(own.dtype),
                gathered,
                shard,
            ),
        )

    return lax.fori_loop(0, place, one, state)


def passed_along(value, axis, steps):
    count = lax.axis_size(axis)
    first, last = (max(0, -steps), min(count, count - steps))
    return lax.ppermute(value, axis, [(source, source + steps) for source in range(first, last)])


def span_update(states, inputs, ridge_diag):
    gram_start, cross_start = states
    queries, key_rows, value_rows, log_rates, gate_rows = inputs
    q_heads = jnp.transpose(queries, (1, 0, 2))
    k_heads = jnp.transpose(key_rows, (1, 0, 2))
    v_heads = jnp.transpose(value_rows, (1, 0, 2))
    cumulative = jnp.transpose(jnp.cumsum(log_rates, axis=0))
    length = cumulative.shape[1]
    causal = (jnp.arange(length)[:, None] >= jnp.arange(length)[None, :])[None]
    distance = cumulative[:, :, None] - cumulative[:, None, :]
    decay_mix = (
        jnp.where(causal, jnp.exp(jnp.where(causal, distance, 0.0)), 0.0)
        * jnp.transpose(gate_rows)[:, None, :]
    )
    start_scale = jnp.exp(cumulative)[:, :, None]
    iterate = jnp.zeros_like(q_heads)
    remain = q_heads
    search = q_heads
    norm_now = jnp.sum(remain * remain, axis=-1, keepdims=True)
    for sweep_index in range(CG_ITERS):
        carried = start_scale * jnp.einsum("hcd,hed->hce", search, gram_start, precision=exact_mode)
        operator_products = jnp.einsum("hjd,hid->hji", search, k_heads, precision=exact_mode)
        local_part = jnp.einsum(
            "hji,hid->hjd", decay_mix * operator_products, k_heads, precision=exact_mode
        )
        image_vec = carried + local_part + ridge_diag[:, None, :] * search
        step_size = norm_now / (jnp.sum(search * image_vec, axis=-1, keepdims=True) + 1e-06)
        iterate = iterate + step_size * search
        remain = remain - step_size * image_vec
        norm_next = jnp.sum(remain * remain, axis=-1, keepdims=True)
        search = remain + norm_next / (norm_now + 1e-06) * search
        norm_now = norm_next
    products = jnp.einsum("hjd,hid->hji", iterate, k_heads, precision=exact_mode)
    mesa_rows = start_scale * jnp.einsum("hje,hde->hjd", iterate, cross_start, precision=exact_mode)
    mesa_rows = mesa_rows + jnp.einsum(
        "hji,hid->hjd", decay_mix * products, v_heads, precision=exact_mode
    )
    tail_weight = (jnp.exp(cumulative[:, -1:] - cumulative) * jnp.transpose(gate_rows))[:, :, None]
    end_scale = jnp.exp(cumulative[:, -1])[:, None, None]
    gram_end = end_scale * gram_start + jnp.einsum(
        "hid,hie->hde", k_heads * tail_weight, k_heads, precision=exact_mode
    )
    cross_end = end_scale * cross_start + jnp.einsum(
        "hid,hie->hde", v_heads * tail_weight, k_heads, precision=exact_mode
    )
    return ((gram_end, cross_end), jnp.transpose(mesa_rows, (1, 0, 2)))


def mesa_pass(
    queries, key_rows, value_rows, log_rates, gate_rows, ridge_diag, gram_start, cross_start
):
    row_total = queries.shape[0]
    span_count = row_total // SPAN

    def shaped(array_in):
        return array_in.reshape((span_count, SPAN) + array_in.shape[1:])

    def advance(states, inputs):
        return span_update(states, inputs, ridge_diag)

    finished, outputs = lax.scan(
        advance,
        (gram_start, cross_start),
        (
            shaped(queries),
            shaped(key_rows),
            shaped(value_rows),
            shaped(log_rates),
            shaped(gate_rows),
        ),
    )
    return outputs.reshape(row_total, -1)


def fold_block(state_now, queries, key_value, query_first, key_first):
    running_max, running_sum, weighted = state_now
    row_count, head_count, head_size = queries.shape
    key_rows = key_value[0].reshape(-1, head_count, head_size)
    value_rows = key_value[1].reshape(-1, head_count, head_size)
    scores = jnp.einsum(
        "qhd,khd->hqk", queries, key_rows, preferred_element_type=jnp.float32
    ) * head_size ** (-0.5)
    query_pos = query_first + jnp.arange(row_count, dtype=jnp.int32)[:, None]
    key_pos = key_first + jnp.arange(key_rows.shape[0], dtype=jnp.int32)[None, :]
    distance = query_pos - key_pos
    inside = ((distance >= 0) & (distance < WINDOW) & (key_pos >= 0))[None]
    scores = jnp.where(inside, scores, masked_score)
    new_max = jnp.maximum(running_max, jnp.max(scores, axis=-1))
    weights = jnp.exp(scores - new_max[:, :, None]) * inside.astype(jnp.float32)
    rescale = jnp.exp(running_max - new_max)
    running_sum = running_sum * rescale + jnp.sum(weights, axis=-1)
    weighted = weighted * rescale[:, :, None] + jnp.einsum(
        "hqk,khd->hqd", weights.astype(jnp.bfloat16), value_rows, preferred_element_type=jnp.float32
    )
    return (new_max, running_sum, weighted)


def combine_pair(earlier, later):
    return (earlier[0] + later[0], jnp.exp(later[0])[:, None, None] * earlier[1] + later[1])


def slab_body(
    attn_query, attn_key, attn_value, mesa_query, mesa_key, log_decay, input_gate, regularizer
):
    row_count = attn_query.shape[0]
    head_count, head_size = regularizer.shape
    shape3 = (row_count, head_count, head_size)
    slab_first = lax.axis_index("seq") * row_count
    keys_float = mesa_key.astype(jnp.float32).reshape(shape3)
    slab_log = jnp.sum(log_decay, axis=0)
    tail_log = slab_log[None, :] - jnp.cumsum(log_decay, axis=0)
    weight_rows = (jnp.exp(tail_log) * input_gate)[:, :, None]
    gram_local = jnp.einsum(
        "lhd,lhe->hde", keys_float * weight_rows, keys_float, precision=exact_mode
    )
    zero_log = jnp.zeros_like(slab_log)
    zero_state = jnp.zeros_like(gram_local)
    gram_prefix = prefix((slab_log, gram_local), "seq", combine_pair, (zero_log, zero_state))[1]
    queries = attn_query.reshape(shape3)
    key_value = jnp.stack([attn_key, attn_value])
    state_now = (
        jnp.full((head_count, row_count), masked_score, jnp.float32),
        jnp.zeros((head_count, row_count), jnp.float32),
        jnp.zeros((head_count, row_count, head_size), jnp.float32),
    )
    state_now = fold_block(state_now, queries, key_value, slab_first, slab_first)
    reach = -(-WINDOW // row_count)
    moving = key_value
    for hop_index in range(1, reach + 1):
        moving = passed_along(moving, "seq", 1)
        state_now = fold_block(
            state_now, queries, moving, slab_first, slab_first - hop_index * row_count
        )
    normed = state_now[2] / state_now[1][:, :, None]
    attention = jnp.transpose(normed, (1, 0, 2)).reshape(row_count, -1).astype(jnp.bfloat16)
    values_float = attention.astype(jnp.float32).reshape(shape3)
    cross_local = jnp.einsum(
        "lhd,lhe->hde", values_float * weight_rows, keys_float, precision=exact_mode
    )
    cross_prefix = prefix((slab_log, cross_local), "seq", combine_pair, (zero_log, zero_state))[1]
    mesa_out = mesa_pass(
        mesa_query.astype(jnp.float32).reshape(shape3),
        keys_float,
        values_float,
        log_decay,
        input_gate,
        regularizer,
        gram_prefix,
        cross_prefix,
    )
    return (attention, mesa_out.astype(jnp.bfloat16))


CHUNK = 128
WAYS = 4
BF16 = jnp.bfloat16
F32 = jnp.float32
NT = (((1,), (1,)), ((), ()))
TN = (((0,), (0,)), ((), ()))


def dot(a, b, dims=None):
    if dims is None:
        return jnp.dot(a, b, preferred_element_type=F32)
    return lax.dot_general(a, b, dims, preferred_element_type=F32)


def two_terms(a):
    high = a.astype(BF16)
    low = (a - high.astype(F32)).astype(BF16)
    return jnp.concatenate([high, low], axis=1)


def score_blocks(queries, k_ref, base, count, rows, masks):
    scores, top = [], None
    for j in range(count):
        s = dot(queries, k_ref[pl.ds(base + j * rows, rows), :], NT)
        if masks[j] is not None:
            s = jnp.where(masks[j], s, masked_score)
        scores.append(s)
        top = s if top is None else jnp.maximum(top, s)
    return scores, jnp.max(top, axis=1, keepdims=True)


def weigh(scores, top, v_ref, base, rows, scale):
    total, weights = None, []
    for s in scores:
        w = jnp.exp2((s - top) * scale)
        total = w if total is None else total + w
        weights.append(w.astype(BF16))
    total = jnp.sum(total, axis=1, keepdims=True)
    summed = dot(
        jnp.concatenate(weights, axis=1), v_ref[pl.ds(base, len(scores) * rows), :]
    )
    return total, summed


def index_gap(rows):
    shape = (rows, rows)
    return lax.broadcasted_iota(jnp.int32, shape, 0) - lax.broadcasted_iota(jnp.int32, shape, 1)


def score_scale(size):
    return math.log2(math.e) / math.sqrt(size)


def block_of(i, rows):
    return pl.ds(pl.multiple_of(i * rows, rows), rows)


def attend_back(q_ref, k_ref, v_ref, o_ref, l_ref, i, low, count, rows):
    size = q_ref.shape[1]
    scale = score_scale(size)
    gap = index_gap(rows)
    masks = [gap + (i - low - j) * rows < 0 if j < 2 else None for j in range(count)]
    queries = q_ref[block_of(i, rows), :]
    scores, top = score_blocks(queries, k_ref, low * rows, count, rows, masks)
    total, summed = weigh(scores, top, v_ref, low * rows, rows, scale)
    o_ref[block_of(i, rows), :] = (summed / total).astype(BF16)
    level = jnp.broadcast_to(top * scale + jnp.log2(total), (rows, size))
    l_ref[i] = jnp.transpose(level)[:8, :]


def attend_own(q_ref, k_ref, v_ref, o_ref, l_ref, out_ref, i, count, rows):
    size = q_ref.shape[1]
    scale = score_scale(size)
    gap = index_gap(rows)
    masks = [gap + (i - j) * rows >= 0 if j >= count - 2 else None for j in range(count)]
    queries = q_ref[block_of(i, rows), :]
    scores, top = score_blocks(queries, k_ref, 0, count, rows, masks)
    total, summed = weigh(scores, top, v_ref, 0, rows, scale)
    earlier = jnp.transpose(jnp.broadcast_to(l_ref[i][:1, :], (size, rows)))
    level = top * scale
    peak = jnp.maximum(earlier, level)
    share_own, share_earlier = jnp.exp2(level - peak), jnp.exp2(earlier - peak)
    joined = summed * share_own + o_ref[block_of(i, rows), :].astype(F32) * share_earlier
    out_ref[block_of(i, rows), :] = (joined / (total * share_own + share_earlier)).astype(BF16)


def flat(c, per):
    return c[0] * per + c[1]


def span(c, per):
    return pl.ds(pl.multiple_of(flat(c, per) * CHUNK, CHUNK), CHUNK)


def chunk_ids(g, per, ways=WAYS):
    slabs = ways // per
    return [(g * slabs + w // per, w % per) for w in range(ways)]


def column_form(row):
    return jnp.transpose(jnp.broadcast_to(row, (CHUNK, CHUNK)))


def rates_of(rates_ref, c):
    slab, place = c
    per = rates_ref.shape[1] // 4
    return rates_ref[slab, place : place + 1, :], rates_ref[slab, per + place : per + place + 1, :]


def tail_keys(k_ref, rates_ref, c, per):
    cum, gate = rates_of(rates_ref, c)
    weight = column_form(jnp.exp(cum[:, CHUNK - 1 :] - cum) * gate)
    keys = k_ref[span(c, per), :]
    return (keys.astype(F32) * weight).astype(BF16), jnp.exp(cum[:, CHUNK - 1 :])


def mix_of(rates_ref, c):
    cum, gate = rates_of(rates_ref, c)
    col = column_form(cum)
    shape = (CHUNK, CHUNK)
    causal = lax.broadcasted_iota(jnp.int32, shape, 0) >= lax.broadcasted_iota(
        jnp.int32, shape, 1
    )
    mix = jnp.exp(jnp.where(causal, col - cum, masked_score)) * gate
    return mix, jnp.exp(col)


def gram_states(k_ref, other_ref, rates_ref, first_ref, starts_ref, last_ref):
    per = rates_ref.shape[1] // 4
    chunks = rates_ref.shape[0] * per

    def step(g, state):
        for c in chunk_ids(g, per):
            starts_ref[flat(c, per)] = state.astype(BF16)
            keys, end = tail_keys(k_ref, rates_ref, c, per)
            state = end * state + dot(keys, other_ref[span(c, per), :], TN)
        return state

    last = lax.fori_loop(0, chunks // WAYS, step, first_ref[...].astype(F32))
    last_ref[...] = last.astype(BF16)


def solve_all(q_ref, k_ref, rates_ref, ridge_ref, gram_ref, x_ref):
    ridge = ridge_ref
    per = rates_ref.shape[1] // 4
    chunks = rates_ref.shape[0] * per

    def group(g, carry):
        ids = chunk_ids(g, per)
        mixes = [mix_of(rates_ref, c) for c in ids]
        keys = [k_ref[span(c, per), :] for c in ids]
        grams = [gram_ref[flat(c, per)] for c in ids]
        sides = [
            jnp.concatenate(
                [jnp.concatenate([a, a], axis=1), jnp.concatenate([k, k], axis=1)], axis=0
            )
            for a, k in zip(grams, keys)
        ]
        stacks = [jnp.concatenate([k, k], axis=0) for k in keys]
        state = []
        for c in ids:
            q = q_ref[span(c, per), :].astype(F32)
            state.append((jnp.zeros_like(q), q, q, jnp.sum(q * q, axis=1, keepdims=True)))

        def sweep(n, state):
            both = [dot(two_terms(s[2]), side, NT) for s, side in zip(state, sides)]
            local = [
                dot(two_terms(m[0] * b[:, CHUNK:]), k) for m, b, k in zip(mixes, both, stacks)
            ]
            out = []
            for (x, r, p, rr), b, l, m in zip(state, both, local, mixes):
                a = m[1] * b[:, :CHUNK] + l + ridge * p
                alpha = rr / (jnp.sum(p * a, axis=1, keepdims=True) + 1e-6)
                x = x + alpha * p
                r = r - alpha * a
                new = jnp.sum(r * r, axis=1, keepdims=True)
                p = r + (new / (rr + 1e-6)) * p
                out.append((x, r, p, new))
            return tuple(out)

        state = lax.fori_loop(0, CG_ITERS, sweep, tuple(state))
        for c, s in zip(ids, state):
            x_ref[span(c, per), :] = s[0]
        return carry

    lax.fori_loop(0, chunks // WAYS, group, 0)


def read_out(k_ref, v_ref, rates_ref, cross_ref, x_ref, out_ref, slab):
    per = rates_ref.shape[1] // 4
    for c in chunk_ids(slab, per, per):
        mix, start = mix_of(rates_ref, c)
        keys, values, cross = k_ref[span(c, per), :], v_ref[span(c, per), :], cross_ref[flat(c, per)]
        x = two_terms(x_ref[span(c, per), :])
        products = dot(x, jnp.concatenate([keys, keys], axis=1), NT)
        rows = start * dot(x, jnp.concatenate([cross, cross], axis=0))
        rows = rows + dot(two_terms(mix * products), jnp.concatenate([values, values], axis=0))
        out_ref[span(c, per), :] = rows.astype(BF16)


KINDS = 13
Q, K, V, MK, MQ, RATES, ATT, OUT, QX, PART, LEVEL, GRAM, CROSS = range(KINDS)


def group_kernel(n, g, *refs):
    ins, rates_in, ridge_in = refs[:5], refs[5], refs[6]
    results = refs[7:9]
    bufs, qx, rates, homes = refs[9:14], refs[14], refs[15], refs[16:18]
    o_out, o_in, l_out, l_in = refs[18:22]
    g_first, g_last, c_first, c_last = refs[22:26]
    gram, cross, x = refs[26:29]
    send, recv, own = refs[29:32]
    q, k, v, mk, mq = bufs
    att, out = homes
    rows, size = ins[0].shape[0], ridge_in.shape[1]
    per_device = rates.shape[0]
    wide = per_device * size
    groups = n // g
    group, me = lax.axis_index("groups"), lax.axis_index("seq")
    sup, place = me // g, lax.rem(me, g)

    def row_block(ref, s):
        return ref.at[pl.ds(pl.multiple_of(s * rows, rows), rows), :]

    def head_col(ref, j):
        return ref.at[:, pl.ds(pl.multiple_of(j * size, size), size)]

    def cell(ref, s, j):
        return ref.at[
            pl.ds(pl.multiple_of(s * rows, rows), rows),
            pl.ds(pl.multiple_of(j * size, size), size),
        ]

    def ends(a, j, source, target):
        if a in (MK, MQ):
            src = ins[a].at[:, pl.ds(pl.multiple_of(target * wide, wide), wide)]
            return src, row_block(bufs[a], source)
        if a in (Q, K, V):
            return head_col(ins[a], target * per_device + j), cell(bufs[a], source, j)
        if a == QX:
            return head_col(ins[Q], target * per_device + j), cell(qx, source, j)
        if a == RATES:
            return rates_in.at[pl.ds(target * per_device, per_device)], rates.at[:, source]
        return cell(homes[a - ATT], target, j), head_col(results[a - ATT], source * per_device + j)

    def copy_to(src, dst, a, j, sent, got, peer):
        return pltpu.make_async_remote_copy(
            src_ref=src,
            dst_ref=dst,
            send_sem=send.at[a, j, sent],
            recv_sem=recv.at[a, j, got],
            device_id=(group, peer),
            device_id_type=pl.DeviceIdType.MESH,
        )

    def remote(a, j, source, target, peer):
        src, dst = ends(a, j, source, target)
        return copy_to(src, dst, a, j, target, source, peer)

    def local(a, j):
        src, dst = ends(a, j, place, place)
        return pltpu.make_async_copy(src, dst, own.at[a, j])

    def onward(a, j, i):
        if a == PART:
            src, dst = cell(o_out, i, j), cell(o_in, i, j)
        elif a == LEVEL:
            src, dst = l_out.at[j, i], l_in.at[j, i]
        elif a == GRAM:
            src, dst = g_last.at[j], g_first.at[j]
        else:
            src, dst = c_last.at[j], c_first.at[j]
        return copy_to(src, dst, a, j, i, i, me + g)

    has_next, has_previous = sup + 1 < groups, sup > 0

    def loop(first, last, act):
        def one(t, carry):
            act(t)
            return carry

        lax.fori_loop(first, last, one, 0)

    def others(act):
        loop(1, g, lambda t: act(lax.rem(place + t, g)))

    def signal(peer):
        pl.semaphore_signal(
            barrier, inc=1, device_id=(group, peer), device_id_type=pl.DeviceIdType.MESH
        )

    def home(e):
        return sup * g + e

    def push(a, j):
        others(lambda e: remote(a, j, place, e, home(e)).start())
        local(a, j).start()

    def arrive(a, j):
        others(lambda e: remote(a, j, e, place, home(e)).wait_recv())
        local(a, j).wait()

    def give(a, j, e):
        @pl.when(e != place)
        def _():
            remote(a, j, place, e, home(e)).start()

        @pl.when(e == place)
        def _():
            local(a, j).start()

    barrier = pltpu.get_barrier_semaphore()
    others(lambda e: signal(home(e)))

    @pl.when(has_previous)
    def _():
        loop(0, g, lambda e: signal(home(e) - g))

    @pl.when(has_next)
    def _():
        loop(0, g, lambda e: signal(home(e) + g))

    near = has_previous.astype(jnp.int32) + has_next.astype(jnp.int32)
    pl.semaphore_wait(barrier, g - 1 + g * near)

    for a in (RATES, MK, MQ):
        push(a, 0)

    def push_head(j):
        push(K, j)
        push(V, j)

        @pl.when(has_previous)
        def _():
            def one(t):
                e = lax.rem(place + t, g)
                remote(QX, j, place, e, home(e) - g).start()

            loop(0, g, one)

        push(Q, j)

    loop(0, per_device, push_head)

    @pl.when(jnp.logical_not(has_previous))
    def _():
        g_first[...] = jnp.zeros_like(g_first)
        c_first[...] = jnp.zeros_like(c_first)
        o_in[...] = jnp.zeros_like(o_in)
        l_in[...] = jnp.full_like(l_in, masked_score)

    arrive(RATES, 0)
    arrive(MK, 0)

    def gram_head(j):
        @pl.when(has_previous)
        def _():
            onward(GRAM, j, 0).wait_recv()

        keys = head_col(mk, j)
        gram_states(keys, keys, rates.at[j], g_first.at[j], gram.at[j], g_last.at[j])

        @pl.when(has_next)
        def _():
            onward(GRAM, j, 0).start()

    loop(0, per_device, gram_head)
    arrive(MQ, 0)

    def solve_head(j):
        ridge = ridge_in[pl.ds(place * per_device + j, 1), :]
        solve_all(head_col(mq, j), head_col(mk, j), rates.at[j], ridge, gram.at[j], head_col(x, j))

    loop(0, per_device, solve_head)

    def attend_head(j):
        queries, keys, values = head_col(q, j), head_col(k, j), head_col(v, j)
        arrive(K, j)
        arrive(V, j)

        @pl.when(has_next)
        def _():
            def one(i):
                remote(QX, j, i, place, home(i) + g).wait_recv()
                for low in range(0, g, 2):

                    @pl.when((i >= low) & (i < low + 2))
                    def _(low=low):
                        attend_back(
                            head_col(qx, j), keys, values, head_col(o_out, j), l_out.at[j],
                            i, low, g - low, rows,
                        )

                onward(PART, j, i).start()
                onward(LEVEL, j, i).start()

            loop(0, g, one)

        arrive(Q, j)

        def one(i):
            @pl.when(has_previous)
            def _():
                onward(PART, j, i).wait_recv()
                onward(LEVEL, j, i).wait_recv()

            for low in range(0, g, 2):

                @pl.when((i >= low) & (i < low + 2))
                def _(low=low):
                    attend_own(
                        queries, keys, values, head_col(o_in, j), l_in.at[j], head_col(att, j),
                        i, low + 2, rows,
                    )

            give(ATT, j, i)

        loop(0, g, one)

        @pl.when(has_previous)
        def _():
            onward(CROSS, j, 0).wait_recv()

        gram_states(
            head_col(mk, j), head_col(att, j), rates.at[j], c_first.at[j], cross.at[j], c_last.at[j]
        )

        @pl.when(has_next)
        def _():
            onward(CROSS, j, 0).start()

        def slab_out(i):
            read_out(
                head_col(mk, j), head_col(att, j), rates.at[j], cross.at[j], head_col(x, j),
                head_col(out, j), i,
            )
            give(OUT, j, i)

        loop(0, g, slab_out)

    loop(0, per_device, attend_head)

    def finish(j):
        for a in (ATT, OUT):
            arrive(a, j)
        for a in (Q, K, V, ATT, OUT):
            others(lambda e: remote(a, j, place, e, home(e)).wait_send())

        @pl.when(has_previous)
        def _():
            loop(0, g, lambda e: remote(QX, j, place, e, home(e) - g).wait_send())

        @pl.when(has_next)
        def _():
            def one(i):
                onward(PART, j, i).wait_send()
                onward(LEVEL, j, i).wait_send()

            loop(0, g, one)
            onward(GRAM, j, 0).wait_send()
            onward(CROSS, j, 0).wait_send()

    loop(0, per_device, finish)
    for a in (RATES, MK, MQ):
        others(lambda e: remote(a, 0, place, e, home(e)).wait_send())


def group_body(
    attn_query, attn_key, attn_value, mesa_query, mesa_key, log_decay, input_gate, regularizer
):
    rows = attn_query.shape[0]
    heads, size = regularizer.shape
    devices = lax.axis_size("seq")
    g = WINDOW // rows
    per_device, tokens = heads // g, WINDOW
    per, chunks = rows // CHUNK, tokens // CHUNK
    cum = jnp.cumsum(log_decay.reshape(per, CHUNK, heads), axis=1)
    rates = jnp.concatenate([cum, input_gate.reshape(per, CHUNK, heads)], axis=0)
    rates = jnp.pad(jnp.transpose(rates, (2, 0, 1)), ((0, 0), (0, 2 * per), (0, 0)))
    slab = jax.ShapeDtypeStruct((rows, heads * size), BF16)
    vmem = pl.BlockSpec(memory_space=pltpu.VMEM)
    anywhere = pl.BlockSpec(memory_space=pl.ANY)
    tall = pltpu.VMEM((tokens, per_device * size), BF16)
    levels = pltpu.VMEM((per_device, g, 8, rows), F32)
    state = pltpu.VMEM((per_device, size, size), BF16)
    states = pltpu.VMEM((per_device, chunks, size, size), BF16)
    return pl.pallas_call(
        functools.partial(group_kernel, devices, g),
        out_shape=(slab, slab),
        in_specs=[anywhere] * 5 + [vmem] * 2,
        out_specs=(anywhere, anywhere),
        scratch_shapes=[tall] * 6
        + [pltpu.VMEM((per_device, g, 4 * per, CHUNK), F32)]
        + [tall] * 4
        + [levels] * 2
        + [state] * 4
        + [states] * 2
        + [
            pltpu.VMEM((tokens, per_device * size), F32),
            pltpu.SemaphoreType.DMA((KINDS, per_device, g)),
            pltpu.SemaphoreType.DMA((KINDS, per_device, g)),
            pltpu.SemaphoreType.DMA((KINDS, per_device)),
        ],
        compiler_params=pltpu.CompilerParams(
            collective_id=0, has_side_effects=True, vmem_limit_bytes=56 * 1024 * 1024
        ),
    )(attn_query, attn_key, attn_value, mesa_key, mesa_query, rates, regularizer)


def fits_groups(mesh, rows, heads, size):
    g = WINDOW // rows
    return (
        size == CHUNK
        and WINDOW % rows == 0
        and g % 2 == 0
        and mesh.shape["seq"] % g == 0
        and heads % g == 0
        and rows % CHUNK == 0
        and WAYS % (rows // CHUNK) == 0
        and WINDOW % (CHUNK * WAYS) == 0
    )


def solution(mesh):
    spec = P(("groups", "seq"), None)

    def body(*args):
        heads, size = args[7].shape
        fits = fits_groups(mesh, args[0].shape[0], heads, size)
        return (group_body if fits else slab_body)(*args)

    return jax.shard_map(
        body,
        mesh=mesh,
        in_specs=(spec,) * 7 + (P(),),
        out_specs=(spec, spec),
        check_vma=False,
    )
```

```python
import jax
import jax.numpy as jnp
from jax import lax
from jax.experimental import pallas as pl
from jax.experimental.pallas import tpu as pltpu
from jax.sharding import PartitionSpec as P
import functools
import math

WINDOW = 2048
SPAN = 64
CG_ITERS = 8


exact_mode = lax.Precision.HIGHEST
masked_score = -1e30


def prefix(shard, axis, join, neutral):
    place = lax.axis_index(axis)
    gathered = jax.tree.map(
        lambda a, kind: lax.all_gather(a.astype(kind), axis), shard, (jnp.bfloat16, jnp.bfloat16)
    )
    state = jax.tree.map(lambda a, e: jnp.zeros_like(a) + jnp.asarray(e, a.dtype), shard, neutral)

    def one(lap, state):
        return join(
            state,
            jax.tree.map(
                lambda a, own: lax.dynamic_index_in_dim(a, lap, 0, False).astype(own.dtype),
                gathered,
                shard,
            ),
        )

    return lax.fori_loop(0, place, one, state)


def passed_along(value, axis, steps):
    count = lax.axis_size(axis)
    first, last = (max(0, -steps), min(count, count - steps))
    return lax.ppermute(value, axis, [(source, source + steps) for source in range(first, last)])


def span_update(states, inputs, ridge_diag):
    gram_start, cross_start = states
    queries, key_rows, value_rows, log_rates, gate_rows = inputs
    q_heads = jnp.transpose(queries, (1, 0, 2))
    k_heads = jnp.transpose(key_rows, (1, 0, 2))
    v_heads = jnp.transpose(value_rows, (1, 0, 2))
    cumulative = jnp.transpose(jnp.cumsum(log_rates, axis=0))
    length = cumulative.shape[1]
    causal = (jnp.arange(length)[:, None] >= jnp.arange(length)[None, :])[None]
    distance = cumulative[:, :, None] - cumulative[:, None, :]
    decay_mix = (
        jnp.where(causal, jnp.exp(jnp.where(causal, distance, 0.0)), 0.0)
        * jnp.transpose(gate_rows)[:, None, :]
    )
    start_scale = jnp.exp(cumulative)[:, :, None]
    iterate = jnp.zeros_like(q_heads)
    remain = q_heads
    search = q_heads
    norm_now = jnp.sum(remain * remain, axis=-1, keepdims=True)
    for sweep_index in range(CG_ITERS):
        carried = start_scale * jnp.einsum("hcd,hed->hce", search, gram_start, precision=exact_mode)
        operator_products = jnp.einsum("hjd,hid->hji", search, k_heads, precision=exact_mode)
        local_part = jnp.einsum(
            "hji,hid->hjd", decay_mix * operator_products, k_heads, precision=exact_mode
        )
        image_vec = carried + local_part + ridge_diag[:, None, :] * search
        step_size = norm_now / (jnp.sum(search * image_vec, axis=-1, keepdims=True) + 1e-06)
        iterate = iterate + step_size * search
        remain = remain - step_size * image_vec
        norm_next = jnp.sum(remain * remain, axis=-1, keepdims=True)
        search = remain + norm_next / (norm_now + 1e-06) * search
        norm_now = norm_next
    products = jnp.einsum("hjd,hid->hji", iterate, k_heads, precision=exact_mode)
    mesa_rows = start_scale * jnp.einsum("hje,hde->hjd", iterate, cross_start, precision=exact_mode)
    mesa_rows = mesa_rows + jnp.einsum(
        "hji,hid->hjd", decay_mix * products, v_heads, precision=exact_mode
    )
    tail_weight = (jnp.exp(cumulative[:, -1:] - cumulative) * jnp.transpose(gate_rows))[:, :, None]
    end_scale = jnp.exp(cumulative[:, -1])[:, None, None]
    gram_end = end_scale * gram_start + jnp.einsum(
        "hid,hie->hde", k_heads * tail_weight, k_heads, precision=exact_mode
    )
    cross_end = end_scale * cross_start + jnp.einsum(
        "hid,hie->hde", v_heads * tail_weight, k_heads, precision=exact_mode
    )
    return ((gram_end, cross_end), jnp.transpose(mesa_rows, (1, 0, 2)))


def mesa_pass(
    queries, key_rows, value_rows, log_rates, gate_rows, ridge_diag, gram_start, cross_start
):
    row_total = queries.shape[0]
    span_count = row_total // SPAN

    def shaped(array_in):
        return array_in.reshape((span_count, SPAN) + array_in.shape[1:])

    def advance(states, inputs):
        return span_update(states, inputs, ridge_diag)

    finished, outputs = lax.scan(
        advance,
        (gram_start, cross_start),
        (
            shaped(queries),
            shaped(key_rows),
            shaped(value_rows),
            shaped(log_rates),
            shaped(gate_rows),
        ),
    )
    return outputs.reshape(row_total, -1)


def fold_block(state_now, queries, key_value, query_first, key_first):
    running_max, running_sum, weighted = state_now
    row_count, head_count, head_size = queries.shape
    key_rows = key_value[0].reshape(-1, head_count, head_size)
    value_rows = key_value[1].reshape(-1, head_count, head_size)
    scores = jnp.einsum(
        "qhd,khd->hqk", queries, key_rows, preferred_element_type=jnp.float32
    ) * head_size ** (-0.5)
    query_pos = query_first + jnp.arange(row_count, dtype=jnp.int32)[:, None]
    key_pos = key_first + jnp.arange(key_rows.shape[0], dtype=jnp.int32)[None, :]
    distance = query_pos - key_pos
    inside = ((distance >= 0) & (distance < WINDOW) & (key_pos >= 0))[None]
    scores = jnp.where(inside, scores, masked_score)
    new_max = jnp.maximum(running_max, jnp.max(scores, axis=-1))
    weights = jnp.exp(scores - new_max[:, :, None]) * inside.astype(jnp.float32)
    rescale = jnp.exp(running_max - new_max)
    running_sum = running_sum * rescale + jnp.sum(weights, axis=-1)
    weighted = weighted * rescale[:, :, None] + jnp.einsum(
        "hqk,khd->hqd", weights.astype(jnp.bfloat16), value_rows, preferred_element_type=jnp.float32
    )
    return (new_max, running_sum, weighted)


def combine_pair(earlier, later):
    return (earlier[0] + later[0], jnp.exp(later[0])[:, None, None] * earlier[1] + later[1])


def slab_body(
    attn_query, attn_key, attn_value, mesa_query, mesa_key, log_decay, input_gate, regularizer
):
    row_count = attn_query.shape[0]
    head_count, head_size = regularizer.shape
    shape3 = (row_count, head_count, head_size)
    slab_first = lax.axis_index("seq") * row_count
    keys_float = mesa_key.astype(jnp.float32).reshape(shape3)
    slab_log = jnp.sum(log_decay, axis=0)
    tail_log = slab_log[None, :] - jnp.cumsum(log_decay, axis=0)
    weight_rows = (jnp.exp(tail_log) * input_gate)[:, :, None]
    gram_local = jnp.einsum(
        "lhd,lhe->hde", keys_float * weight_rows, keys_float, precision=exact_mode
    )
    zero_log = jnp.zeros_like(slab_log)
    zero_state = jnp.zeros_like(gram_local)
    gram_prefix = prefix((slab_log, gram_local), "seq", combine_pair, (zero_log, zero_state))[1]
    queries = attn_query.reshape(shape3)
    key_value = jnp.stack([attn_key, attn_value])
    state_now = (
        jnp.full((head_count, row_count), masked_score, jnp.float32),
        jnp.zeros((head_count, row_count), jnp.float32),
        jnp.zeros((head_count, row_count, head_size), jnp.float32),
    )
    state_now = fold_block(state_now, queries, key_value, slab_first, slab_first)
    reach = -(-WINDOW // row_count)
    moving = key_value
    for hop_index in range(1, reach + 1):
        moving = passed_along(moving, "seq", 1)
        state_now = fold_block(
            state_now, queries, moving, slab_first, slab_first - hop_index * row_count
        )
    normed = state_now[2] / state_now[1][:, :, None]
    attention = jnp.transpose(normed, (1, 0, 2)).reshape(row_count, -1).astype(jnp.bfloat16)
    values_float = attention.astype(jnp.float32).reshape(shape3)
    cross_local = jnp.einsum(
        "lhd,lhe->hde", values_float * weight_rows, keys_float, precision=exact_mode
    )
    cross_prefix = prefix((slab_log, cross_local), "seq", combine_pair, (zero_log, zero_state))[1]
    mesa_out = mesa_pass(
        mesa_query.astype(jnp.float32).reshape(shape3),
        keys_float,
        values_float,
        log_decay,
        input_gate,
        regularizer,
        gram_prefix,
        cross_prefix,
    )
    return (attention, mesa_out.astype(jnp.bfloat16))


CHUNK = 128
WAYS = 4
BF16 = jnp.bfloat16
F32 = jnp.float32
NT = (((1,), (1,)), ((), ()))
TN = (((0,), (0,)), ((), ()))


def dot(a, b, dims=None):
    if dims is None:
        return jnp.dot(a, b, preferred_element_type=F32)
    return lax.dot_general(a, b, dims, preferred_element_type=F32)


def two_terms(a):
    high = a.astype(BF16)
    low = (a - high.astype(F32)).astype(BF16)
    return jnp.concatenate([high, low], axis=1)


def score_blocks(queries, k_ref, base, count, rows, masks):
    scores, top = [], None
    for j in range(count):
        s = dot(queries, k_ref[pl.ds(base + j * rows, rows), :], NT)
        if masks[j] is not None:
            s = jnp.where(masks[j], s, masked_score)
        scores.append(s)
        top = s if top is None else jnp.maximum(top, s)
    return scores, jnp.max(top, axis=1, keepdims=True)


def weigh(scores, top, v_ref, base, rows, scale):
    total, weights = None, []
    for s in scores:
        w = jnp.exp2((s - top) * scale)
        total = w if total is None else total + w
        weights.append(w.astype(BF16))
    total = jnp.sum(total, axis=1, keepdims=True)
    summed = dot(
        jnp.concatenate(weights, axis=1), v_ref[pl.ds(base, len(scores) * rows), :]
    )
    return total, summed


def index_gap(rows):
    shape = (rows, rows)
    return lax.broadcasted_iota(jnp.int32, shape, 0) - lax.broadcasted_iota(jnp.int32, shape, 1)


def block_of(i, rows):
    if isinstance(i, int):
        return pl.ds(i * rows, rows)
    return pl.ds(pl.multiple_of(i * rows, rows), rows)


def partial(q_ref, k_ref, v_ref, i, base, masks, rows):
    scale = math.log2(math.e) / math.sqrt(q_ref.shape[1])
    queries = q_ref[block_of(i, rows), :]
    scores, top = score_blocks(queries, k_ref, base, len(masks), rows, masks)
    total, summed = weigh(scores, top, v_ref, base, rows, scale)
    return top * scale, total, summed


def joined(part, o_ref, l_ref, i, rows):
    level, total, summed = part
    earlier = jnp.transpose(jnp.broadcast_to(l_ref[i][:1, :], (summed.shape[1], rows)))
    peak = jnp.maximum(earlier, level)
    share_own, share_earlier = jnp.exp2(level - peak), jnp.exp2(earlier - peak)
    summed = summed * share_own + o_ref[block_of(i, rows), :].astype(F32) * share_earlier
    return peak, total * share_own + share_earlier, summed


def store_part(part, o_ref, l_ref, i, rows):
    level, total, summed = part
    o_ref[block_of(i, rows), :] = (summed / total).astype(BF16)
    level = jnp.broadcast_to(level + jnp.log2(total), summed.shape)
    l_ref[i] = jnp.transpose(level)[:8, :]


def attend_far(q_ref, k_ref, v_ref, o_ref, l_ref, rows):
    blocks = k_ref.shape[0] // rows
    beyond = index_gap(rows) < 0
    for i in range(blocks):
        masks = [beyond] + [None] * (blocks - i - 1)
        store_part(partial(q_ref, k_ref, v_ref, i, i * rows, masks, rows), o_ref, l_ref, i, rows)


def attend_middle(q_ref, k_ref, v_ref, o_in, l_in, o_ref, l_ref, rows):
    blocks = k_ref.shape[0] // rows

    def one(i, carry):
        part = partial(q_ref, k_ref, v_ref, i, 0, [None] * blocks, rows)
        store_part(joined(part, o_in, l_in, i, rows), o_ref, l_ref, i, rows)
        return carry

    lax.fori_loop(0, blocks, one, 0)


def attend_own(q_ref, k_ref, v_ref, o_in, l_in, out_ref, rows, done):
    blocks = k_ref.shape[0] // rows
    causal = index_gap(rows) >= 0
    for i in range(blocks):
        part = partial(q_ref, k_ref, v_ref, i, 0, [None] * i + [causal], rows)
        level, total, summed = joined(part, o_in, l_in, i, rows)
        out_ref[block_of(i, rows), :] = (summed / total).astype(BF16)
        done(i)


def flat(c, per):
    return c[0] * per + c[1]


def span(c, per):
    return pl.ds(pl.multiple_of(flat(c, per) * CHUNK, CHUNK), CHUNK)


def chunk_ids(g, per, ways=WAYS):
    slabs = ways // per
    return [(g * slabs + w // per, w % per) for w in range(ways)]


def column_form(row):
    return jnp.transpose(jnp.broadcast_to(row, (CHUNK, CHUNK)))


def rates_of(rates_ref, c):
    slab, place = c
    per = rates_ref.shape[1] // 4
    return rates_ref[slab, place : place + 1, :], rates_ref[slab, per + place : per + place + 1, :]


def tail_keys(k_ref, rates_ref, c, per):
    cum, gate = rates_of(rates_ref, c)
    weight = column_form(jnp.exp(cum[:, CHUNK - 1 :] - cum) * gate)
    keys = k_ref[span(c, per), :]
    return (keys.astype(F32) * weight).astype(BF16), jnp.exp(cum[:, CHUNK - 1 :])


def mix_of(rates_ref, c):
    cum, gate = rates_of(rates_ref, c)
    col = column_form(cum)
    shape = (CHUNK, CHUNK)
    causal = lax.broadcasted_iota(jnp.int32, shape, 0) >= lax.broadcasted_iota(
        jnp.int32, shape, 1
    )
    mix = jnp.exp(jnp.where(causal, col - cum, masked_score)) * gate
    return mix, jnp.exp(col)


def state_totals(k_ref, other_ref, rates_ref, zero_ref, total_ref):
    per = rates_ref.shape[1] // 4
    chunks = rates_ref.shape[0] * per

    def step(g, carry):
        state, decay = carry
        for c in chunk_ids(g, per):
            zero_ref[flat(c, per)] = state
            keys, end = tail_keys(k_ref, rates_ref, c, per)
            state = end * state + dot(keys, other_ref[span(c, per), :], TN)
            decay = decay * end
        return state, decay

    state, decay = lax.fori_loop(
        0, chunks // WAYS, step, (jnp.zeros((CHUNK, CHUNK), F32), jnp.ones((1, 1), F32))
    )
    total_ref[...] = state.astype(BF16)
    return decay


def state_starts(rates_ref, zero_ref, totals_ref, decay_ref, count, starts_ref):
    per = rates_ref.shape[1] // 4
    chunks = rates_ref.shape[0] * per

    def plane(p, first):
        return decay_ref(p) * first + totals_ref[p].astype(F32)

    first = lax.fori_loop(0, count, plane, jnp.zeros((CHUNK, CHUNK), F32))

    def step(g, first):
        for c in chunk_ids(g, per):
            starts_ref[flat(c, per)] = (zero_ref[flat(c, per)] + first).astype(BF16)
            cum, gate = rates_of(rates_ref, c)
            first = first * jnp.exp(cum[:, CHUNK - 1 :])
        return first

    lax.fori_loop(0, chunks // WAYS, step, first)


def solve_all(q_ref, k_ref, rates_ref, ridge_ref, gram_ref, x_ref):
    ridge = ridge_ref
    per = rates_ref.shape[1] // 4
    chunks = rates_ref.shape[0] * per

    def group(g, carry):
        ids = chunk_ids(g, per)
        mixes = [mix_of(rates_ref, c) for c in ids]
        keys = [k_ref[span(c, per), :] for c in ids]
        grams = [gram_ref[flat(c, per)] for c in ids]
        sides = [
            jnp.concatenate(
                [jnp.concatenate([a, a], axis=1), jnp.concatenate([k, k], axis=1)], axis=0
            )
            for a, k in zip(grams, keys)
        ]
        stacks = [jnp.concatenate([k, k], axis=0) for k in keys]
        state = []
        for c in ids:
            q = q_ref[span(c, per), :].astype(F32)
            state.append((jnp.zeros_like(q), q, q, jnp.sum(q * q, axis=1, keepdims=True)))

        def sweep(n, state):
            both = [dot(two_terms(s[2]), side, NT) for s, side in zip(state, sides)]
            local = [
                dot(two_terms(m[0] * b[:, CHUNK:]), k) for m, b, k in zip(mixes, both, stacks)
            ]
            out = []
            for (x, r, p, rr), b, l, m in zip(state, both, local, mixes):
                a = m[1] * b[:, :CHUNK] + l + ridge * p
                alpha = rr / (jnp.sum(p * a, axis=1, keepdims=True) + 1e-6)
                x = x + alpha * p
                r = r - alpha * a
                new = jnp.sum(r * r, axis=1, keepdims=True)
                p = r + (new / (rr + 1e-6)) * p
                out.append((x, r, p, new))
            return tuple(out)

        state = lax.fori_loop(0, CG_ITERS, sweep, tuple(state))
        for c, s in zip(ids, state):
            x_ref[span(c, per), :] = s[0]
        return carry

    lax.fori_loop(0, chunks // WAYS, group, 0)


def read_out(k_ref, v_ref, rates_ref, cross_ref, x_ref, out_ref, slab):
    per = rates_ref.shape[1] // 4
    for c in chunk_ids(slab, per, per):
        mix, start = mix_of(rates_ref, c)
        keys, values, cross = k_ref[span(c, per), :], v_ref[span(c, per), :], cross_ref[flat(c, per)]
        x = two_terms(x_ref[span(c, per), :])
        products = dot(x, jnp.concatenate([keys, keys], axis=1), NT)
        rows = start * dot(x, jnp.concatenate([cross, cross], axis=0))
        rows = rows + dot(two_terms(mix * products), jnp.concatenate([values, values], axis=0))
        out_ref[span(c, per), :] = rows.astype(BF16)


REACH = 2
Q, K, V, MK, MQ, RATES, ATT, OUT, GRAM, CROSS, DECAY = range(11)
QX, PART, LEVEL = (11, 13, 15)
KINDS = 17


def plane_kernel(n, g, *refs):
    ins, rates_in, ridge_in = refs[:5], refs[5], refs[6]
    results = refs[7:9]
    bufs, rates, homes = refs[9:14], refs[14], refs[15:17]
    later = (refs[9],) + refs[17:19]
    o_out, o_in = (None,) + refs[19:21], (None,) + refs[21:23]
    l_out, l_in = (None,) + refs[23:25], (None,) + refs[25:27]
    total_out, total_in = {GRAM: refs[27], CROSS: refs[28]}, {GRAM: refs[29], CROSS: refs[30]}
    decay_out, decay_in, zero = refs[31:34]
    gram, cross, x = refs[34:37]
    send, recv, own = refs[37:40]
    q, k, v, mk, mq = bufs
    att, out = homes
    rows, size = ins[0].shape[0], ridge_in.shape[1]
    per_device = rates.shape[0]
    wide = per_device * size
    planes = n // g
    group, me = lax.axis_index("groups"), lax.axis_index("seq")
    plane, place = me // g, lax.rem(me, g)

    def row_block(ref, s):
        return ref.at[pl.ds(pl.multiple_of(s * rows, rows), rows), :]

    def head_col(ref, j):
        return ref.at[:, pl.ds(pl.multiple_of(j * size, size), size)]

    def cell(ref, s, j):
        return ref.at[
            pl.ds(pl.multiple_of(s * rows, rows), rows),
            pl.ds(pl.multiple_of(j * size, size), size),
        ]

    def ends(a, j, source, target):
        if a in (MK, MQ):
            src = ins[a].at[:, pl.ds(pl.multiple_of(target * wide, wide), wide)]
            return src, row_block(bufs[a], source)
        if a in (Q, K, V):
            return head_col(ins[a], target * per_device + j), cell(bufs[a], source, j)
        if a == RATES:
            return rates_in.at[pl.ds(target * per_device, per_device)], rates.at[:, source]
        return cell(homes[a - ATT], target, j), head_col(results[a - ATT], source * per_device + j)

    def copy_to(src, dst, a, j, sent, got, peer):
        return pltpu.make_async_remote_copy(
            src_ref=src,
            dst_ref=dst,
            send_sem=send.at[a, j, sent],
            recv_sem=recv.at[a, j, got],
            device_id=(group, peer),
            device_id_type=pl.DeviceIdType.MESH,
        )

    def home(e):
        return plane * g + e

    def remote(a, j, source, target, peer):
        src, dst = ends(a, j, source, target)
        return copy_to(src, dst, a, j, target, source, home(peer))

    def local(a, j):
        src, dst = ends(a, j, place, place)
        return pltpu.make_async_copy(src, dst, own.at[a, j])

    def back(d, j):
        return copy_to(
            head_col(later[d - 1], j), head_col(later[d], j), QX + d - 1, j, 0, 0, me - g
        )

    def onward(a, d, j):
        if a == PART:
            src, dst = head_col(o_out[d], j), head_col(o_in[d], j)
        else:
            src, dst = l_out[d].at[j], l_in[d].at[j]
        return copy_to(src, dst, a + d - 1, j, 0, 0, me + g)

    def state(a, j, source, target, peer_plane):
        if a == DECAY:
            src, dst = decay_out, decay_in.at[source]
        else:
            src, dst = total_out[a].at[j], total_in[a].at[j, source]
        return copy_to(src, dst, a, j, target, source, peer_plane * g + place)

    def loop(first, last, act):
        def one(t, carry):
            act(t)
            return carry

        lax.fori_loop(first, last, one, 0)

    def others(act):
        loop(1, g, lambda t: act(lax.rem(place + t, g)))

    def later_planes(act):
        loop(plane + 1, planes, act)

    def signal(peer):
        pl.semaphore_signal(
            barrier, inc=1, device_id=(group, peer), device_id_type=pl.DeviceIdType.MESH
        )

    def push(a, j):
        others(lambda e: remote(a, j, place, e, e).start())
        local(a, j).start()

    def arrive(a, j):
        others(lambda e: remote(a, j, e, place, e).wait_recv())
        local(a, j).wait()

    def give(a, j, e):
        @pl.when(e != place)
        def _():
            remote(a, j, place, e, e).start()

        @pl.when(e == place)
        def _():
            local(a, j).start()

    def reaches(d):
        return plane + d < planes

    has_previous = plane > 0

    barrier = pltpu.get_barrier_semaphore()
    others(lambda e: signal(home(e)))
    loop(1, planes, lambda t: signal(lax.rem(plane + t, planes) * g + place))
    pl.semaphore_wait(barrier, g - 1 + planes - 1)

    push(RATES, 0)
    for j in range(per_device):
        push(Q, j)

    @pl.when(jnp.logical_not(has_previous))
    def _():
        for d in range(1, REACH + 1):
            o_in[d][...] = jnp.zeros_like(o_in[d])
            l_in[d][...] = jnp.full_like(l_in[d], masked_score)

    def forward(j):
        arrive(Q, j)

        @pl.when(has_previous)
        def _():
            back(1, j).start()

    def relay(j):
        @pl.when(reaches(1))
        def _():
            back(1, j).wait_recv()

            @pl.when(has_previous)
            def _():
                back(2, j).start()

    def push_values(j):
        push(K, j)
        push(V, j)

    for j in range(per_device):
        forward(j)
        if j == 0:
            push(MK, 0)
            push_values(0)
        if j > 0:
            relay(j - 1)
    push(MQ, 0)
    push_values(1)
    arrive(RATES, 0)
    arrive(MK, 0)

    def head_totals(a, j, others_ref):
        decay = state_totals(
            head_col(mk, j), head_col(others_ref, j), rates.at[j], zero.at[a - GRAM, j],
            total_out[a].at[j],
        )
        later_planes(lambda p: state(a, j, plane, p, p).start())
        return decay

    def head_starts(a, j, starts_ref):
        loop(0, plane, lambda p: state(a, j, p, plane, p).wait_recv())
        state_starts(
            rates.at[j], zero.at[a - GRAM, j], total_in[a].at[j],
            lambda p: decay_in[p, pl.ds(j, 1), :], plane, starts_ref.at[j],
        )

    def gram_head(j):
        decay = head_totals(GRAM, j, mk)
        decay_out[pl.ds(j, 1), :] = jnp.broadcast_to(decay, (1, size))

    loop(0, per_device, gram_head)
    later_planes(lambda p: state(DECAY, 0, plane, p, p).start())
    relay(per_device - 1)

    def step(s):
        far, middle, near, last = s, s - 1, s - 2, s - 3

        @pl.when(far < per_device)
        def _():
            j = far
            arrive(K, j)
            arrive(V, j)

            @pl.when(j + 2 < per_device)
            def _():
                push_values(j + 2)

            @pl.when(reaches(2))
            def _():
                back(2, j).wait_recv()
                attend_far(
                    head_col(later[2], j), head_col(k, j), head_col(v, j),
                    head_col(o_out[2], j), l_out[2].at[j], rows,
                )
                onward(PART, 2, j).start()
                onward(LEVEL, 2, j).start()

        @pl.when((middle >= 0) & (middle < per_device))
        def _():
            j = middle

            @pl.when(reaches(1))
            def _():
                @pl.when(has_previous)
                def _():
                    onward(PART, 2, j).wait_recv()
                    onward(LEVEL, 2, j).wait_recv()

                attend_middle(
                    head_col(later[1], j), head_col(k, j), head_col(v, j),
                    head_col(o_in[2], j), l_in[2].at[j],
                    head_col(o_out[1], j), l_out[1].at[j], rows,
                )
                onward(PART, 1, j).start()
                onward(LEVEL, 1, j).start()

            @pl.when(j == 0)
            def _():
                arrive(MQ, 0)
                loop(0, plane, lambda p: state(DECAY, 0, p, plane, p).wait_recv())

            head_starts(GRAM, j, gram)
            solve_all(
                head_col(mq, j), head_col(mk, j), rates.at[j],
                ridge_in[pl.ds(place * per_device + j, 1), :], gram.at[j], head_col(x, j),
            )

        @pl.when((near >= 0) & (near < per_device))
        def _():
            j = near

            @pl.when(has_previous)
            def _():
                onward(PART, 1, j).wait_recv()
                onward(LEVEL, 1, j).wait_recv()

            attend_own(
                head_col(q, j), head_col(k, j), head_col(v, j), head_col(o_in[1], j),
                l_in[1].at[j], head_col(att, j), rows, lambda i: give(ATT, j, i),
            )
            head_totals(CROSS, j, att)

        @pl.when(last >= 0)
        def _():
            j = last
            head_starts(CROSS, j, cross)

            def slab_out(i):
                read_out(
                    head_col(mk, j), head_col(att, j), rates.at[j], cross.at[j], head_col(x, j),
                    head_col(out, j), i,
                )
                give(OUT, j, i)

            loop(0, g, slab_out)

    loop(0, per_device + 3, step)

    def finish(j):
        for a in (ATT, OUT):
            arrive(a, j)
        for a in (Q, K, V, ATT, OUT):
            others(lambda e: remote(a, j, place, e, e).wait_send())

        @pl.when(has_previous)
        def _():
            back(1, j).wait_send()

            @pl.when(reaches(1))
            def _():
                back(2, j).wait_send()

        for d in range(1, REACH + 1):

            @pl.when(reaches(d))
            def _(d=d):
                onward(PART, d, j).wait_send()
                onward(LEVEL, d, j).wait_send()

        for a in (GRAM, CROSS):
            later_planes(lambda p: state(a, j, plane, p, p).wait_send())

    loop(0, per_device, finish)
    later_planes(lambda p: state(DECAY, 0, plane, p, p).wait_send())
    for a in (RATES, MK, MQ):
        others(lambda e: remote(a, 0, place, e, e).wait_send())


def plane_body(
    attn_query, attn_key, attn_value, mesa_query, mesa_key, log_decay, input_gate, regularizer
):
    rows = attn_query.shape[0]
    heads, size = regularizer.shape
    devices = lax.axis_size("seq")
    g = WINDOW // (REACH * rows)
    per_device, tokens, planes = heads // g, g * rows, devices // g
    per, chunks = rows // CHUNK, tokens // CHUNK
    cum = jnp.cumsum(log_decay.reshape(per, CHUNK, heads), axis=1)
    rates = jnp.concatenate([cum, input_gate.reshape(per, CHUNK, heads)], axis=0)
    rates = jnp.pad(jnp.transpose(rates, (2, 0, 1)), ((0, 0), (0, 2 * per), (0, 0)))
    slab = jax.ShapeDtypeStruct((rows, heads * size), BF16)
    vmem = pl.BlockSpec(memory_space=pltpu.VMEM)
    anywhere = pl.BlockSpec(memory_space=pl.ANY)
    tall = pltpu.VMEM((tokens, per_device * size), BF16)
    levels = pltpu.VMEM((per_device, g, 8, rows), F32)
    total = pltpu.VMEM((per_device, size, size), BF16)
    totals = pltpu.VMEM((per_device, planes, size, size), BF16)
    states = pltpu.VMEM((per_device, chunks, size, size), BF16)
    slots = max(g, planes)
    return pl.pallas_call(
        functools.partial(plane_kernel, devices, g),
        out_shape=(slab, slab),
        in_specs=[anywhere] * 5 + [vmem] * 2,
        out_specs=(anywhere, anywhere),
        scratch_shapes=[tall] * 5
        + [pltpu.VMEM((per_device, g, 4 * per, CHUNK), F32)]
        + [tall] * (2 + REACH + 2 * REACH)
        + [levels] * (2 * REACH)
        + [total] * 2
        + [totals] * 2
        + [
            pltpu.VMEM((8, size), F32),
            pltpu.VMEM((planes, 8, size), F32),
            pltpu.VMEM((2, per_device, chunks, size, size), F32),
        ]
        + [states] * 2
        + [
            pltpu.VMEM((tokens, per_device * size), F32),
            pltpu.SemaphoreType.DMA((KINDS, per_device, slots)),
            pltpu.SemaphoreType.DMA((KINDS, per_device, slots)),
            pltpu.SemaphoreType.DMA((KINDS, per_device)),
        ],
        compiler_params=pltpu.CompilerParams(
            collective_id=0, has_side_effects=True, vmem_limit_bytes=56 * 1024 * 1024
        ),
    )(attn_query, attn_key, attn_value, mesa_key, mesa_query, rates, regularizer)


def fits_planes(mesh, rows, heads, size):
    if WINDOW % (REACH * rows):
        return False
    g = WINDOW // (REACH * rows)
    return (
        size == CHUNK
        and mesh.shape["seq"] % g == 0
        and heads % g == 0
        and 2 <= heads // g <= 8
        and rows % CHUNK == 0
        and WAYS % (rows // CHUNK) == 0
        and g * rows % (CHUNK * WAYS) == 0
    )


def solution(mesh):
    spec = P(("groups", "seq"), None)

    def body(*args):
        heads, size = args[7].shape
        fits = fits_planes(mesh, args[0].shape[0], heads, size)
        return (plane_body if fits else slab_body)(*args)

    return jax.shard_map(
        body,
        mesh=mesh,
        in_specs=(spec,) * 7 + (P(),),
        out_specs=(spec, spec),
        check_vma=False,
    )
```

```python
import jax
import jax.numpy as jnp
from jax import lax
from jax.experimental import pallas as pl
from jax.experimental.pallas import tpu as pltpu
from jax.sharding import PartitionSpec as P
import functools
import math

WINDOW = 2048
SPAN = 64
CG_ITERS = 8


exact_mode = lax.Precision.HIGHEST
masked_score = -1e30


def prefix(shard, axis, join, neutral):
    place = lax.axis_index(axis)
    gathered = jax.tree.map(
        lambda a, kind: lax.all_gather(a.astype(kind), axis), shard, (jnp.bfloat16, jnp.bfloat16)
    )
    state = jax.tree.map(lambda a, e: jnp.zeros_like(a) + jnp.asarray(e, a.dtype), shard, neutral)

    def one(lap, state):
        return join(
            state,
            jax.tree.map(
                lambda a, own: lax.dynamic_index_in_dim(a, lap, 0, False).astype(own.dtype),
                gathered,
                shard,
            ),
        )

    return lax.fori_loop(0, place, one, state)


def passed_along(value, axis, steps):
    count = lax.axis_size(axis)
    first, last = (max(0, -steps), min(count, count - steps))
    return lax.ppermute(value, axis, [(source, source + steps) for source in range(first, last)])


def span_update(states, inputs, ridge_diag):
    gram_start, cross_start = states
    queries, key_rows, value_rows, log_rates, gate_rows = inputs
    q_heads = jnp.transpose(queries, (1, 0, 2))
    k_heads = jnp.transpose(key_rows, (1, 0, 2))
    v_heads = jnp.transpose(value_rows, (1, 0, 2))
    cumulative = jnp.transpose(jnp.cumsum(log_rates, axis=0))
    length = cumulative.shape[1]
    causal = (jnp.arange(length)[:, None] >= jnp.arange(length)[None, :])[None]
    distance = cumulative[:, :, None] - cumulative[:, None, :]
    decay_mix = (
        jnp.where(causal, jnp.exp(jnp.where(causal, distance, 0.0)), 0.0)
        * jnp.transpose(gate_rows)[:, None, :]
    )
    start_scale = jnp.exp(cumulative)[:, :, None]
    iterate = jnp.zeros_like(q_heads)
    remain = q_heads
    search = q_heads
    norm_now = jnp.sum(remain * remain, axis=-1, keepdims=True)
    for sweep_index in range(CG_ITERS):
        carried = start_scale * jnp.einsum("hcd,hed->hce", search, gram_start, precision=exact_mode)
        operator_products = jnp.einsum("hjd,hid->hji", search, k_heads, precision=exact_mode)
        local_part = jnp.einsum(
            "hji,hid->hjd", decay_mix * operator_products, k_heads, precision=exact_mode
        )
        image_vec = carried + local_part + ridge_diag[:, None, :] * search
        step_size = norm_now / (jnp.sum(search * image_vec, axis=-1, keepdims=True) + 1e-06)
        iterate = iterate + step_size * search
        remain = remain - step_size * image_vec
        norm_next = jnp.sum(remain * remain, axis=-1, keepdims=True)
        search = remain + norm_next / (norm_now + 1e-06) * search
        norm_now = norm_next
    products = jnp.einsum("hjd,hid->hji", iterate, k_heads, precision=exact_mode)
    mesa_rows = start_scale * jnp.einsum("hje,hde->hjd", iterate, cross_start, precision=exact_mode)
    mesa_rows = mesa_rows + jnp.einsum(
        "hji,hid->hjd", decay_mix * products, v_heads, precision=exact_mode
    )
    tail_weight = (jnp.exp(cumulative[:, -1:] - cumulative) * jnp.transpose(gate_rows))[:, :, None]
    end_scale = jnp.exp(cumulative[:, -1])[:, None, None]
    gram_end = end_scale * gram_start + jnp.einsum(
        "hid,hie->hde", k_heads * tail_weight, k_heads, precision=exact_mode
    )
    cross_end = end_scale * cross_start + jnp.einsum(
        "hid,hie->hde", v_heads * tail_weight, k_heads, precision=exact_mode
    )
    return ((gram_end, cross_end), jnp.transpose(mesa_rows, (1, 0, 2)))


def mesa_pass(
    queries, key_rows, value_rows, log_rates, gate_rows, ridge_diag, gram_start, cross_start
):
    row_total = queries.shape[0]
    span_count = row_total // SPAN

    def shaped(array_in):
        return array_in.reshape((span_count, SPAN) + array_in.shape[1:])

    def advance(states, inputs):
        return span_update(states, inputs, ridge_diag)

    finished, outputs = lax.scan(
        advance,
        (gram_start, cross_start),
        (
            shaped(queries),
            shaped(key_rows),
            shaped(value_rows),
            shaped(log_rates),
            shaped(gate_rows),
        ),
    )
    return outputs.reshape(row_total, -1)


def fold_block(state_now, queries, key_value, query_first, key_first):
    running_max, running_sum, weighted = state_now
    row_count, head_count, head_size = queries.shape
    key_rows = key_value[0].reshape(-1, head_count, head_size)
    value_rows = key_value[1].reshape(-1, head_count, head_size)
    scores = jnp.einsum(
        "qhd,khd->hqk", queries, key_rows, preferred_element_type=jnp.float32
    ) * head_size ** (-0.5)
    query_pos = query_first + jnp.arange(row_count, dtype=jnp.int32)[:, None]
    key_pos = key_first + jnp.arange(key_rows.shape[0], dtype=jnp.int32)[None, :]
    distance = query_pos - key_pos
    inside = ((distance >= 0) & (distance < WINDOW) & (key_pos >= 0))[None]
    scores = jnp.where(inside, scores, masked_score)
    new_max = jnp.maximum(running_max, jnp.max(scores, axis=-1))
    weights = jnp.exp(scores - new_max[:, :, None]) * inside.astype(jnp.float32)
    rescale = jnp.exp(running_max - new_max)
    running_sum = running_sum * rescale + jnp.sum(weights, axis=-1)
    weighted = weighted * rescale[:, :, None] + jnp.einsum(
        "hqk,khd->hqd", weights.astype(jnp.bfloat16), value_rows, preferred_element_type=jnp.float32
    )
    return (new_max, running_sum, weighted)


def combine_pair(earlier, later):
    return (earlier[0] + later[0], jnp.exp(later[0])[:, None, None] * earlier[1] + later[1])


def slab_body(
    attn_query, attn_key, attn_value, mesa_query, mesa_key, log_decay, input_gate, regularizer
):
    row_count = attn_query.shape[0]
    head_count, head_size = regularizer.shape
    shape3 = (row_count, head_count, head_size)
    slab_first = lax.axis_index("seq") * row_count
    keys_float = mesa_key.astype(jnp.float32).reshape(shape3)
    slab_log = jnp.sum(log_decay, axis=0)
    tail_log = slab_log[None, :] - jnp.cumsum(log_decay, axis=0)
    weight_rows = (jnp.exp(tail_log) * input_gate)[:, :, None]
    gram_local = jnp.einsum(
        "lhd,lhe->hde", keys_float * weight_rows, keys_float, precision=exact_mode
    )
    zero_log = jnp.zeros_like(slab_log)
    zero_state = jnp.zeros_like(gram_local)
    gram_prefix = prefix((slab_log, gram_local), "seq", combine_pair, (zero_log, zero_state))[1]
    queries = attn_query.reshape(shape3)
    key_value = jnp.stack([attn_key, attn_value])
    state_now = (
        jnp.full((head_count, row_count), masked_score, jnp.float32),
        jnp.zeros((head_count, row_count), jnp.float32),
        jnp.zeros((head_count, row_count, head_size), jnp.float32),
    )
    state_now = fold_block(state_now, queries, key_value, slab_first, slab_first)
    reach = -(-WINDOW // row_count)
    moving = key_value
    for hop_index in range(1, reach + 1):
        moving = passed_along(moving, "seq", 1)
        state_now = fold_block(
            state_now, queries, moving, slab_first, slab_first - hop_index * row_count
        )
    normed = state_now[2] / state_now[1][:, :, None]
    attention = jnp.transpose(normed, (1, 0, 2)).reshape(row_count, -1).astype(jnp.bfloat16)
    values_float = attention.astype(jnp.float32).reshape(shape3)
    cross_local = jnp.einsum(
        "lhd,lhe->hde", values_float * weight_rows, keys_float, precision=exact_mode
    )
    cross_prefix = prefix((slab_log, cross_local), "seq", combine_pair, (zero_log, zero_state))[1]
    mesa_out = mesa_pass(
        mesa_query.astype(jnp.float32).reshape(shape3),
        keys_float,
        values_float,
        log_decay,
        input_gate,
        regularizer,
        gram_prefix,
        cross_prefix,
    )
    return (attention, mesa_out.astype(jnp.bfloat16))


CHUNK = 128
WAYS = 4
BF16 = jnp.bfloat16
F32 = jnp.float32
NT = (((1,), (1,)), ((), ()))
TN = (((0,), (0,)), ((), ()))


def dot(a, b, dims=None):
    if dims is None:
        return jnp.dot(a, b, preferred_element_type=F32)
    return lax.dot_general(a, b, dims, preferred_element_type=F32)


def score_blocks(queries, k_ref, base, count, rows, masks):
    scores, top = [], None
    for j in range(count):
        s = dot(queries, k_ref[pl.ds(base + j * rows, rows), :], NT)
        if masks[j] is not None:
            s = jnp.where(masks[j], s, masked_score)
        scores.append(s)
        top = s if top is None else jnp.maximum(top, s)
    return scores, jnp.max(top, axis=1, keepdims=True)


def weigh(scores, top, v_ref, base, rows, scale):
    total, weights = None, []
    for s in scores:
        w = jnp.exp2((s - top) * scale)
        total = w if total is None else total + w
        weights.append(w.astype(BF16))
    total = jnp.sum(total, axis=1, keepdims=True)
    summed = dot(
        jnp.concatenate(weights, axis=1), v_ref[pl.ds(base, len(scores) * rows), :]
    )
    return total, summed


def index_gap(rows):
    shape = (rows, rows)
    return lax.broadcasted_iota(jnp.int32, shape, 0) - lax.broadcasted_iota(jnp.int32, shape, 1)


def block_of(i, rows):
    if isinstance(i, int):
        return pl.ds(i * rows, rows)
    return pl.ds(pl.multiple_of(i * rows, rows), rows)


def partial(q_ref, k_ref, v_ref, i, base, masks, rows):
    scale = math.log2(math.e) / math.sqrt(q_ref.shape[1])
    queries = q_ref[block_of(i, rows), :]
    scores, top = score_blocks(queries, k_ref, base, len(masks), rows, masks)
    total, summed = weigh(scores, top, v_ref, base, rows, scale)
    return top * scale, total, summed


def joined(part, o_ref, l_ref, i, rows):
    level, total, summed = part
    earlier = jnp.transpose(jnp.broadcast_to(l_ref[i][:1, :], (summed.shape[1], rows)))
    peak = jnp.maximum(earlier, level)
    share_own, share_earlier = jnp.exp2(level - peak), jnp.exp2(earlier - peak)
    summed = summed * share_own + o_ref[block_of(i, rows), :].astype(F32) * share_earlier
    return peak, total * share_own + share_earlier, summed


def store_part(part, o_ref, l_ref, i, rows):
    level, total, summed = part
    o_ref[block_of(i, rows), :] = (summed / total).astype(BF16)
    level = jnp.broadcast_to(level + jnp.log2(total), summed.shape)
    l_ref[i] = jnp.transpose(level)[:8, :]


def attend_far(q_ref, k_ref, v_ref, o_ref, l_ref, rows, done):
    blocks = k_ref.shape[0] // rows
    beyond = index_gap(rows) < 0
    for i in range(blocks):
        masks = [beyond] + [None] * (blocks - i - 1)
        store_part(partial(q_ref, k_ref, v_ref, i, i * rows, masks, rows), o_ref, l_ref, i, rows)
        done(i)


def attend_middle(q_ref, k_ref, v_ref, o_in, l_in, o_ref, l_ref, rows, ready, done):
    blocks = k_ref.shape[0] // rows

    def one(i, carry):
        part = partial(q_ref, k_ref, v_ref, i, 0, [None] * blocks, rows)
        ready(i)
        store_part(joined(part, o_in, l_in, i, rows), o_ref, l_ref, i, rows)
        done(i)
        return carry

    lax.fori_loop(0, blocks, one, 0)


def attend_own(q_ref, k_ref, v_ref, o_in, l_in, out_ref, rows, ready, done):
    blocks = k_ref.shape[0] // rows
    causal = index_gap(rows) >= 0
    for i in range(blocks):
        part = partial(q_ref, k_ref, v_ref, i, 0, [None] * i + [causal], rows)
        ready(i)
        level, total, summed = joined(part, o_in, l_in, i, rows)
        out_ref[block_of(i, rows), :] = (summed / total).astype(BF16)
        done(i)


def flat(c, per):
    return c[0] * per + c[1]


def span(c, per):
    return pl.ds(pl.multiple_of(flat(c, per) * CHUNK, CHUNK), CHUNK)


def chunk_ids(g, per, ways=WAYS):
    slabs = ways // per
    return [(g * slabs + w // per, w % per) for w in range(ways)]


def column_form(row):
    return jnp.transpose(jnp.broadcast_to(row, (CHUNK, CHUNK)))


def rates_of(rates_ref, c):
    slab, place = c
    per = rates_ref.shape[1] // 4
    return rates_ref[slab, place : place + 1, :], rates_ref[slab, per + place : per + place + 1, :]


def tail_keys(k_ref, rates_ref, c, per):
    cum, gate = rates_of(rates_ref, c)
    weight = column_form(jnp.exp(cum[:, CHUNK - 1 :] - cum) * gate)
    keys = k_ref[span(c, per), :]
    return (keys.astype(F32) * weight).astype(BF16), jnp.exp(cum[:, CHUNK - 1 :])


def mix_of(rates_ref, c):
    cum, gate = rates_of(rates_ref, c)
    col = column_form(cum)
    shape = (CHUNK, CHUNK)
    causal = lax.broadcasted_iota(jnp.int32, shape, 0) >= lax.broadcasted_iota(
        jnp.int32, shape, 1
    )
    mix = jnp.exp(jnp.where(causal, col - cum, masked_score)) * gate
    return mix, jnp.exp(col)


def state_totals(k_ref, other_ref, rates_ref, zero_ref, total_ref):
    per = rates_ref.shape[1] // 4
    chunks = rates_ref.shape[0] * per

    def step(g, carry):
        state, decay = carry
        for c in chunk_ids(g, per):
            zero_ref[flat(c, per)] = state
            keys, end = tail_keys(k_ref, rates_ref, c, per)
            state = end * state + dot(keys, other_ref[span(c, per), :], TN)
            decay = decay * end
        return state, decay

    state, decay = lax.fori_loop(
        0, chunks // WAYS, step, (jnp.zeros((CHUNK, CHUNK), F32), jnp.ones((1, 1), F32))
    )
    total_ref[...] = state.astype(BF16)
    return decay


def state_starts(rates_ref, zero_ref, totals_ref, decay_ref, count, starts_ref):
    per = rates_ref.shape[1] // 4
    chunks = rates_ref.shape[0] * per

    def plane(p, first):
        return decay_ref(p) * first + totals_ref[p].astype(F32)

    first = lax.fori_loop(0, count, plane, jnp.zeros((CHUNK, CHUNK), F32))

    def step(g, first):
        for c in chunk_ids(g, per):
            starts_ref[flat(c, per)] = (zero_ref[flat(c, per)] + first).astype(BF16)
            cum, gate = rates_of(rates_ref, c)
            first = first * jnp.exp(cum[:, CHUNK - 1 :])
        return first

    lax.fori_loop(0, chunks // WAYS, step, first)


def solve_all(q_ref, k_ref, rates_ref, ridge_ref, gram_ref, x_ref):
    per = rates_ref.shape[1] // 4
    chunks = rates_ref.shape[0] * per
    ways = math.gcd(chunks, 8)
    ridge = column_form(ridge_ref)
    later = lax.broadcasted_iota(jnp.int32, (CHUNK, CHUNK), 1) >= lax.broadcasted_iota(
        jnp.int32, (CHUNK, CHUNK), 0
    )

    def group(g, carry):
        ids = chunk_ids(g, per, ways)
        mixes, starts, keys, sides, state = [], [], [], [], []
        for c in ids:
            cum, gate = rates_of(rates_ref, c)
            gap = jnp.where(later, cum - column_form(cum), masked_score)
            mixes.append(jnp.exp(gap) * column_form(gate))
            starts.append(jnp.exp(cum))
            keys.append(k_ref[span(c, per), :])
            sides.append(
                jnp.concatenate([gram_ref[flat(c, per)], jnp.transpose(keys[-1])], axis=1)
            )
            q = jnp.transpose(q_ref[span(c, per), :]).astype(F32)
            state.append((jnp.zeros_like(q), q, q, jnp.sum(q * q, axis=0, keepdims=True)))
        for sweep_index in range(CG_ITERS):
            directions = [s[2].astype(BF16) for s in state]
            products = [dot(k, p) for k, p in zip(keys, directions)]
            images = [
                dot(
                    side,
                    jnp.concatenate(
                        [(start * p.astype(F32)).astype(BF16), (mix * b).astype(BF16)], axis=0
                    ),
                )
                for side, start, mix, p, b in zip(sides, starts, mixes, directions, products)
            ]
            for w, a in enumerate(images):
                x, r, _, rr = state[w]
                p = directions[w].astype(F32)
                a = a + ridge * p
                alpha = rr / (jnp.sum(p * a, axis=0, keepdims=True) + 1e-6)
                x = x + alpha * p
                r = r - alpha * a
                new = jnp.sum(r * r, axis=0, keepdims=True)
                state[w] = (x, r, r + (new / (rr + 1e-6)) * p, new)
        for c, s in zip(ids, state):
            x_ref[span(c, per), :] = jnp.transpose(s[0].astype(BF16))
        return carry

    lax.fori_loop(0, chunks // ways, group, 0)


def read_out(k_ref, v_ref, rates_ref, cross_ref, x_ref, out_ref, slab):
    per = rates_ref.shape[1] // 4
    for c in chunk_ids(slab, per, per):
        mix, start = mix_of(rates_ref, c)
        x = x_ref[span(c, per), :]
        products = dot(x, k_ref[span(c, per), :], NT)
        rows = start * dot(x, cross_ref[flat(c, per)])
        rows = rows + dot((mix * products).astype(BF16), v_ref[span(c, per), :])
        out_ref[span(c, per), :] = rows.astype(BF16)


REACH = 2
Q, K, V, MK, MQ, RATES, ATT, OUT, GRAM, CROSS, DECAY = range(11)
QX, PART, LEVEL = (11, 13, 15)
KINDS = 17


def push_order(heads):
    order = [(Q, 0), (K, 0), (V, 0), (Q, 1)]
    order += [(Q, j) for j in range(2, min(3, heads))]
    order += [(MK, j) for j in range(heads)]
    order += [(Q, j) for j in range(3, heads)]
    order += [(K, 1), (V, 1), (MQ, 0), (MQ, 1)]
    for j in range(2, heads):
        order += [(K, j), (V, j), (MQ, j)]
    return order


def plane_kernel(n, g, *refs):
    ins, rates_in, ridge_in = refs[:5], refs[5], refs[6]
    results = refs[7:9]
    bufs, rates, homes = refs[9:14], refs[14], refs[15:17]
    later = (refs[9],) + refs[17:19]
    o_out, o_in = (None,) + refs[19:21], (None,) + refs[21:23]
    l_out, l_in = (None,) + refs[23:25], (None,) + refs[25:27]
    total_out, total_in = {GRAM: refs[27], CROSS: refs[28]}, {GRAM: refs[29], CROSS: refs[30]}
    decay_out, decay_in, zero = refs[31:34]
    gram, cross, x = refs[34:37]
    send, recv, own = refs[37:40]
    q, k, v, mk, mq = bufs
    att, out = homes
    rows, size = ins[0].shape[0], ridge_in.shape[1]
    per_device = rates.shape[0]
    planes = n // g
    group, me = lax.axis_index("groups"), lax.axis_index("seq")
    plane, place = me // g, lax.rem(me, g)

    def head_col(ref, j):
        return ref.at[:, pl.ds(pl.multiple_of(j * size, size), size)]

    def cell(ref, s, j):
        return ref.at[
            pl.ds(pl.multiple_of(s * rows, rows), rows),
            pl.ds(pl.multiple_of(j * size, size), size),
        ]

    def ends(a, j, source, target):
        if a in (Q, K, V, MK, MQ):
            return head_col(ins[a], target * per_device + j), cell(bufs[a], source, j)
        if a == RATES:
            return rates_in.at[pl.ds(target * per_device, per_device)], rates.at[:, source]
        return cell(homes[a - ATT], target, j), head_col(results[a - ATT], source * per_device + j)

    def copy_to(src, dst, a, j, sent, got, peer):
        return pltpu.make_async_remote_copy(
            src_ref=src,
            dst_ref=dst,
            send_sem=send.at[a, j, sent],
            recv_sem=recv.at[a, j, got],
            device_id=(group, peer),
            device_id_type=pl.DeviceIdType.MESH,
        )

    def home(e):
        return plane * g + e

    def remote(a, j, source, target, peer):
        src, dst = ends(a, j, source, target)
        return copy_to(src, dst, a, j, target, source, home(peer))

    def local(a, j):
        src, dst = ends(a, j, place, place)
        return pltpu.make_async_copy(src, dst, own.at[a, j])

    def back(d, j, e):
        return copy_to(
            cell(later[d - 1], e, j), cell(later[d], e, j), QX + d - 1, j, e, e, me - g
        )

    def onward(a, d, j, i):
        if a == PART:
            src, dst = cell(o_out[d], i, j), cell(o_in[d], i, j)
        else:
            src, dst = l_out[d].at[j, i], l_in[d].at[j, i]
        return copy_to(src, dst, a + d - 1, j, i, i, me + g)

    def pass_on(d, j, i):
        onward(PART, d, j, i).start()
        onward(LEVEL, d, j, i).start()

    def take(d, j, i):
        @pl.when(has_previous)
        def _():
            onward(PART, d, j, i).wait_recv()
            onward(LEVEL, d, j, i).wait_recv()

    def state(a, j, source, target, peer_plane):
        if a == DECAY:
            src, dst = decay_out, decay_in.at[source]
        else:
            src, dst = total_out[a].at[j], total_in[a].at[j, source]
        return copy_to(src, dst, a, j, target, source, peer_plane * g + place)

    def loop(first, last, act):
        def one(t, carry):
            act(t)
            return carry

        lax.fori_loop(first, last, one, 0)

    def others(act):
        loop(1, g, lambda t: act(lax.rem(place + t, g)))

    def later_planes(act):
        loop(plane + 1, planes, act)

    def signal(peer):
        pl.semaphore_signal(
            barrier, inc=1, device_id=(group, peer), device_id_type=pl.DeviceIdType.MESH
        )

    def push(a, j):
        others(lambda e: remote(a, j, place, e, e).start())
        local(a, j).start()

    def arrive(a, j):
        others(lambda e: remote(a, j, e, place, e).wait_recv())
        local(a, j).wait()

    def give(a, j, e):
        @pl.when(e != place)
        def _():
            remote(a, j, place, e, e).start()

        @pl.when(e == place)
        def _():
            local(a, j).start()

    def reaches(d):
        return plane + d < planes

    has_previous = plane > 0

    barrier = pltpu.get_barrier_semaphore()
    others(lambda e: signal(home(e)))
    loop(1, planes, lambda t: signal(lax.rem(plane + t, planes) * g + place))
    pl.semaphore_wait(barrier, g - 1 + planes - 1)

    push(RATES, 0)
    for a, j in push_order(per_device):
        push(a, j)

    @pl.when(jnp.logical_not(has_previous))
    def _():
        for d in range(1, REACH + 1):
            o_in[d][...] = jnp.zeros_like(o_in[d])
            l_in[d][...] = jnp.full_like(l_in[d], masked_score)

    def near_first(act):
        loop(0, g, lambda t: act(place ^ t))

    def forward(j):
        def one(e):
            @pl.when(e == place)
            def _():
                local(Q, j).wait()

            @pl.when(e != place)
            def _():
                remote(Q, j, e, place, e).wait_recv()

            @pl.when(has_previous)
            def _():
                back(1, j, e).start()

        near_first(one)

    def relay(j):
        @pl.when(reaches(1))
        def _():
            def one(e):
                back(1, j, e).wait_recv()

                @pl.when(has_previous)
                def _():
                    back(2, j, e).start()

            near_first(one)

    forward(0)
    forward(1)
    relay(0)
    arrive(RATES, 0)

    def head_totals(a, j, others_ref):
        decay = state_totals(
            head_col(mk, j), head_col(others_ref, j), rates.at[j], zero.at[a - GRAM, j],
            total_out[a].at[j],
        )
        later_planes(lambda p: state(a, j, plane, p, p).start())
        return decay

    def head_starts(a, j, starts_ref):
        loop(0, plane, lambda p: state(a, j, p, plane, p).wait_recv())
        state_starts(
            rates.at[j], zero.at[a - GRAM, j], total_in[a].at[j],
            lambda p: decay_in[p, pl.ds(j, 1), :], plane, starts_ref.at[j],
        )

    def gram_head(j):
        arrive(MK, j)
        decay = head_totals(GRAM, j, mk)
        decay_out[pl.ds(j, 1), :] = jnp.broadcast_to(decay, (1, size))

    def step(s):
        far, middle, near, last = s, s - 1, s - 2, s - 3

        @pl.when(far + 1 < per_device)
        def _():
            relay(far + 1)

        @pl.when(far + 2 < per_device)
        def _():
            forward(far + 2)

        @pl.when(far < per_device)
        def _():
            j = far
            arrive(K, j)
            arrive(V, j)

            @pl.when(reaches(2))
            def _():
                loop(0, g, lambda e: back(2, j, e).wait_recv())
                attend_far(
                    head_col(later[2], j), head_col(k, j), head_col(v, j),
                    head_col(o_out[2], j), l_out[2].at[j], rows, lambda i: pass_on(2, j, i),
                )

        @pl.when((middle >= 0) & (middle < per_device))
        def _():
            j = middle

            @pl.when(reaches(1))
            def _():
                attend_middle(
                    head_col(later[1], j), head_col(k, j), head_col(v, j),
                    head_col(o_in[2], j), l_in[2].at[j],
                    head_col(o_out[1], j), l_out[1].at[j], rows,
                    lambda i: take(2, j, i), lambda i: pass_on(1, j, i),
                )

            @pl.when(j == 0)
            def _():
                loop(0, plane, lambda p: state(DECAY, 0, p, plane, p).wait_recv())

            head_starts(GRAM, j, gram)
            arrive(MQ, j)
            solve_all(
                head_col(mq, j), head_col(mk, j), rates.at[j],
                ridge_in[pl.ds(place * per_device + j, 1), :], gram.at[j], head_col(x, j),
            )

        @pl.when((near >= 0) & (near < per_device))
        def _():
            j = near
            attend_own(
                head_col(q, j), head_col(k, j), head_col(v, j), head_col(o_in[1], j),
                l_in[1].at[j], head_col(att, j), rows,
                lambda i: take(1, j, i), lambda i: give(ATT, j, i),
            )
            head_totals(CROSS, j, att)

        @pl.when(s == 0)
        def _():
            loop(0, per_device, gram_head)
            later_planes(lambda p: state(DECAY, 0, plane, p, p).start())

        @pl.when(last >= 0)
        def _():
            j = last
            head_starts(CROSS, j, cross)

            def slab_out(i):
                read_out(
                    head_col(mk, j), head_col(att, j), rates.at[j], cross.at[j], head_col(x, j),
                    head_col(out, j), i,
                )
                give(OUT, j, i)

            loop(0, g, slab_out)

    loop(0, per_device + 3, step)

    def finish(j):
        for a in (ATT, OUT):
            arrive(a, j)
        for a in (Q, K, V, MK, MQ, ATT, OUT):
            others(lambda e: remote(a, j, place, e, e).wait_send())

        def block(i):
            @pl.when(has_previous)
            def _():
                back(1, j, i).wait_send()

                @pl.when(reaches(1))
                def _():
                    back(2, j, i).wait_send()

            for d in range(1, REACH + 1):

                @pl.when(reaches(d))
                def _(d=d):
                    onward(PART, d, j, i).wait_send()
                    onward(LEVEL, d, j, i).wait_send()

        loop(0, g, block)
        for a in (GRAM, CROSS):
            later_planes(lambda p: state(a, j, plane, p, p).wait_send())

    loop(0, per_device, finish)
    later_planes(lambda p: state(DECAY, 0, plane, p, p).wait_send())
    others(lambda e: remote(RATES, 0, place, e, e).wait_send())


def plane_body(
    attn_query, attn_key, attn_value, mesa_query, mesa_key, log_decay, input_gate, regularizer
):
    rows = attn_query.shape[0]
    heads, size = regularizer.shape
    devices = lax.axis_size("seq")
    g = WINDOW // (REACH * rows)
    per_device, tokens, planes = heads // g, g * rows, devices // g
    per, chunks = rows // CHUNK, tokens // CHUNK
    cum = jnp.cumsum(log_decay.reshape(per, CHUNK, heads), axis=1)
    rates = jnp.concatenate([cum, input_gate.reshape(per, CHUNK, heads)], axis=0)
    rates = jnp.pad(jnp.transpose(rates, (2, 0, 1)), ((0, 0), (0, 2 * per), (0, 0)))
    slab = jax.ShapeDtypeStruct((rows, heads * size), BF16)
    vmem = pl.BlockSpec(memory_space=pltpu.VMEM)
    anywhere = pl.BlockSpec(memory_space=pl.ANY)
    tall = pltpu.VMEM((tokens, per_device * size), BF16)
    levels = pltpu.VMEM((per_device, g, 8, rows), F32)
    total = pltpu.VMEM((per_device, size, size), BF16)
    totals = pltpu.VMEM((per_device, planes, size, size), BF16)
    states = pltpu.VMEM((per_device, chunks, size, size), BF16)
    slots = max(g, planes)
    return pl.pallas_call(
        functools.partial(plane_kernel, devices, g),
        out_shape=(slab, slab),
        in_specs=[anywhere] * 5 + [vmem] * 2,
        out_specs=(anywhere, anywhere),
        scratch_shapes=[tall] * 5
        + [pltpu.VMEM((per_device, g, 4 * per, CHUNK), F32)]
        + [tall] * (2 + REACH + 2 * REACH)
        + [levels] * (2 * REACH)
        + [total] * 2
        + [totals] * 2
        + [
            pltpu.VMEM((8, size), F32),
            pltpu.VMEM((planes, 8, size), F32),
            pltpu.VMEM((2, per_device, chunks, size, size), F32),
        ]
        + [states] * 2
        + [
            tall,
            pltpu.SemaphoreType.DMA((KINDS, per_device, slots)),
            pltpu.SemaphoreType.DMA((KINDS, per_device, slots)),
            pltpu.SemaphoreType.DMA((KINDS, per_device)),
        ],
        compiler_params=pltpu.CompilerParams(
            collective_id=0, has_side_effects=True, vmem_limit_bytes=56 * 1024 * 1024
        ),
    )(attn_query, attn_key, attn_value, mesa_key, mesa_query, rates, regularizer)


def fits_planes(mesh, rows, heads, size):
    if WINDOW % (REACH * rows):
        return False
    g = WINDOW // (REACH * rows)
    return (
        size == CHUNK
        and g & (g - 1) == 0
        and mesh.shape["seq"] % g == 0
        and heads % g == 0
        and 2 <= heads // g <= 8
        and rows % CHUNK == 0
        and WAYS % (rows // CHUNK) == 0
        and g * rows % (CHUNK * WAYS) == 0
    )


def solution(mesh):
    spec = P(("groups", "seq"), None)

    def body(*args):
        heads, size = args[7].shape
        fits = fits_planes(mesh, args[0].shape[0], heads, size)
        return (plane_body if fits else slab_body)(*args)

    return jax.shard_map(
        body,
        mesh=mesh,
        in_specs=(spec,) * 7 + (P(),),
        out_specs=(spec, spec),
        check_vma=False,
    )
```

```python
import jax
import jax.numpy as jnp
from jax import lax
from jax.experimental import pallas as pl
from jax.experimental.pallas import tpu as pltpu
from jax.sharding import PartitionSpec as P
import functools
import math

WINDOW = 2048
SPAN = 64
CG_ITERS = 8


exact_mode = lax.Precision.HIGHEST
masked_score = -1e30


def prefix(shard, axis, join, neutral):
    place = lax.axis_index(axis)
    gathered = jax.tree.map(
        lambda a, kind: lax.all_gather(a.astype(kind), axis), shard, (jnp.bfloat16, jnp.bfloat16)
    )
    state = jax.tree.map(lambda a, e: jnp.zeros_like(a) + jnp.asarray(e, a.dtype), shard, neutral)

    def one(lap, state):
        return join(
            state,
            jax.tree.map(
                lambda a, own: lax.dynamic_index_in_dim(a, lap, 0, False).astype(own.dtype),
                gathered,
                shard,
            ),
        )

    return lax.fori_loop(0, place, one, state)


def passed_along(value, axis, steps):
    count = lax.axis_size(axis)
    first, last = (max(0, -steps), min(count, count - steps))
    return lax.ppermute(value, axis, [(source, source + steps) for source in range(first, last)])


def span_update(states, inputs, ridge_diag):
    gram_start, cross_start = states
    queries, key_rows, value_rows, log_rates, gate_rows = inputs
    q_heads = jnp.transpose(queries, (1, 0, 2))
    k_heads = jnp.transpose(key_rows, (1, 0, 2))
    v_heads = jnp.transpose(value_rows, (1, 0, 2))
    cumulative = jnp.transpose(jnp.cumsum(log_rates, axis=0))
    length = cumulative.shape[1]
    causal = (jnp.arange(length)[:, None] >= jnp.arange(length)[None, :])[None]
    distance = cumulative[:, :, None] - cumulative[:, None, :]
    decay_mix = (
        jnp.where(causal, jnp.exp(jnp.where(causal, distance, 0.0)), 0.0)
        * jnp.transpose(gate_rows)[:, None, :]
    )
    start_scale = jnp.exp(cumulative)[:, :, None]
    iterate = jnp.zeros_like(q_heads)
    remain = q_heads
    search = q_heads
    norm_now = jnp.sum(remain * remain, axis=-1, keepdims=True)
    for sweep_index in range(CG_ITERS):
        carried = start_scale * jnp.einsum("hcd,hed->hce", search, gram_start, precision=exact_mode)
        operator_products = jnp.einsum("hjd,hid->hji", search, k_heads, precision=exact_mode)
        local_part = jnp.einsum(
            "hji,hid->hjd", decay_mix * operator_products, k_heads, precision=exact_mode
        )
        image_vec = carried + local_part + ridge_diag[:, None, :] * search
        step_size = norm_now / (jnp.sum(search * image_vec, axis=-1, keepdims=True) + 1e-06)
        iterate = iterate + step_size * search
        remain = remain - step_size * image_vec
        norm_next = jnp.sum(remain * remain, axis=-1, keepdims=True)
        search = remain + norm_next / (norm_now + 1e-06) * search
        norm_now = norm_next
    products = jnp.einsum("hjd,hid->hji", iterate, k_heads, precision=exact_mode)
    mesa_rows = start_scale * jnp.einsum("hje,hde->hjd", iterate, cross_start, precision=exact_mode)
    mesa_rows = mesa_rows + jnp.einsum(
        "hji,hid->hjd", decay_mix * products, v_heads, precision=exact_mode
    )
    tail_weight = (jnp.exp(cumulative[:, -1:] - cumulative) * jnp.transpose(gate_rows))[:, :, None]
    end_scale = jnp.exp(cumulative[:, -1])[:, None, None]
    gram_end = end_scale * gram_start + jnp.einsum(
        "hid,hie->hde", k_heads * tail_weight, k_heads, precision=exact_mode
    )
    cross_end = end_scale * cross_start + jnp.einsum(
        "hid,hie->hde", v_heads * tail_weight, k_heads, precision=exact_mode
    )
    return ((gram_end, cross_end), jnp.transpose(mesa_rows, (1, 0, 2)))


def mesa_pass(
    queries, key_rows, value_rows, log_rates, gate_rows, ridge_diag, gram_start, cross_start
):
    row_total = queries.shape[0]
    span_count = row_total // SPAN

    def shaped(array_in):
        return array_in.reshape((span_count, SPAN) + array_in.shape[1:])

    def advance(states, inputs):
        return span_update(states, inputs, ridge_diag)

    finished, outputs = lax.scan(
        advance,
        (gram_start, cross_start),
        (
            shaped(queries),
            shaped(key_rows),
            shaped(value_rows),
            shaped(log_rates),
            shaped(gate_rows),
        ),
    )
    return outputs.reshape(row_total, -1)


def fold_block(state_now, queries, key_value, query_first, key_first):
    running_max, running_sum, weighted = state_now
    row_count, head_count, head_size = queries.shape
    key_rows = key_value[0].reshape(-1, head_count, head_size)
    value_rows = key_value[1].reshape(-1, head_count, head_size)
    scores = jnp.einsum(
        "qhd,khd->hqk", queries, key_rows, preferred_element_type=jnp.float32
    ) * head_size ** (-0.5)
    query_pos = query_first + jnp.arange(row_count, dtype=jnp.int32)[:, None]
    key_pos = key_first + jnp.arange(key_rows.shape[0], dtype=jnp.int32)[None, :]
    distance = query_pos - key_pos
    inside = ((distance >= 0) & (distance < WINDOW) & (key_pos >= 0))[None]
    scores = jnp.where(inside, scores, masked_score)
    new_max = jnp.maximum(running_max, jnp.max(scores, axis=-1))
    weights = jnp.exp(scores - new_max[:, :, None]) * inside.astype(jnp.float32)
    rescale = jnp.exp(running_max - new_max)
    running_sum = running_sum * rescale + jnp.sum(weights, axis=-1)
    weighted = weighted * rescale[:, :, None] + jnp.einsum(
        "hqk,khd->hqd", weights.astype(jnp.bfloat16), value_rows, preferred_element_type=jnp.float32
    )
    return (new_max, running_sum, weighted)


def combine_pair(earlier, later):
    return (earlier[0] + later[0], jnp.exp(later[0])[:, None, None] * earlier[1] + later[1])


def slab_body(
    attn_query, attn_key, attn_value, mesa_query, mesa_key, log_decay, input_gate, regularizer
):
    row_count = attn_query.shape[0]
    head_count, head_size = regularizer.shape
    shape3 = (row_count, head_count, head_size)
    slab_first = lax.axis_index("seq") * row_count
    keys_float = mesa_key.astype(jnp.float32).reshape(shape3)
    slab_log = jnp.sum(log_decay, axis=0)
    tail_log = slab_log[None, :] - jnp.cumsum(log_decay, axis=0)
    weight_rows = (jnp.exp(tail_log) * input_gate)[:, :, None]
    gram_local = jnp.einsum(
        "lhd,lhe->hde", keys_float * weight_rows, keys_float, precision=exact_mode
    )
    zero_log = jnp.zeros_like(slab_log)
    zero_state = jnp.zeros_like(gram_local)
    gram_prefix = prefix((slab_log, gram_local), "seq", combine_pair, (zero_log, zero_state))[1]
    queries = attn_query.reshape(shape3)
    key_value = jnp.stack([attn_key, attn_value])
    state_now = (
        jnp.full((head_count, row_count), masked_score, jnp.float32),
        jnp.zeros((head_count, row_count), jnp.float32),
        jnp.zeros((head_count, row_count, head_size), jnp.float32),
    )
    state_now = fold_block(state_now, queries, key_value, slab_first, slab_first)
    reach = -(-WINDOW // row_count)
    moving = key_value
    for hop_index in range(1, reach + 1):
        moving = passed_along(moving, "seq", 1)
        state_now = fold_block(
            state_now, queries, moving, slab_first, slab_first - hop_index * row_count
        )
    normed = state_now[2] / state_now[1][:, :, None]
    attention = jnp.transpose(normed, (1, 0, 2)).reshape(row_count, -1).astype(jnp.bfloat16)
    values_float = attention.astype(jnp.float32).reshape(shape3)
    cross_local = jnp.einsum(
        "lhd,lhe->hde", values_float * weight_rows, keys_float, precision=exact_mode
    )
    cross_prefix = prefix((slab_log, cross_local), "seq", combine_pair, (zero_log, zero_state))[1]
    mesa_out = mesa_pass(
        mesa_query.astype(jnp.float32).reshape(shape3),
        keys_float,
        values_float,
        log_decay,
        input_gate,
        regularizer,
        gram_prefix,
        cross_prefix,
    )
    return (attention, mesa_out.astype(jnp.bfloat16))


CHUNK = 128
WAYS = 4
BF16 = jnp.bfloat16
F32 = jnp.float32
NT = (((1,), (1,)), ((), ()))
TN = (((0,), (0,)), ((), ()))


def dot(a, b, dims=None):
    if dims is None:
        return jnp.dot(a, b, preferred_element_type=F32)
    return lax.dot_general(a, b, dims, preferred_element_type=F32)


def score_blocks(queries, k_ref, base, count, rows, masks):
    scores, top = [], None
    for j in range(count):
        s = dot(queries, k_ref[pl.ds(base + j * rows, rows), :], NT)
        if masks[j] is not None:
            s = jnp.where(masks[j], s, masked_score)
        scores.append(s)
        top = s if top is None else jnp.maximum(top, s)
    return scores, jnp.max(top, axis=1, keepdims=True)


def weigh(scores, top, v_ref, base, rows, scale):
    total, weights = None, []
    for s in scores:
        w = jnp.exp2((s - top) * scale)
        total = w if total is None else total + w
        weights.append(w.astype(BF16))
    total = jnp.sum(total, axis=1, keepdims=True)
    summed = dot(
        jnp.concatenate(weights, axis=1), v_ref[pl.ds(base, len(scores) * rows), :]
    )
    return total, summed


def index_gap(rows):
    shape = (rows, rows)
    return lax.broadcasted_iota(jnp.int32, shape, 0) - lax.broadcasted_iota(jnp.int32, shape, 1)


def block_of(i, rows):
    if isinstance(i, int):
        return pl.ds(i * rows, rows)
    return pl.ds(pl.multiple_of(i * rows, rows), rows)


def partial(q_ref, k_ref, v_ref, i, base, masks, rows):
    scale = math.log2(math.e) / math.sqrt(q_ref.shape[1])
    queries = q_ref[block_of(i, rows), :]
    scores, top = score_blocks(queries, k_ref, base, len(masks), rows, masks)
    total, summed = weigh(scores, top, v_ref, base, rows, scale)
    return top * scale, total, summed


def columns(row, size):
    return jnp.transpose(jnp.broadcast_to(row, (size, row.shape[1])))


def joined(part, o_ref, l_ref, i, rows):
    level, total, summed = part
    earlier = columns(l_ref[i], summed.shape[1])
    peak = jnp.maximum(earlier, level)
    share_own, share_earlier = jnp.exp2(level - peak), jnp.exp2(earlier - peak)
    summed = summed * share_own + o_ref[block_of(i, rows), :].astype(F32) * share_earlier
    return peak, total * share_own + share_earlier, summed


def store_part(part, o_ref, l_ref, i, rows):
    level, total, summed = part
    o_ref[block_of(i, rows), :] = (summed / total).astype(o_ref.dtype)
    level = jnp.broadcast_to(level + jnp.log2(total), summed.shape)
    l_ref[i] = jnp.transpose(level)[:1, :]


def attend_far(q_ref, k_ref, v_ref, o_ref, l_ref, rows, done):
    blocks = k_ref.shape[0] // rows
    beyond = index_gap(rows) < 0
    for i in range(0, blocks, 2):
        for n in (i, i + 1):
            masks = [beyond] + [None] * (blocks - n - 1)
            part = partial(q_ref, k_ref, v_ref, n, n * rows, masks, rows)
            store_part(part, o_ref, l_ref, n, rows)
        done(i)
        done(i + 1)


def attend_middle(q_ref, k_ref, v_ref, o_in, l_in, o_ref, l_ref, rows, ready, done):
    blocks = k_ref.shape[0] // rows

    def two(t, carry):
        pair = (2 * t, 2 * t + 1)
        ready(t)
        for i in pair:
            part = partial(q_ref, k_ref, v_ref, i, 0, [None] * blocks, rows)
            store_part(joined(part, o_in, l_in, i, rows), o_ref, l_ref, i, rows)
        for i in pair:
            done(i)
        return carry

    lax.fori_loop(0, blocks // 2, two, 0)


def attend_own(q_ref, k_ref, v_ref, o_ref, l_ref, rows):
    causal = index_gap(rows) >= 0
    for i in range(k_ref.shape[0] // rows):
        part = partial(q_ref, k_ref, v_ref, i, 0, [None] * i + [causal], rows)
        store_part(part, o_ref, l_ref, i, rows)


def attend_last(o_own, l_own, o_in, l_in, out_ref, rows, ready, done):
    blocks = o_own.shape[0] // rows
    for i in range(0, blocks, 2):
        ready(i // 2)
        for n in (i, i + 1):
            own = (columns(l_own[n], o_own.shape[1]), 1.0, o_own[block_of(n, rows), :])
            level, total, summed = joined(own, o_in, l_in, n, rows)
            out_ref[block_of(n, rows), :] = (summed / total).astype(BF16)
        for n in (i, i + 1):
            done(n)


def flat(c, per):
    return c[0] * per + c[1]


def span(c, per):
    return pl.ds(pl.multiple_of(flat(c, per) * CHUNK, CHUNK), CHUNK)


def chunk_ids(g, per, ways=WAYS):
    slabs = ways // per
    return [(g * slabs + w // per, w % per) for w in range(ways)]


def column_form(row):
    return jnp.transpose(jnp.broadcast_to(row, (CHUNK, CHUNK)))


def rates_of(rates_ref, c):
    slab, place = c
    per = rates_ref.shape[1] // 4
    return rates_ref[slab, place : place + 1, :], rates_ref[slab, per + place : per + place + 1, :]


def tail_keys(k_ref, rates_ref, c, per):
    cum, gate = rates_of(rates_ref, c)
    weight = column_form(jnp.exp(cum[:, CHUNK - 1 :] - cum) * gate)
    keys = k_ref[span(c, per), :]
    return (keys.astype(F32) * weight).astype(BF16), jnp.exp(cum[:, CHUNK - 1 :])


def mix_of(rates_ref, c):
    cum, gate = rates_of(rates_ref, c)
    col = column_form(cum)
    shape = (CHUNK, CHUNK)
    causal = lax.broadcasted_iota(jnp.int32, shape, 0) >= lax.broadcasted_iota(
        jnp.int32, shape, 1
    )
    mix = jnp.exp(jnp.where(causal, col - cum, masked_score)) * gate
    return mix, jnp.exp(col)


def state_totals(k_ref, other_ref, rates_ref, zero_ref):
    per = rates_ref.shape[1] // 4
    chunks = rates_ref.shape[0] * per

    def step(g, carry):
        state, decay = carry
        for c in chunk_ids(g, per):
            zero_ref[flat(c, per)] = state
            keys, end = tail_keys(k_ref, rates_ref, c, per)
            state = end * state + dot(keys, other_ref[span(c, per), :], TN)
            decay = decay * end
        return state, decay

    state, decay = lax.fori_loop(
        0, chunks // WAYS, step, (jnp.zeros((CHUNK, CHUNK), F32), jnp.ones((1, 1), F32))
    )
    zero_ref[chunks] = state
    return decay


def state_starts(rates_ref, zero_ref, first_ref, starts_ref):
    per = rates_ref.shape[1] // 4
    chunks = rates_ref.shape[0] * per

    def step(g, first):
        for c in chunk_ids(g, per):
            starts_ref[flat(c, per)] = (zero_ref[flat(c, per)] + first).astype(BF16)
            cum, gate = rates_of(rates_ref, c)
            first = first * jnp.exp(cum[:, CHUNK - 1 :])
        return first

    lax.fori_loop(0, chunks // WAYS, step, first_ref[...].astype(F32))


def solve_all(q_ref, k_ref, rates_ref, ridge_ref, gram_ref, x_ref):
    per = rates_ref.shape[1] // 4
    chunks = rates_ref.shape[0] * per
    ways = math.gcd(chunks, 8)
    ridge = column_form(ridge_ref)
    later = lax.broadcasted_iota(jnp.int32, (CHUNK, CHUNK), 1) >= lax.broadcasted_iota(
        jnp.int32, (CHUNK, CHUNK), 0
    )

    def group(g, carry):
        ids = chunk_ids(g, per, ways)
        mixes, starts, keys, sides, state = [], [], [], [], []
        for c in ids:
            cum, gate = rates_of(rates_ref, c)
            gap = jnp.where(later, cum - column_form(cum), masked_score)
            mixes.append(jnp.exp(gap) * column_form(gate))
            starts.append(jnp.exp(cum))
            keys.append(k_ref[span(c, per), :])
            sides.append(
                jnp.concatenate([gram_ref[flat(c, per)], jnp.transpose(keys[-1])], axis=1)
            )
            q = jnp.transpose(q_ref[span(c, per), :]).astype(F32)
            state.append((jnp.zeros_like(q), q, q, jnp.sum(q * q, axis=0, keepdims=True)))
        for sweep_index in range(CG_ITERS):
            directions = [s[2].astype(BF16) for s in state]
            products = [dot(k, p) for k, p in zip(keys, directions)]
            images = [
                dot(
                    side,
                    jnp.concatenate(
                        [(start * p.astype(F32)).astype(BF16), (mix * b).astype(BF16)], axis=0
                    ),
                )
                for side, start, mix, p, b in zip(sides, starts, mixes, directions, products)
            ]
            for w, a in enumerate(images):
                x, r, _, rr = state[w]
                p = directions[w].astype(F32)
                a = a + ridge * p
                alpha = rr / (jnp.sum(p * a, axis=0, keepdims=True) + 1e-6)
                x = x + alpha * p
                r = r - alpha * a
                new = jnp.sum(r * r, axis=0, keepdims=True)
                state[w] = (x, r, r + (new / (rr + 1e-6)) * p, new)
        for c, s in zip(ids, state):
            x_ref[span(c, per), :] = jnp.transpose(s[0].astype(BF16))
        return carry

    lax.fori_loop(0, chunks // ways, group, 0)


def read_out(k_ref, v_ref, rates_ref, cross_ref, x_ref, out_ref, slab):
    per = rates_ref.shape[1] // 4
    for c in chunk_ids(slab, per, per):
        mix, start = mix_of(rates_ref, c)
        x = x_ref[span(c, per), :]
        products = dot(x, k_ref[span(c, per), :], NT)
        rows = start * dot(x, cross_ref[flat(c, per)])
        rows = rows + dot((mix * products).astype(BF16), v_ref[span(c, per), :])
        out_ref[span(c, per), :] = rows.astype(BF16)


REACH = 2
Q, K, V, MK, MQ, RATES, ATT, OUT, GRAM, CROSS = range(10)
QX, PART, LEVEL = (10, 12, 14)
KINDS = 16
BY_HEAD = (K, V, MK, MQ, GRAM, CROSS, QX + 1)


def push_order(heads):
    order = [(MK, 0), (Q, 0), (MQ, 0), (Q, 1), (K, 0), (V, 0)]
    for j in range(1, heads):
        order += [(MK, j), (MQ, j)]
        order += [(Q, 2)] if j == 1 and heads > 2 else []
        order += [(K, j), (V, j)]
        order += [(Q, j + 2)] if j + 2 < heads else []
    return order


def plane_kernel(n, g, *refs):
    ins, rates_in, ridge_in = refs[:5], refs[5], refs[6]
    results = refs[7:9]
    bufs, rates, homes = refs[9:14], refs[14], refs[15:17]
    later = (refs[9],) + refs[17:19]
    o_out, o_in = (None,) + refs[19:21], (None,) + refs[21:23]
    l_out, l_in = (None,) + refs[23:25], (None,) + refs[25:27]
    first_out, first_in = {GRAM: refs[27], CROSS: refs[28]}, {GRAM: refs[29], CROSS: refs[30]}
    decays, zero = refs[31:33]
    gram, cross, x = refs[33:36]
    o_own, l_own = refs[36:38]
    send, by_block, by_head, by_pair, at_end, own, own_end = refs[38:45]
    q, k, v, mk, mq = bufs
    att, out = homes
    rows, size = ins[0].shape[0], ridge_in.shape[1]
    per_device = rates.shape[0]
    planes = n // g
    group, me = lax.axis_index("groups"), lax.axis_index("seq")
    plane, place = me // g, lax.rem(me, g)

    def head_col(ref, j):
        return ref.at[:, pl.ds(pl.multiple_of(j * size, size), size)]

    def cell(ref, s, j):
        return ref.at[
            pl.ds(pl.multiple_of(s * rows, rows), rows),
            pl.ds(pl.multiple_of(j * size, size), size),
        ]

    def ends(a, j, source, target):
        if a in (Q, K, V, MK, MQ):
            return head_col(ins[a], target * per_device + j), cell(bufs[a], source, j)
        if a == RATES:
            return rates_in.at[pl.ds(target * per_device, per_device)], rates.at[:, source]
        return cell(homes[a - ATT], target, j), head_col(results[a - ATT], source * per_device + j)

    def arrival(a, j, i):
        if a in (Q, QX):
            return by_block.at[(Q, QX).index(a), j, i]
        if a in BY_HEAD:
            return by_head.at[BY_HEAD.index(a), j]
        if a >= PART:
            return by_pair.at[a - PART, j, i // 2]
        return at_end.at[a - RATES]

    def copy_to(src, dst, a, j, i, peer):
        return pltpu.make_async_remote_copy(
            src_ref=src,
            dst_ref=dst,
            send_sem=send.at[a],
            recv_sem=arrival(a, j, i),
            device_id=(group, peer),
            device_id_type=pl.DeviceIdType.MESH,
        )

    def bytes_of(ref, a, j=0, i=0):
        return copy_to(ref, ref, a, j, i, me)

    def home(e):
        return plane * g + e

    def remote(a, j, source, target, peer):
        src, dst = ends(a, j, source, target)
        return copy_to(src, dst, a, j, source, home(peer))

    def local(a, j):
        src, dst = ends(a, j, place, place)
        sem = own_end.at[a - RATES] if a in (RATES, ATT, OUT) else own.at[a, j]
        return pltpu.make_async_copy(src, dst, sem)

    def back(d, j, e):
        return copy_to(
            cell(later[d - 1], e, j), cell(later[d], e, j), QX + d - 1, j, e, me - g
        )

    def onward(a, d, j, i):
        if a == PART:
            src, dst = cell(o_out[d], i, j), cell(o_in[d], i, j)
        else:
            src, dst = l_out[d].at[j, i], l_in[d].at[j, i]
        return copy_to(src, dst, a + d - 1, j, i, me + g)

    def pass_on(d, j, i):
        onward(PART, d, j, i).start()
        onward(LEVEL, d, j, i).start()

    def take(d, j, t):
        @pl.when(has_previous)
        def _():
            both = pl.ds(pl.multiple_of(2 * t * rows, rows), 2 * rows)
            sums = head_col(o_in[d], j).at[both, :]
            bytes_of(sums, PART + d - 1, j, 2 * t).wait_recv()
            bytes_of(l_in[d].at[j, pl.ds(2 * t, 2)], LEVEL + d - 1, j, 2 * t).wait_recv()

    def state(a, j):
        return copy_to(first_out[a].at[j], first_in[a].at[j], a, j, 0, me + g)

    def loop(first, last, act):
        def one(t, carry):
            act(t)
            return carry

        lax.fori_loop(first, last, one, 0)

    def others(act):
        loop(1, g, lambda t: act(lax.rem(place + t, g)))

    def signal(peer):
        pl.semaphore_signal(
            barrier, inc=1, device_id=(group, peer), device_id_type=pl.DeviceIdType.MESH
        )

    def push(a, j):
        others(lambda e: remote(a, j, place, e, e).start())
        local(a, j).start()

    def arrive(a, j):
        if a == RATES:
            bytes_of(rates.at[:, : g - 1], a).wait_recv()
        else:
            bytes_of(head_col(bufs[a], j).at[: (g - 1) * rows, :], a, j).wait_recv()
        local(a, j).wait()

    def give(a, j, e):
        @pl.when(e != place)
        def _():
            remote(a, j, place, e, e).start()

        @pl.when(e == place)
        def _():
            local(a, j).start()

    def reaches(d):
        return plane + d < planes

    has_previous = plane > 0

    barrier = pltpu.get_barrier_semaphore()
    others(lambda e: signal(home(e)))

    @pl.when(has_previous)
    def _():
        signal(me - g)

    @pl.when(reaches(1))
    def _():
        signal(me + g)

    neighbours = has_previous.astype(jnp.int32) + reaches(1).astype(jnp.int32)
    pl.semaphore_wait(barrier, g - 1 + neighbours)

    push(RATES, 0)
    for a, j in push_order(per_device):
        push(a, j)

    @pl.when(jnp.logical_not(has_previous))
    def _():
        for d in range(1, REACH + 1):
            o_in[d][...] = jnp.zeros_like(o_in[d])
            l_in[d][...] = jnp.full_like(l_in[d], masked_score)
        for a in (GRAM, CROSS):
            first_in[a][...] = jnp.zeros_like(first_in[a])

    def near_first(act):
        loop(0, g, lambda t: act(place ^ t))

    def forward(j):
        def one(e):
            @pl.when(e == place)
            def _():
                local(Q, j).wait()

            @pl.when(e != place)
            def _():
                remote(Q, j, e, place, e).wait_recv()

            @pl.when(has_previous)
            def _():
                back(1, j, e).start()

        near_first(one)

    def relay(j):
        @pl.when(reaches(1))
        def _():
            def one(e):
                back(1, j, e).wait_recv()

                @pl.when(has_previous)
                def _():
                    back(2, j, e).start()

            near_first(one)

    arrive(RATES, 0)

    def head_totals(a, j, others_ref):
        return state_totals(
            head_col(mk, j), head_col(others_ref, j), rates.at[j], zero.at[a - GRAM, j]
        )

    def hand_on(a, j):
        @pl.when(has_previous)
        def _():
            state(a, j).wait_recv()

        @pl.when(reaches(1))
        def _():
            first = first_in[a][j].astype(F32)
            following = decays[pl.ds(j, 1), :] * first + zero[a - GRAM, j, zero.shape[2] - 1]
            first_out[a][j] = following.astype(BF16)
            state(a, j).start()

    def head_starts(a, j, starts_ref):
        state_starts(rates.at[j], zero.at[a - GRAM, j], first_in[a].at[j], starts_ref.at[j])

    def total_head(j):
        arrive(MK, j)
        decay = head_totals(GRAM, j, mk)
        decays[pl.ds(j, 1), :] = jnp.broadcast_to(decay, (1, size))

        @pl.when(jnp.logical_not(has_previous))
        def _():
            hand_on(GRAM, j)

    def step(s):
        first, middle, near, last = s, s - 1, s - 2, s - 3

        @pl.when(s == 0)
        def _():
            total_head(0)
            forward(0)

        @pl.when(first < per_device)
        def _():
            j = first

            @pl.when(has_previous)
            def _():
                hand_on(GRAM, j)

            head_starts(GRAM, j, gram)
            arrive(MQ, j)
            solve_all(
                head_col(mq, j), head_col(mk, j), rates.at[j],
                ridge_in[pl.ds(place * per_device + j, 1), :], gram.at[j], head_col(x, j),
            )

        @pl.when((last >= 0) & (plane == 1))
        def _():
            hand_on(CROSS, last)

        @pl.when((s < 2) & (s + 1 < per_device))
        def _():
            forward(s + 1)

        @pl.when((s == 1) & (s < per_device))
        def _():
            relay(1)

        @pl.when((middle >= 0) & (middle < per_device) & reaches(2))
        def _():
            j = middle
            bytes_of(head_col(later[2], j), QX + 1, j).wait_recv()
            attend_far(
                head_col(later[2], j), head_col(k, j), head_col(v, j),
                head_col(o_out[2], j), l_out[2].at[j], rows, lambda i: pass_on(2, j, i),
            )

        @pl.when(first < per_device)
        def _():
            j = first
            arrive(K, j)
            arrive(V, j)
            attend_own(
                head_col(q, j), head_col(k, j), head_col(v, j), head_col(o_own, j), l_own.at[j],
                rows,
            )

        @pl.when(s == 0)
        def _():
            relay(0)

        @pl.when((s > 0) & (s + 2 < per_device))
        def _():
            forward(s + 2)

        @pl.when((s > 0) & (s + 1 < per_device))
        def _():
            relay(s + 1)

        @pl.when(s + 1 < per_device)
        def _():
            total_head(s + 1)

        @pl.when((near >= 0) & (near < per_device))
        def _():
            j = near
            attend_last(
                head_col(o_own, j), l_own.at[j], head_col(o_in[1], j), l_in[1].at[j],
                head_col(att, j), rows, lambda i: take(1, j, i), lambda i: give(ATT, j, i),
            )
            head_totals(CROSS, j, att)

            @pl.when(jnp.logical_not(has_previous))
            def _():
                hand_on(CROSS, j)

        @pl.when((middle >= 0) & (middle < per_device) & reaches(1))
        def _():
            j = middle
            attend_middle(
                head_col(later[1], j), head_col(k, j), head_col(v, j),
                head_col(o_in[2], j), l_in[2].at[j],
                head_col(o_out[1], j), l_out[1].at[j], rows,
                lambda i: take(2, j, i), lambda i: pass_on(1, j, i),
            )

        @pl.when(last >= 0)
        def _():
            j = last

            @pl.when(plane > 1)
            def _():
                hand_on(CROSS, j)

            head_starts(CROSS, j, cross)

            def slab_out(i):
                read_out(
                    head_col(mk, j), head_col(att, j), rates.at[j], cross.at[j], head_col(x, j),
                    head_col(out, j), i,
                )
                give(OUT, j, i)

            loop(0, g, slab_out)

    loop(0, per_device + 3, step)

    def finish():
        for a in (ATT, OUT):
            result = results[a - ATT]
            bytes_of(result.at[:, : (g - 1) * per_device * size], a).wait_recv()
            part = result.at[:, : per_device * size]
            pltpu.make_async_copy(part, part, own_end.at[a - RATES]).wait()
            bytes_of(homes[a - ATT].at[: (g - 1) * rows, :], a).wait_send()
        for a in (Q, K, V, MK, MQ):
            bytes_of(bufs[a].at[: (g - 1) * rows, :], a).wait_send()
        bytes_of(rates.at[:, : g - 1], RATES).wait_send()

        @pl.when(has_previous)
        def _():
            bytes_of(later[0], QX).wait_send()

            @pl.when(reaches(1))
            def _():
                bytes_of(later[1], QX + 1).wait_send()

        for d in range(1, REACH + 1):

            @pl.when(reaches(d))
            def _(d=d):
                bytes_of(o_out[d], PART + d - 1).wait_send()
                bytes_of(l_out[d], LEVEL + d - 1).wait_send()

        @pl.when(reaches(1))
        def _():
            for a in (GRAM, CROSS):
                bytes_of(first_out[a], a).wait_send()

    finish()


def plane_body(
    attn_query, attn_key, attn_value, mesa_query, mesa_key, log_decay, input_gate, regularizer
):
    rows = attn_query.shape[0]
    heads, size = regularizer.shape
    devices = lax.axis_size("seq")
    g = WINDOW // (REACH * rows)
    per_device, tokens = heads // g, g * rows
    per, chunks = rows // CHUNK, tokens // CHUNK
    cum = jnp.cumsum(log_decay.reshape(per, CHUNK, heads), axis=1)
    rates = jnp.concatenate([cum, input_gate.reshape(per, CHUNK, heads)], axis=0)
    rates = jnp.pad(jnp.transpose(rates, (2, 0, 1)), ((0, 0), (0, 2 * per), (0, 0)))
    slab = jax.ShapeDtypeStruct((rows, heads * size), BF16)
    vmem = pl.BlockSpec(memory_space=pltpu.VMEM)
    anywhere = pl.BlockSpec(memory_space=pl.ANY)
    tall = pltpu.VMEM((tokens, per_device * size), BF16)
    levels = pltpu.VMEM((per_device, g, 1, rows), F32)
    first = pltpu.VMEM((per_device, size, size), BF16)
    states = pltpu.VMEM((per_device, chunks, size, size), BF16)
    return pl.pallas_call(
        functools.partial(plane_kernel, devices, g),
        out_shape=(slab, slab),
        in_specs=[anywhere] * 5 + [vmem] * 2,
        out_specs=(anywhere, anywhere),
        scratch_shapes=[tall] * 5
        + [pltpu.VMEM((per_device, g, 4 * per, CHUNK), F32)]
        + [tall] * (2 + REACH + 2 * REACH)
        + [levels] * (2 * REACH)
        + [first] * 4
        + [
            pltpu.VMEM((8, size), F32),
            pltpu.VMEM((2, per_device, chunks + 1, size, size), F32),
        ]
        + [states] * 2
        + [
            tall,
            pltpu.VMEM((tokens, per_device * size), F32),
            levels,
            pltpu.SemaphoreType.DMA((KINDS,)),
            pltpu.SemaphoreType.DMA((2, per_device, g)),
            pltpu.SemaphoreType.DMA((len(BY_HEAD), per_device)),
            pltpu.SemaphoreType.DMA((2 * REACH, per_device, g // 2)),
            pltpu.SemaphoreType.DMA((3,)),
            pltpu.SemaphoreType.DMA((5, per_device)),
            pltpu.SemaphoreType.DMA((3,)),
        ],
        compiler_params=pltpu.CompilerParams(
            collective_id=0, has_side_effects=True, vmem_limit_bytes=56 * 1024 * 1024
        ),
    )(attn_query, attn_key, attn_value, mesa_key, mesa_query, rates, regularizer)


def fits_planes(mesh, rows, heads, size):
    if WINDOW % (REACH * rows):
        return False
    g = WINDOW // (REACH * rows)
    return (
        size == CHUNK
        and g & (g - 1) == 0
        and mesh.shape["seq"] % g == 0
        and heads % g == 0
        and 2 <= heads // g <= 8
        and g % 2 == 0
        and rows % CHUNK == 0
        and WAYS % (rows // CHUNK) == 0
        and g * rows % (CHUNK * WAYS) == 0
    )


def solution(mesh):
    spec = P(("groups", "seq"), None)

    def body(*args):
        heads, size = args[7].shape
        fits = fits_planes(mesh, args[0].shape[0], heads, size)
        return (plane_body if fits else slab_body)(*args)

    return jax.shard_map(
        body,
        mesh=mesh,
        in_specs=(spec,) * 7 + (P(),),
        out_specs=(spec, spec),
        check_vma=False,
    )
```

```python
import jax
import jax.numpy as jnp
from jax import lax
from jax.experimental import pallas as pl
from jax.experimental.pallas import tpu as pltpu
from jax.sharding import PartitionSpec as P
import functools
import math

WINDOW = 2048
SPAN = 64
CG_ITERS = 8


exact_mode = lax.Precision.HIGHEST
masked_score = -1e30


def prefix(shard, axis, join, neutral):
    place = lax.axis_index(axis)
    gathered = jax.tree.map(
        lambda a, kind: lax.all_gather(a.astype(kind), axis), shard, (jnp.bfloat16, jnp.bfloat16)
    )
    state = jax.tree.map(lambda a, e: jnp.zeros_like(a) + jnp.asarray(e, a.dtype), shard, neutral)

    def one(lap, state):
        return join(
            state,
            jax.tree.map(
                lambda a, own: lax.dynamic_index_in_dim(a, lap, 0, False).astype(own.dtype),
                gathered,
                shard,
            ),
        )

    return lax.fori_loop(0, place, one, state)


def passed_along(value, axis, steps):
    count = lax.axis_size(axis)
    first, last = (max(0, -steps), min(count, count - steps))
    return lax.ppermute(value, axis, [(source, source + steps) for source in range(first, last)])


def span_update(states, inputs, ridge_diag):
    gram_start, cross_start = states
    queries, key_rows, value_rows, log_rates, gate_rows = inputs
    q_heads = jnp.transpose(queries, (1, 0, 2))
    k_heads = jnp.transpose(key_rows, (1, 0, 2))
    v_heads = jnp.transpose(value_rows, (1, 0, 2))
    cumulative = jnp.transpose(jnp.cumsum(log_rates, axis=0))
    length = cumulative.shape[1]
    causal = (jnp.arange(length)[:, None] >= jnp.arange(length)[None, :])[None]
    distance = cumulative[:, :, None] - cumulative[:, None, :]
    decay_mix = (
        jnp.where(causal, jnp.exp(jnp.where(causal, distance, 0.0)), 0.0)
        * jnp.transpose(gate_rows)[:, None, :]
    )
    start_scale = jnp.exp(cumulative)[:, :, None]
    iterate = jnp.zeros_like(q_heads)
    remain = q_heads
    search = q_heads
    norm_now = jnp.sum(remain * remain, axis=-1, keepdims=True)
    for sweep_index in range(CG_ITERS):
        carried = start_scale * jnp.einsum("hcd,hed->hce", search, gram_start, precision=exact_mode)
        operator_products = jnp.einsum("hjd,hid->hji", search, k_heads, precision=exact_mode)
        local_part = jnp.einsum(
            "hji,hid->hjd", decay_mix * operator_products, k_heads, precision=exact_mode
        )
        image_vec = carried + local_part + ridge_diag[:, None, :] * search
        step_size = norm_now / (jnp.sum(search * image_vec, axis=-1, keepdims=True) + 1e-06)
        iterate = iterate + step_size * search
        remain = remain - step_size * image_vec
        norm_next = jnp.sum(remain * remain, axis=-1, keepdims=True)
        search = remain + norm_next / (norm_now + 1e-06) * search
        norm_now = norm_next
    products = jnp.einsum("hjd,hid->hji", iterate, k_heads, precision=exact_mode)
    mesa_rows = start_scale * jnp.einsum("hje,hde->hjd", iterate, cross_start, precision=exact_mode)
    mesa_rows = mesa_rows + jnp.einsum(
        "hji,hid->hjd", decay_mix * products, v_heads, precision=exact_mode
    )
    tail_weight = (jnp.exp(cumulative[:, -1:] - cumulative) * jnp.transpose(gate_rows))[:, :, None]
    end_scale = jnp.exp(cumulative[:, -1])[:, None, None]
    gram_end = end_scale * gram_start + jnp.einsum(
        "hid,hie->hde", k_heads * tail_weight, k_heads, precision=exact_mode
    )
    cross_end = end_scale * cross_start + jnp.einsum(
        "hid,hie->hde", v_heads * tail_weight, k_heads, precision=exact_mode
    )
    return ((gram_end, cross_end), jnp.transpose(mesa_rows, (1, 0, 2)))


def mesa_pass(
    queries, key_rows, value_rows, log_rates, gate_rows, ridge_diag, gram_start, cross_start
):
    row_total = queries.shape[0]
    span_count = row_total // SPAN

    def shaped(array_in):
        return array_in.reshape((span_count, SPAN) + array_in.shape[1:])

    def advance(states, inputs):
        return span_update(states, inputs, ridge_diag)

    finished, outputs = lax.scan(
        advance,
        (gram_start, cross_start),
        (
            shaped(queries),
            shaped(key_rows),
            shaped(value_rows),
            shaped(log_rates),
            shaped(gate_rows),
        ),
    )
    return outputs.reshape(row_total, -1)


def fold_block(state_now, queries, key_value, query_first, key_first):
    running_max, running_sum, weighted = state_now
    row_count, head_count, head_size = queries.shape
    key_rows = key_value[0].reshape(-1, head_count, head_size)
    value_rows = key_value[1].reshape(-1, head_count, head_size)
    scores = jnp.einsum(
        "qhd,khd->hqk", queries, key_rows, preferred_element_type=jnp.float32
    ) * head_size ** (-0.5)
    query_pos = query_first + jnp.arange(row_count, dtype=jnp.int32)[:, None]
    key_pos = key_first + jnp.arange(key_rows.shape[0], dtype=jnp.int32)[None, :]
    distance = query_pos - key_pos
    inside = ((distance >= 0) & (distance < WINDOW) & (key_pos >= 0))[None]
    scores = jnp.where(inside, scores, masked_score)
    new_max = jnp.maximum(running_max, jnp.max(scores, axis=-1))
    weights = jnp.exp(scores - new_max[:, :, None]) * inside.astype(jnp.float32)
    rescale = jnp.exp(running_max - new_max)
    running_sum = running_sum * rescale + jnp.sum(weights, axis=-1)
    weighted = weighted * rescale[:, :, None] + jnp.einsum(
        "hqk,khd->hqd", weights.astype(jnp.bfloat16), value_rows, preferred_element_type=jnp.float32
    )
    return (new_max, running_sum, weighted)


def combine_pair(earlier, later):
    return (earlier[0] + later[0], jnp.exp(later[0])[:, None, None] * earlier[1] + later[1])


def slab_body(
    attn_query, attn_key, attn_value, mesa_query, mesa_key, log_decay, input_gate, regularizer
):
    row_count = attn_query.shape[0]
    head_count, head_size = regularizer.shape
    shape3 = (row_count, head_count, head_size)
    slab_first = lax.axis_index("seq") * row_count
    keys_float = mesa_key.astype(jnp.float32).reshape(shape3)
    slab_log = jnp.sum(log_decay, axis=0)
    tail_log = slab_log[None, :] - jnp.cumsum(log_decay, axis=0)
    weight_rows = (jnp.exp(tail_log) * input_gate)[:, :, None]
    gram_local = jnp.einsum(
        "lhd,lhe->hde", keys_float * weight_rows, keys_float, precision=exact_mode
    )
    zero_log = jnp.zeros_like(slab_log)
    zero_state = jnp.zeros_like(gram_local)
    gram_prefix = prefix((slab_log, gram_local), "seq", combine_pair, (zero_log, zero_state))[1]
    queries = attn_query.reshape(shape3)
    key_value = jnp.stack([attn_key, attn_value])
    state_now = (
        jnp.full((head_count, row_count), masked_score, jnp.float32),
        jnp.zeros((head_count, row_count), jnp.float32),
        jnp.zeros((head_count, row_count, head_size), jnp.float32),
    )
    state_now = fold_block(state_now, queries, key_value, slab_first, slab_first)
    reach = -(-WINDOW // row_count)
    moving = key_value
    for hop_index in range(1, reach + 1):
        moving = passed_along(moving, "seq", 1)
        state_now = fold_block(
            state_now, queries, moving, slab_first, slab_first - hop_index * row_count
        )
    normed = state_now[2] / state_now[1][:, :, None]
    attention = jnp.transpose(normed, (1, 0, 2)).reshape(row_count, -1).astype(jnp.bfloat16)
    values_float = attention.astype(jnp.float32).reshape(shape3)
    cross_local = jnp.einsum(
        "lhd,lhe->hde", values_float * weight_rows, keys_float, precision=exact_mode
    )
    cross_prefix = prefix((slab_log, cross_local), "seq", combine_pair, (zero_log, zero_state))[1]
    mesa_out = mesa_pass(
        mesa_query.astype(jnp.float32).reshape(shape3),
        keys_float,
        values_float,
        log_decay,
        input_gate,
        regularizer,
        gram_prefix,
        cross_prefix,
    )
    return (attention, mesa_out.astype(jnp.bfloat16))


CHUNK = 128
WAYS = 4
BF16 = jnp.bfloat16
F32 = jnp.float32
NT = (((1,), (1,)), ((), ()))


def dot(a, b, dims=None):
    if dims is None:
        return jnp.dot(a, b, preferred_element_type=F32)
    return lax.dot_general(a, b, dims, preferred_element_type=F32)


def score_blocks(queries, k_ref, base, count, rows, masks):
    scores, top = [], None
    for j in range(count):
        s = dot(queries, k_ref[pl.ds(base + j * rows, rows), :], NT)
        if masks[j] is not None:
            s = jnp.where(masks[j], s, masked_score)
        scores.append(s)
        top = s if top is None else jnp.maximum(top, s)
    return scores, jnp.max(top, axis=1, keepdims=True)


def weigh(scores, top, v_ref, base, rows, scale):
    total, weights = None, []
    for s in scores:
        w = jnp.exp2((s - top) * scale)
        total = w if total is None else total + w
        weights.append(w.astype(BF16))
    total = jnp.sum(total, axis=1, keepdims=True)
    summed = dot(
        jnp.concatenate(weights, axis=1), v_ref[pl.ds(base, len(scores) * rows), :]
    )
    return total, summed


def index_gap(rows):
    shape = (rows, rows)
    return lax.broadcasted_iota(jnp.int32, shape, 0) - lax.broadcasted_iota(jnp.int32, shape, 1)


def block_of(i, rows):
    if isinstance(i, int):
        return pl.ds(i * rows, rows)
    return pl.ds(pl.multiple_of(i * rows, rows), rows)


def partial(q_ref, k_ref, v_ref, i, base, masks, rows):
    scale = math.log2(math.e) / math.sqrt(q_ref.shape[1])
    queries = q_ref[block_of(i, rows), :]
    scores, top = score_blocks(queries, k_ref, base, len(masks), rows, masks)
    total, summed = weigh(scores, top, v_ref, base, rows, scale)
    return top * scale, total, summed


def columns(row, size):
    return jnp.transpose(jnp.broadcast_to(row, (size, row.shape[1])))


def joined(part, o_ref, l_ref, i, rows):
    level, total, summed = part
    earlier = columns(l_ref[i], summed.shape[1])
    peak = jnp.maximum(earlier, level)
    share_own, share_earlier = jnp.exp2(level - peak), jnp.exp2(earlier - peak)
    summed = summed * share_own + o_ref[block_of(i, rows), :].astype(F32) * share_earlier
    return peak, total * share_own + share_earlier, summed


def store_part(part, o_ref, l_ref, i, rows):
    level, total, summed = part
    o_ref[block_of(i, rows), :] = (summed / total).astype(o_ref.dtype)
    level = jnp.broadcast_to(level + jnp.log2(total), summed.shape)
    l_ref[i] = jnp.transpose(level)[:1, :]


def attend_far(q_ref, k_ref, v_ref, o_ref, l_ref, rows, done):
    blocks = k_ref.shape[0] // rows
    beyond = index_gap(rows) < 0
    for i in range(0, blocks, 2):
        for n in (i, i + 1):
            masks = [beyond] + [None] * (blocks - n - 1)
            part = partial(q_ref, k_ref, v_ref, n, n * rows, masks, rows)
            store_part(part, o_ref, l_ref, n, rows)
        done(i)
        done(i + 1)


def attend_middle(q_ref, k_ref, v_ref, o_in, l_in, o_ref, l_ref, rows, ready, done):
    blocks = k_ref.shape[0] // rows

    def two(t, carry):
        pair = (2 * t, 2 * t + 1)
        ready(t)
        for i in pair:
            part = partial(q_ref, k_ref, v_ref, i, 0, [None] * blocks, rows)
            store_part(joined(part, o_in, l_in, i, rows), o_ref, l_ref, i, rows)
        for i in pair:
            done(i)
        return carry

    lax.fori_loop(0, blocks // 2, two, 0)


def attend_own(q_ref, k_ref, v_ref, o_ref, l_ref, rows):
    causal = index_gap(rows) >= 0
    for i in range(k_ref.shape[0] // rows):
        part = partial(q_ref, k_ref, v_ref, i, 0, [None] * i + [causal], rows)
        store_part(part, o_ref, l_ref, i, rows)


def attend_last(o_own, l_own, o_in, l_in, out_ref, rows, ready, done):
    blocks = o_own.shape[0] // rows
    for i in range(0, blocks, 2):
        ready(i // 2)
        for n in (i, i + 1):
            own = (columns(l_own[n], o_own.shape[1]), 1.0, o_own[block_of(n, rows), :])
            level, total, summed = joined(own, o_in, l_in, n, rows)
            out_ref[block_of(n, rows), :] = (summed / total).astype(BF16)
        for n in (i, i + 1):
            done(n)


def flat(c, per):
    return c[0] * per + c[1]


def span(c, per):
    return pl.ds(pl.multiple_of(flat(c, per) * CHUNK, CHUNK), CHUNK)


def chunk_ids(g, per, ways=WAYS):
    slabs = ways // per
    return [(g * slabs + w // per, w % per) for w in range(ways)]


def column_form(row):
    return jnp.transpose(jnp.broadcast_to(row, (CHUNK, CHUNK)))


def rates_of(rates_ref, c):
    slab, place = c
    per = rates_ref.shape[1] // 4
    return rates_ref[slab, place : place + 1, :], rates_ref[slab, per + place : per + place + 1, :]


def tail_keys(turned_ref, rates_ref, c, per):
    cum, gate = rates_of(rates_ref, c)
    weight = jnp.exp(cum[:, CHUNK - 1 :] - cum) * gate
    return (turned_ref[flat(c, per)].astype(F32) * weight).astype(BF16), jnp.exp(cum[:, CHUNK - 1 :])


def mix_of(rates_ref, c):
    cum, gate = rates_of(rates_ref, c)
    col = column_form(cum)
    shape = (CHUNK, CHUNK)
    causal = lax.broadcasted_iota(jnp.int32, shape, 0) >= lax.broadcasted_iota(
        jnp.int32, shape, 1
    )
    mix = jnp.exp(jnp.where(causal, col - cum, masked_score)) * gate
    return mix, jnp.exp(col)


def turn_keys(k_ref, turned_ref):
    def one(c, carry):
        rows = pl.ds(pl.multiple_of(c * CHUNK, CHUNK), CHUNK)
        turned_ref[c] = jnp.transpose(k_ref[rows, :])
        return carry

    lax.fori_loop(0, turned_ref.shape[0], one, 0, unroll=4)


def state_totals(turned_ref, other_ref, rates_ref, zero_ref):
    per = rates_ref.shape[1] // 4
    chunks = rates_ref.shape[0] * per

    def step(g, carry):
        state, decay = carry
        for c in chunk_ids(g, per):
            zero_ref[flat(c, per)] = state
            keys, end = tail_keys(turned_ref, rates_ref, c, per)
            state = end * state + dot(keys, other_ref[span(c, per), :])
            decay = decay * end
        return state, decay

    state, decay = lax.fori_loop(
        0, chunks // WAYS, step, (jnp.zeros((CHUNK, CHUNK), F32), jnp.ones((1, 1), F32))
    )
    zero_ref[chunks] = state
    return decay


def state_starts(rates_ref, zero_ref, first_ref, starts_ref):
    per = rates_ref.shape[1] // 4
    chunks = rates_ref.shape[0] * per

    def step(g, first):
        for c in chunk_ids(g, per):
            starts_ref[flat(c, per)] = (zero_ref[flat(c, per)] + first).astype(BF16)
            cum, gate = rates_of(rates_ref, c)
            first = first * jnp.exp(cum[:, CHUNK - 1 :])
        return first

    lax.fori_loop(0, chunks // WAYS, step, first_ref[...].astype(F32))


def solve_all(q_ref, k_ref, turned_ref, rates_ref, ridge_ref, gram_ref, x_ref):
    per = rates_ref.shape[1] // 4
    chunks = rates_ref.shape[0] * per
    ways = math.gcd(chunks, 8)
    ridge = column_form(ridge_ref)
    later = lax.broadcasted_iota(jnp.int32, (CHUNK, CHUNK), 1) >= lax.broadcasted_iota(
        jnp.int32, (CHUNK, CHUNK), 0
    )

    def group(g, carry):
        ids = chunk_ids(g, per, ways)
        mixes, starts, keys, sides, state = [], [], [], [], []
        for c in ids:
            cum, gate = rates_of(rates_ref, c)
            gap = jnp.where(later, cum - column_form(cum), masked_score)
            mixes.append(jnp.exp(gap) * column_form(gate))
            starts.append(jnp.exp(cum))
            keys.append(k_ref[span(c, per), :])
            sides.append(
                jnp.concatenate([gram_ref[flat(c, per)], turned_ref[flat(c, per)]], axis=1)
            )
            q = jnp.transpose(q_ref[span(c, per), :]).astype(F32)
            state.append((jnp.zeros_like(q), q, q, jnp.sum(q * q, axis=0, keepdims=True)))
        for sweep_index in range(CG_ITERS):
            directions = [s[2].astype(BF16) for s in state]
            products = [dot(k, p) for k, p in zip(keys, directions)]
            images = [
                dot(
                    side,
                    jnp.concatenate(
                        [(start * p.astype(F32)).astype(BF16), (mix * b).astype(BF16)], axis=0
                    ),
                )
                for side, start, mix, p, b in zip(sides, starts, mixes, directions, products)
            ]
            for w, a in enumerate(images):
                x, r, _, rr = state[w]
                p = directions[w].astype(F32)
                a = a + ridge * p
                alpha = rr / (jnp.sum(p * a, axis=0, keepdims=True) + 1e-6)
                x = x + alpha * p
                r = r - alpha * a
                new = jnp.sum(r * r, axis=0, keepdims=True)
                state[w] = (x, r, r + (new / (rr + 1e-6)) * p, new)
        for c, s in zip(ids, state):
            x_ref[span(c, per), :] = jnp.transpose(s[0].astype(BF16))
        return carry

    lax.fori_loop(0, chunks // ways, group, 0)


def read_out(k_ref, v_ref, rates_ref, cross_ref, x_ref, out_ref, slab):
    per = rates_ref.shape[1] // 4
    for c in chunk_ids(slab, per, per):
        mix, start = mix_of(rates_ref, c)
        x = x_ref[span(c, per), :]
        products = dot(x, k_ref[span(c, per), :], NT)
        rows = start * dot(x, cross_ref[flat(c, per)])
        rows = rows + dot((mix * products).astype(BF16), v_ref[span(c, per), :])
        out_ref[span(c, per), :] = rows.astype(BF16)


REACH = 2
Q, K, V, MK, MQ, RATES, ATT, OUT, GRAM, CROSS = range(10)
QX, PART, LEVEL = (10, 12, 14)
KINDS = 16
BY_HEAD = (K, V, MK, MQ, GRAM, CROSS, QX + 1)


def push_order(heads):
    order = [(MK, 0), (Q, 0), (MQ, 0), (Q, 1), (K, 0), (V, 0)]
    for j in range(1, heads):
        order += [(MK, j), (MQ, j)]
        order += [(Q, 2)] if j == 1 and heads > 2 else []
        order += [(K, j), (V, j)]
        order += [(Q, j + 2)] if j + 2 < heads else []
    return order


def plane_kernel(n, g, *refs):
    ins, rates_in, ridge_in = refs[:5], refs[5], refs[6]
    results = refs[7:9]
    bufs, rates, homes = refs[9:14], refs[14], refs[15:17]
    later = (refs[9],) + refs[17:19]
    o_out, o_in = (None,) + refs[19:21], (None,) + refs[21:23]
    l_out, l_in = (None,) + refs[23:25], (None,) + refs[25:27]
    first_out, first_in = {GRAM: refs[27], CROSS: refs[28]}, {GRAM: refs[29], CROSS: refs[30]}
    decays, zero = refs[31:33]
    gram, cross, turned, x = refs[33:37]
    o_own, l_own = refs[37:39]
    send, by_block, by_head, by_pair, at_end, own, own_end = refs[39:46]
    q, k, v, mk, mq = bufs
    att, out = homes
    rows, size = ins[0].shape[0], ridge_in.shape[1]
    per_device = rates.shape[0]
    planes = n // g
    group, me = lax.axis_index("groups"), lax.axis_index("seq")
    plane, place = me // g, lax.rem(me, g)

    def head_col(ref, j):
        return ref.at[:, pl.ds(pl.multiple_of(j * size, size), size)]

    def cell(ref, s, j):
        return ref.at[
            pl.ds(pl.multiple_of(s * rows, rows), rows),
            pl.ds(pl.multiple_of(j * size, size), size),
        ]

    def ends(a, j, source, target):
        if a in (Q, K, V, MK, MQ):
            return head_col(ins[a], target * per_device + j), cell(bufs[a], source, j)
        if a == RATES:
            return rates_in.at[pl.ds(target * per_device, per_device)], rates.at[:, source]
        return cell(homes[a - ATT], target, j), head_col(results[a - ATT], source * per_device + j)

    def arrival(a, j, i):
        if a in (Q, QX):
            return by_block.at[(Q, QX).index(a), j, i]
        if a in BY_HEAD:
            return by_head.at[BY_HEAD.index(a), j]
        if a >= PART:
            return by_pair.at[a - PART, j, i // 2]
        return at_end.at[a - RATES]

    def copy_to(src, dst, a, j, i, peer):
        return pltpu.make_async_remote_copy(
            src_ref=src,
            dst_ref=dst,
            send_sem=send.at[a],
            recv_sem=arrival(a, j, i),
            device_id=(group, peer),
            device_id_type=pl.DeviceIdType.MESH,
        )

    def bytes_of(ref, a, j=0, i=0):
        return copy_to(ref, ref, a, j, i, me)

    def home(e):
        return plane * g + e

    def remote(a, j, source, target, peer):
        src, dst = ends(a, j, source, target)
        return copy_to(src, dst, a, j, source, home(peer))

    def local(a, j):
        src, dst = ends(a, j, place, place)
        sem = own_end.at[a - RATES] if a in (RATES, ATT, OUT) else own.at[a, j]
        return pltpu.make_async_copy(src, dst, sem)

    def back(d, j, e):
        return copy_to(
            cell(later[d - 1], e, j), cell(later[d], e, j), QX + d - 1, j, e, me - g
        )

    def onward(a, d, j, i):
        if a == PART:
            src, dst = cell(o_out[d], i, j), cell(o_in[d], i, j)
        else:
            src, dst = l_out[d].at[j, i], l_in[d].at[j, i]
        return copy_to(src, dst, a + d - 1, j, i, me + g)

    def pass_on(d, j, i):
        onward(PART, d, j, i).start()
        onward(LEVEL, d, j, i).start()

    def take(d, j, t):
        @pl.when(has_previous)
        def _():
            both = pl.ds(pl.multiple_of(2 * t * rows, rows), 2 * rows)
            sums = head_col(o_in[d], j).at[both, :]
            bytes_of(sums, PART + d - 1, j, 2 * t).wait_recv()
            bytes_of(l_in[d].at[j, pl.ds(2 * t, 2)], LEVEL + d - 1, j, 2 * t).wait_recv()

    def state(a, j):
        return copy_to(first_out[a].at[j], first_in[a].at[j], a, j, 0, me + g)

    def loop(first, last, act):
        def one(t, carry):
            act(t)
            return carry

        lax.fori_loop(first, last, one, 0)

    def others(act):
        loop(1, g, lambda t: act(lax.rem(place + t, g)))

    def signal(peer):
        pl.semaphore_signal(
            barrier, inc=1, device_id=(group, peer), device_id_type=pl.DeviceIdType.MESH
        )

    def push(a, j):
        others(lambda e: remote(a, j, place, e, e).start())
        local(a, j).start()

    def arrive(a, j):
        if a == RATES:
            bytes_of(rates.at[:, : g - 1], a).wait_recv()
        else:
            bytes_of(head_col(bufs[a], j).at[: (g - 1) * rows, :], a, j).wait_recv()
        local(a, j).wait()

    def give(a, j, e):
        @pl.when(e != place)
        def _():
            remote(a, j, place, e, e).start()

        @pl.when(e == place)
        def _():
            local(a, j).start()

    def reaches(d):
        return plane + d < planes

    has_previous = plane > 0

    barrier = pltpu.get_barrier_semaphore()
    others(lambda e: signal(home(e)))

    @pl.when(has_previous)
    def _():
        signal(me - g)

    @pl.when(reaches(1))
    def _():
        signal(me + g)

    neighbours = has_previous.astype(jnp.int32) + reaches(1).astype(jnp.int32)
    pl.semaphore_wait(barrier, g - 1 + neighbours)

    push(RATES, 0)
    for a, j in push_order(per_device):
        push(a, j)

    @pl.when(jnp.logical_not(has_previous))
    def _():
        for d in range(1, REACH + 1):
            o_in[d][...] = jnp.zeros_like(o_in[d])
            l_in[d][...] = jnp.full_like(l_in[d], masked_score)
        for a in (GRAM, CROSS):
            first_in[a][...] = jnp.zeros_like(first_in[a])

    def near_first(act):
        loop(0, g, lambda t: act(place ^ t))

    def forward(j):
        def one(e):
            @pl.when(e == place)
            def _():
                local(Q, j).wait()

            @pl.when(e != place)
            def _():
                remote(Q, j, e, place, e).wait_recv()

            @pl.when(has_previous)
            def _():
                back(1, j, e).start()

        near_first(one)

    def relay(j):
        @pl.when(reaches(1))
        def _():
            def one(e):
                back(1, j, e).wait_recv()

                @pl.when(has_previous)
                def _():
                    back(2, j, e).start()

            near_first(one)

    arrive(RATES, 0)

    def head_totals(a, j, others_ref):
        return state_totals(
            turned.at[j], head_col(others_ref, j), rates.at[j], zero.at[a - GRAM, j]
        )

    def hand_on(a, j):
        @pl.when(has_previous)
        def _():
            state(a, j).wait_recv()

        @pl.when(reaches(1))
        def _():
            first = first_in[a][j].astype(F32)
            following = decays[pl.ds(j, 1), :] * first + zero[a - GRAM, j, zero.shape[2] - 1]
            first_out[a][j] = following.astype(BF16)
            state(a, j).start()

    def head_starts(a, j, starts_ref):
        state_starts(rates.at[j], zero.at[a - GRAM, j], first_in[a].at[j], starts_ref.at[j])

    def total_head(j):
        arrive(MK, j)
        turn_keys(head_col(mk, j), turned.at[j])
        decay = head_totals(GRAM, j, mk)
        decays[pl.ds(j, 1), :] = jnp.broadcast_to(decay, (1, size))

        @pl.when(jnp.logical_not(has_previous))
        def _():
            hand_on(GRAM, j)

    def far_head(j):
        bytes_of(head_col(later[2], j), QX + 1, j).wait_recv()
        attend_far(
            head_col(later[2], j), head_col(k, j), head_col(v, j),
            head_col(o_out[2], j), l_out[2].at[j], rows, lambda i: pass_on(2, j, i),
        )

    def merge_head(j):
        attend_last(
            head_col(o_own, j), l_own.at[j], head_col(o_in[1], j), l_in[1].at[j],
            head_col(att, j), rows, lambda i: take(1, j, i), lambda i: give(ATT, j, i),
        )
        head_totals(CROSS, j, att)

        @pl.when(jnp.logical_not(has_previous))
        def _():
            hand_on(CROSS, j)

    def step(s):
        first, middle, near, last = s, s - 1, s - 2, s - 3

        @pl.when(s == 0)
        def _():
            total_head(0)
            forward(0)

        @pl.when(first < per_device)
        def _():
            j = first

            @pl.when(has_previous)
            def _():
                hand_on(GRAM, j)

            head_starts(GRAM, j, gram)
            arrive(MQ, j)
            solve_all(
                head_col(mq, j), head_col(mk, j), turned.at[j], rates.at[j],
                ridge_in[pl.ds(place * per_device + j, 1), :], gram.at[j], head_col(x, j),
            )

        @pl.when((last >= 0) & (plane == 1))
        def _():
            hand_on(CROSS, last)

        @pl.when((s < 2) & (s + 1 < per_device))
        def _():
            forward(s + 1)

        @pl.when((s == 1) & (s < per_device))
        def _():
            relay(1)

        @pl.when((middle >= 0) & (middle < per_device - 1) & reaches(2))
        def _():
            far_head(middle)

        @pl.when(first < per_device)
        def _():
            j = first
            arrive(K, j)
            arrive(V, j)
            attend_own(
                head_col(q, j), head_col(k, j), head_col(v, j), head_col(o_own, j), l_own.at[j],
                rows,
            )

        @pl.when(s == 0)
        def _():
            relay(0)

        @pl.when((s > 0) & (s + 2 < per_device))
        def _():
            forward(s + 2)

        @pl.when((s > 0) & (s + 1 < per_device))
        def _():
            relay(s + 1)

        @pl.when(s + 1 < per_device)
        def _():
            total_head(s + 1)

        @pl.when((first == per_device - 1) & reaches(2))
        def _():
            far_head(first)

        @pl.when((near >= 0) & (near < per_device) & (plane == 0))
        def _():
            merge_head(near)

        @pl.when((middle >= 0) & (middle < per_device) & reaches(1))
        def _():
            j = middle
            attend_middle(
                head_col(later[1], j), head_col(k, j), head_col(v, j),
                head_col(o_in[2], j), l_in[2].at[j],
                head_col(o_out[1], j), l_out[1].at[j], rows,
                lambda i: take(2, j, i), lambda i: pass_on(1, j, i),
            )

        @pl.when((near >= 0) & (near < per_device) & has_previous)
        def _():
            merge_head(near)

        @pl.when(last >= 0)
        def _():
            j = last

            @pl.when(plane > 1)
            def _():
                hand_on(CROSS, j)

            head_starts(CROSS, j, cross)

            def slab_out(i):
                read_out(
                    head_col(mk, j), head_col(att, j), rates.at[j], cross.at[j], head_col(x, j),
                    head_col(out, j), i,
                )
                give(OUT, j, i)

            loop(0, g, slab_out)

    loop(0, per_device + 3, step)

    def finish():
        for a in (ATT, OUT):
            result = results[a - ATT]
            bytes_of(result.at[:, : (g - 1) * per_device * size], a).wait_recv()
            part = result.at[:, : per_device * size]
            pltpu.make_async_copy(part, part, own_end.at[a - RATES]).wait()
            bytes_of(homes[a - ATT].at[: (g - 1) * rows, :], a).wait_send()
        for a in (Q, K, V, MK, MQ):
            bytes_of(bufs[a].at[: (g - 1) * rows, :], a).wait_send()
        bytes_of(rates.at[:, : g - 1], RATES).wait_send()

        @pl.when(has_previous)
        def _():
            bytes_of(later[0], QX).wait_send()

            @pl.when(reaches(1))
            def _():
                bytes_of(later[1], QX + 1).wait_send()

        for d in range(1, REACH + 1):

            @pl.when(reaches(d))
            def _(d=d):
                bytes_of(o_out[d], PART + d - 1).wait_send()
                bytes_of(l_out[d], LEVEL + d - 1).wait_send()

        @pl.when(reaches(1))
        def _():
            for a in (GRAM, CROSS):
                bytes_of(first_out[a], a).wait_send()

    finish()


def plane_body(
    attn_query, attn_key, attn_value, mesa_query, mesa_key, log_decay, input_gate, regularizer
):
    rows = attn_query.shape[0]
    heads, size = regularizer.shape
    devices = lax.axis_size("seq")
    g = WINDOW // (REACH * rows)
    per_device, tokens = heads // g, g * rows
    per, chunks = rows // CHUNK, tokens // CHUNK
    cum = jnp.cumsum(log_decay.reshape(per, CHUNK, heads), axis=1)
    rates = jnp.concatenate([cum, input_gate.reshape(per, CHUNK, heads)], axis=0)
    rates = jnp.pad(jnp.transpose(rates, (2, 0, 1)), ((0, 0), (0, 2 * per), (0, 0)))
    slab = jax.ShapeDtypeStruct((rows, heads * size), BF16)
    vmem = pl.BlockSpec(memory_space=pltpu.VMEM)
    anywhere = pl.BlockSpec(memory_space=pl.ANY)
    tall = pltpu.VMEM((tokens, per_device * size), BF16)
    levels = pltpu.VMEM((per_device, g, 1, rows), F32)
    first = pltpu.VMEM((per_device, size, size), BF16)
    states = pltpu.VMEM((per_device, chunks, size, size), BF16)
    return pl.pallas_call(
        functools.partial(plane_kernel, devices, g),
        out_shape=(slab, slab),
        in_specs=[anywhere] * 5 + [vmem] * 2,
        out_specs=(anywhere, anywhere),
        scratch_shapes=[tall] * 5
        + [pltpu.VMEM((per_device, g, 4 * per, CHUNK), F32)]
        + [tall] * (2 + REACH + 2 * REACH)
        + [levels] * (2 * REACH)
        + [first] * 4
        + [
            pltpu.VMEM((8, size), F32),
            pltpu.VMEM((2, per_device, chunks + 1, size, size), F32),
        ]
        + [states] * 3
        + [
            tall,
            pltpu.VMEM((tokens, per_device * size), F32),
            levels,
            pltpu.SemaphoreType.DMA((KINDS,)),
            pltpu.SemaphoreType.DMA((2, per_device, g)),
            pltpu.SemaphoreType.DMA((len(BY_HEAD), per_device)),
            pltpu.SemaphoreType.DMA((2 * REACH, per_device, g // 2)),
            pltpu.SemaphoreType.DMA((3,)),
            pltpu.SemaphoreType.DMA((5, per_device)),
            pltpu.SemaphoreType.DMA((3,)),
        ],
        compiler_params=pltpu.CompilerParams(
            collective_id=0, has_side_effects=True, vmem_limit_bytes=56 * 1024 * 1024
        ),
    )(attn_query, attn_key, attn_value, mesa_key, mesa_query, rates, regularizer)


def fits_planes(mesh, rows, heads, size):
    if WINDOW % (REACH * rows):
        return False
    g = WINDOW // (REACH * rows)
    return (
        size == CHUNK
        and g & (g - 1) == 0
        and mesh.shape["seq"] % g == 0
        and heads % g == 0
        and 2 <= heads // g <= 8
        and g % 2 == 0
        and rows % CHUNK == 0
        and WAYS % (rows // CHUNK) == 0
        and g * rows % (CHUNK * WAYS) == 0
    )


def solution(mesh):
    spec = P(("groups", "seq"), None)

    def body(*args):
        heads, size = args[7].shape
        fits = fits_planes(mesh, args[0].shape[0], heads, size)
        return (plane_body if fits else slab_body)(*args)

    return jax.shard_map(
        body,
        mesh=mesh,
        in_specs=(spec,) * 7 + (P(),),
        out_specs=(spec, spec),
        check_vma=False,
    )
```

```python
import jax
import jax.numpy as jnp
from jax import lax
from jax.experimental import pallas as pl
from jax.experimental.pallas import tpu as pltpu
from jax.sharding import PartitionSpec as P
import functools
import math

WINDOW = 2048
SPAN = 64
CG_ITERS = 8


exact_mode = lax.Precision.HIGHEST
masked_score = -1e30


def prefix(shard, axis, join, neutral):
    place = lax.axis_index(axis)
    gathered = jax.tree.map(
        lambda a, kind: lax.all_gather(a.astype(kind), axis), shard, (jnp.bfloat16, jnp.bfloat16)
    )
    state = jax.tree.map(lambda a, e: jnp.zeros_like(a) + jnp.asarray(e, a.dtype), shard, neutral)

    def one(lap, state):
        return join(
            state,
            jax.tree.map(
                lambda a, own: lax.dynamic_index_in_dim(a, lap, 0, False).astype(own.dtype),
                gathered,
                shard,
            ),
        )

    return lax.fori_loop(0, place, one, state)


def passed_along(value, axis, steps):
    count = lax.axis_size(axis)
    first, last = (max(0, -steps), min(count, count - steps))
    return lax.ppermute(value, axis, [(source, source + steps) for source in range(first, last)])


def span_update(states, inputs, ridge_diag):
    gram_start, cross_start = states
    queries, key_rows, value_rows, log_rates, gate_rows = inputs
    q_heads = jnp.transpose(queries, (1, 0, 2))
    k_heads = jnp.transpose(key_rows, (1, 0, 2))
    v_heads = jnp.transpose(value_rows, (1, 0, 2))
    cumulative = jnp.transpose(jnp.cumsum(log_rates, axis=0))
    length = cumulative.shape[1]
    causal = (jnp.arange(length)[:, None] >= jnp.arange(length)[None, :])[None]
    distance = cumulative[:, :, None] - cumulative[:, None, :]
    decay_mix = (
        jnp.where(causal, jnp.exp(jnp.where(causal, distance, 0.0)), 0.0)
        * jnp.transpose(gate_rows)[:, None, :]
    )
    start_scale = jnp.exp(cumulative)[:, :, None]
    iterate = jnp.zeros_like(q_heads)
    remain = q_heads
    search = q_heads
    norm_now = jnp.sum(remain * remain, axis=-1, keepdims=True)
    for sweep_index in range(CG_ITERS):
        carried = start_scale * jnp.einsum("hcd,hed->hce", search, gram_start, precision=exact_mode)
        operator_products = jnp.einsum("hjd,hid->hji", search, k_heads, precision=exact_mode)
        local_part = jnp.einsum(
            "hji,hid->hjd", decay_mix * operator_products, k_heads, precision=exact_mode
        )
        image_vec = carried + local_part + ridge_diag[:, None, :] * search
        step_size = norm_now / (jnp.sum(search * image_vec, axis=-1, keepdims=True) + 1e-06)
        iterate = iterate + step_size * search
        remain = remain - step_size * image_vec
        norm_next = jnp.sum(remain * remain, axis=-1, keepdims=True)
        search = remain + norm_next / (norm_now + 1e-06) * search
        norm_now = norm_next
    products = jnp.einsum("hjd,hid->hji", iterate, k_heads, precision=exact_mode)
    mesa_rows = start_scale * jnp.einsum("hje,hde->hjd", iterate, cross_start, precision=exact_mode)
    mesa_rows = mesa_rows + jnp.einsum(
        "hji,hid->hjd", decay_mix * products, v_heads, precision=exact_mode
    )
    tail_weight = (jnp.exp(cumulative[:, -1:] - cumulative) * jnp.transpose(gate_rows))[:, :, None]
    end_scale = jnp.exp(cumulative[:, -1])[:, None, None]
    gram_end = end_scale * gram_start + jnp.einsum(
        "hid,hie->hde", k_heads * tail_weight, k_heads, precision=exact_mode
    )
    cross_end = end_scale * cross_start + jnp.einsum(
        "hid,hie->hde", v_heads * tail_weight, k_heads, precision=exact_mode
    )
    return ((gram_end, cross_end), jnp.transpose(mesa_rows, (1, 0, 2)))


def mesa_pass(
    queries, key_rows, value_rows, log_rates, gate_rows, ridge_diag, gram_start, cross_start
):
    row_total = queries.shape[0]
    span_count = row_total // SPAN

    def shaped(array_in):
        return array_in.reshape((span_count, SPAN) + array_in.shape[1:])

    def advance(states, inputs):
        return span_update(states, inputs, ridge_diag)

    finished, outputs = lax.scan(
        advance,
        (gram_start, cross_start),
        (
            shaped(queries),
            shaped(key_rows),
            shaped(value_rows),
            shaped(log_rates),
            shaped(gate_rows),
        ),
    )
    return outputs.reshape(row_total, -1)


def fold_block(state_now, queries, key_value, query_first, key_first):
    running_max, running_sum, weighted = state_now
    row_count, head_count, head_size = queries.shape
    key_rows = key_value[0].reshape(-1, head_count, head_size)
    value_rows = key_value[1].reshape(-1, head_count, head_size)
    scores = jnp.einsum(
        "qhd,khd->hqk", queries, key_rows, preferred_element_type=jnp.float32
    ) * head_size ** (-0.5)
    query_pos = query_first + jnp.arange(row_count, dtype=jnp.int32)[:, None]
    key_pos = key_first + jnp.arange(key_rows.shape[0], dtype=jnp.int32)[None, :]
    distance = query_pos - key_pos
    inside = ((distance >= 0) & (distance < WINDOW) & (key_pos >= 0))[None]
    scores = jnp.where(inside, scores, masked_score)
    new_max = jnp.maximum(running_max, jnp.max(scores, axis=-1))
    weights = jnp.exp(scores - new_max[:, :, None]) * inside.astype(jnp.float32)
    rescale = jnp.exp(running_max - new_max)
    running_sum = running_sum * rescale + jnp.sum(weights, axis=-1)
    weighted = weighted * rescale[:, :, None] + jnp.einsum(
        "hqk,khd->hqd", weights.astype(jnp.bfloat16), value_rows, preferred_element_type=jnp.float32
    )
    return (new_max, running_sum, weighted)


def combine_pair(earlier, later):
    return (earlier[0] + later[0], jnp.exp(later[0])[:, None, None] * earlier[1] + later[1])


def slab_body(
    attn_query, attn_key, attn_value, mesa_query, mesa_key, log_decay, input_gate, regularizer
):
    row_count = attn_query.shape[0]
    head_count, head_size = regularizer.shape
    shape3 = (row_count, head_count, head_size)
    slab_first = lax.axis_index("seq") * row_count
    keys_float = mesa_key.astype(jnp.float32).reshape(shape3)
    slab_log = jnp.sum(log_decay, axis=0)
    tail_log = slab_log[None, :] - jnp.cumsum(log_decay, axis=0)
    weight_rows = (jnp.exp(tail_log) * input_gate)[:, :, None]
    gram_local = jnp.einsum(
        "lhd,lhe->hde", keys_float * weight_rows, keys_float, precision=exact_mode
    )
    zero_log = jnp.zeros_like(slab_log)
    zero_state = jnp.zeros_like(gram_local)
    gram_prefix = prefix((slab_log, gram_local), "seq", combine_pair, (zero_log, zero_state))[1]
    queries = attn_query.reshape(shape3)
    key_value = jnp.stack([attn_key, attn_value])
    state_now = (
        jnp.full((head_count, row_count), masked_score, jnp.float32),
        jnp.zeros((head_count, row_count), jnp.float32),
        jnp.zeros((head_count, row_count, head_size), jnp.float32),
    )
    state_now = fold_block(state_now, queries, key_value, slab_first, slab_first)
    reach = -(-WINDOW // row_count)
    moving = key_value
    for hop_index in range(1, reach + 1):
        moving = passed_along(moving, "seq", 1)
        state_now = fold_block(
            state_now, queries, moving, slab_first, slab_first - hop_index * row_count
        )
    normed = state_now[2] / state_now[1][:, :, None]
    attention = jnp.transpose(normed, (1, 0, 2)).reshape(row_count, -1).astype(jnp.bfloat16)
    values_float = attention.astype(jnp.float32).reshape(shape3)
    cross_local = jnp.einsum(
        "lhd,lhe->hde", values_float * weight_rows, keys_float, precision=exact_mode
    )
    cross_prefix = prefix((slab_log, cross_local), "seq", combine_pair, (zero_log, zero_state))[1]
    mesa_out = mesa_pass(
        mesa_query.astype(jnp.float32).reshape(shape3),
        keys_float,
        values_float,
        log_decay,
        input_gate,
        regularizer,
        gram_prefix,
        cross_prefix,
    )
    return (attention, mesa_out.astype(jnp.bfloat16))


CHUNK = 128
WAYS = 4
BF16 = jnp.bfloat16
F32 = jnp.float32
NT = (((1,), (1,)), ((), ()))


def dot(a, b, dims=None):
    if dims is None:
        return jnp.dot(a, b, preferred_element_type=F32)
    return lax.dot_general(a, b, dims, preferred_element_type=F32)


def score_blocks(queries, k_ref, base, count, rows, masks):
    scores, top = [], None
    for j in range(count):
        s = dot(queries, k_ref[pl.ds(base + j * rows, rows), :], NT)
        if masks[j] is not None:
            s = jnp.where(masks[j], s, masked_score)
        scores.append(s)
        top = s if top is None else jnp.maximum(top, s)
    return scores, jnp.max(top, axis=1, keepdims=True)


def weigh(scores, top, v_ref, base, rows, scale):
    total, weights = None, []
    for s in scores:
        w = jnp.exp2((s - top) * scale)
        total = w if total is None else total + w
        weights.append(w.astype(BF16))
    total = jnp.sum(total, axis=1, keepdims=True)
    summed = dot(
        jnp.concatenate(weights, axis=1), v_ref[pl.ds(base, len(scores) * rows), :]
    )
    return total, summed


def index_gap(rows):
    shape = (rows, rows)
    return lax.broadcasted_iota(jnp.int32, shape, 0) - lax.broadcasted_iota(jnp.int32, shape, 1)


def block_of(i, rows):
    if isinstance(i, int):
        return pl.ds(i * rows, rows)
    return pl.ds(pl.multiple_of(i * rows, rows), rows)


def partial(q_ref, k_ref, v_ref, i, base, masks, rows):
    scale = math.log2(math.e) / math.sqrt(q_ref.shape[1])
    queries = q_ref[block_of(i, rows), :]
    scores, top = score_blocks(queries, k_ref, base, len(masks), rows, masks)
    total, summed = weigh(scores, top, v_ref, base, rows, scale)
    return top * scale, total, summed


def columns(row, size):
    return jnp.transpose(jnp.broadcast_to(row, (size, row.shape[1])))


def joined(part, o_ref, l_ref, i, rows):
    level, total, summed = part
    earlier = columns(l_ref[i], summed.shape[1])
    peak = jnp.maximum(earlier, level)
    share_own, share_earlier = jnp.exp2(level - peak), jnp.exp2(earlier - peak)
    summed = summed * share_own + o_ref[block_of(i, rows), :].astype(F32) * share_earlier
    return peak, total * share_own + share_earlier, summed


def store_part(part, o_ref, l_ref, i, rows):
    level, total, summed = part
    o_ref[block_of(i, rows), :] = (summed / total).astype(o_ref.dtype)
    level = jnp.broadcast_to(level + jnp.log2(total), summed.shape)
    l_ref[i] = jnp.transpose(level)[:1, :]


def attend_far(q_ref, k_ref, v_ref, o_ref, l_ref, rows, done):
    blocks = k_ref.shape[0] // rows
    beyond = index_gap(rows) < 0
    for i in range(0, blocks, 2):
        for n in (i, i + 1):
            masks = [beyond] + [None] * (blocks - n - 1)
            part = partial(q_ref, k_ref, v_ref, n, n * rows, masks, rows)
            store_part(part, o_ref, l_ref, n, rows)
        done(i)
        done(i + 1)


def attend_middle(q_ref, k_ref, v_ref, o_in, l_in, o_ref, l_ref, rows, ready, done):
    blocks = k_ref.shape[0] // rows

    def two(t, carry):
        pair = (2 * t, 2 * t + 1)
        ready(t)
        for i in pair:
            part = partial(q_ref, k_ref, v_ref, i, 0, [None] * blocks, rows)
            store_part(joined(part, o_in, l_in, i, rows), o_ref, l_ref, i, rows)
        for i in pair:
            done(i)
        return carry

    lax.fori_loop(0, blocks // 2, two, 0)


def attend_own(q_ref, k_ref, v_ref, o_ref, l_ref, rows):
    causal = index_gap(rows) >= 0
    for i in range(k_ref.shape[0] // rows):
        part = partial(q_ref, k_ref, v_ref, i, 0, [None] * i + [causal], rows)
        store_part(part, o_ref, l_ref, i, rows)


def attend_last(o_own, l_own, o_in, l_in, out_ref, rows, ready, done):
    blocks = o_own.shape[0] // rows
    for i in range(0, blocks, 2):
        ready(i // 2)
        for n in (i, i + 1):
            own = (columns(l_own[n], o_own.shape[1]), 1.0, o_own[block_of(n, rows), :])
            level, total, summed = joined(own, o_in, l_in, n, rows)
            out_ref[block_of(n, rows), :] = (summed / total).astype(BF16)
        for n in (i, i + 1):
            done(n)


def flat(c, per):
    return c[0] * per + c[1]


def span(c, per):
    return pl.ds(pl.multiple_of(flat(c, per) * CHUNK, CHUNK), CHUNK)


def chunk_ids(g, per, ways=WAYS):
    slabs = ways // per
    return [(g * slabs + w // per, w % per) for w in range(ways)]


def column_form(row):
    return jnp.transpose(jnp.broadcast_to(row, (CHUNK, CHUNK)))


def rates_of(rates_ref, c):
    slab, place = c
    per = rates_ref.shape[1] // 4
    return rates_ref[slab, place : place + 1, :], rates_ref[slab, per + place : per + place + 1, :]


def tail_keys(turned_ref, rates_ref, c, per):
    cum, gate = rates_of(rates_ref, c)
    weight = jnp.exp(cum[:, CHUNK - 1 :] - cum) * gate
    return (turned_ref[flat(c, per)].astype(F32) * weight).astype(BF16), jnp.exp(cum[:, CHUNK - 1 :])


def mix_of(rates_ref, c):
    cum, gate = rates_of(rates_ref, c)
    col = column_form(cum)
    shape = (CHUNK, CHUNK)
    causal = lax.broadcasted_iota(jnp.int32, shape, 0) >= lax.broadcasted_iota(
        jnp.int32, shape, 1
    )
    mix = jnp.exp(jnp.where(causal, col - cum, masked_score)) * gate
    return mix, jnp.exp(col)


def turn_keys(k_ref, turned_ref):
    def one(c, carry):
        rows = pl.ds(pl.multiple_of(c * CHUNK, CHUNK), CHUNK)
        turned_ref[c] = jnp.transpose(k_ref[rows, :])
        return carry

    lax.fori_loop(0, turned_ref.shape[0], one, 0, unroll=4)


def state_totals(turned_ref, other_ref, rates_ref, zero_ref):
    per = rates_ref.shape[1] // 4
    chunks = rates_ref.shape[0] * per

    def step(g, carry):
        state, decay = carry
        for c in chunk_ids(g, per):
            zero_ref[flat(c, per)] = state
            keys, end = tail_keys(turned_ref, rates_ref, c, per)
            state = end * state + dot(keys, other_ref[span(c, per), :])
            decay = decay * end
        return state, decay

    state, decay = lax.fori_loop(
        0, chunks // WAYS, step, (jnp.zeros((CHUNK, CHUNK), F32), jnp.ones((1, 1), F32))
    )
    zero_ref[chunks] = state
    return decay


def state_starts(rates_ref, zero_ref, first_ref, starts_ref):
    per = rates_ref.shape[1] // 4
    chunks = rates_ref.shape[0] * per

    def step(g, first):
        for c in chunk_ids(g, per):
            starts_ref[flat(c, per)] = (zero_ref[flat(c, per)] + first).astype(BF16)
            cum, gate = rates_of(rates_ref, c)
            first = first * jnp.exp(cum[:, CHUNK - 1 :])
        return first

    lax.fori_loop(0, chunks // WAYS, step, first_ref[...].astype(F32))


def solve_all(q_ref, k_ref, turned_ref, rates_ref, ridge_ref, gram_ref, x_ref):
    per = rates_ref.shape[1] // 4
    chunks = rates_ref.shape[0] * per
    ways = math.gcd(chunks, 8)
    ridge = column_form(ridge_ref)
    later = lax.broadcasted_iota(jnp.int32, (CHUNK, CHUNK), 1) >= lax.broadcasted_iota(
        jnp.int32, (CHUNK, CHUNK), 0
    )

    def group(g, carry):
        ids = chunk_ids(g, per, ways)
        mixes, starts, keys, sides, state = [], [], [], [], []
        for c in ids:
            cum, gate = rates_of(rates_ref, c)
            gap = jnp.where(later, cum - column_form(cum), masked_score)
            mixes.append(jnp.exp(gap) * column_form(gate))
            starts.append(jnp.exp(cum))
            keys.append(k_ref[span(c, per), :])
            sides.append(
                jnp.concatenate([gram_ref[flat(c, per)], turned_ref[flat(c, per)]], axis=1)
            )
            q = jnp.transpose(q_ref[span(c, per), :]).astype(F32)
            state.append((jnp.zeros_like(q), q, q, jnp.sum(q * q, axis=0, keepdims=True)))
        for sweep_index in range(CG_ITERS):
            directions = [s[2].astype(BF16) for s in state]
            products = [dot(k, p) for k, p in zip(keys, directions)]
            images = [
                dot(
                    side,
                    jnp.concatenate(
                        [(start * p.astype(F32)).astype(BF16), (mix * b).astype(BF16)], axis=0
                    ),
                )
                for side, start, mix, p, b in zip(sides, starts, mixes, directions, products)
            ]
            for w, a in enumerate(images):
                x, r, _, rr = state[w]
                p = directions[w].astype(F32)
                a = a + ridge * p
                alpha = rr / (jnp.sum(p * a, axis=0, keepdims=True) + 1e-6)
                x = x + alpha * p
                r = r - alpha * a
                new = jnp.sum(r * r, axis=0, keepdims=True)
                state[w] = (x, r, r + (new / (rr + 1e-6)) * p, new)
        for c, s in zip(ids, state):
            x_ref[span(c, per), :] = jnp.transpose(s[0].astype(BF16))
        return carry

    lax.fori_loop(0, chunks // ways, group, 0)


def read_out(k_ref, v_ref, rates_ref, cross_ref, x_ref, out_ref, slab):
    per = rates_ref.shape[1] // 4
    for c in chunk_ids(slab, per, per):
        mix, start = mix_of(rates_ref, c)
        x = x_ref[span(c, per), :]
        products = dot(x, k_ref[span(c, per), :], NT)
        rows = start * dot(x, cross_ref[flat(c, per)])
        rows = rows + dot((mix * products).astype(BF16), v_ref[span(c, per), :])
        out_ref[span(c, per), :] = rows.astype(BF16)


REACH = 2
Q, K, V, MK, MQ, RATES, ATT, OUT, GRAM, CROSS = range(10)
QX, PART, LEVEL = (10, 12, 14)
KINDS = 16
BY_HEAD = (K, V, MK, MQ, GRAM, CROSS, QX + 1)


def push_order(heads):
    order = [(Q, 0), (MK, 0), (MQ, 0), (K, 0), (V, 0), (Q, 1)]
    for j in range(1, heads):
        order += [(MK, j), (MQ, j)]
        order += [(Q, 2)] if j == 1 and heads > 2 else []
        order += [(K, j), (V, j)]
        order += [(Q, j + 2)] if j + 2 < heads else []
    return order


def plane_kernel(n, g, *refs):
    ins, rates_in, ridge_in = refs[:5], refs[5], refs[6]
    results = refs[7:9]
    bufs, rates, homes = refs[9:14], refs[14], refs[15:17]
    later = (refs[9],) + refs[17:19]
    o_out, o_in = (None,) + refs[19:21], (None,) + refs[21:23]
    l_out, l_in = (None,) + refs[23:25], (None,) + refs[25:27]
    first_out, first_in = {GRAM: refs[27], CROSS: refs[28]}, {GRAM: refs[29], CROSS: refs[30]}
    decays, zero = refs[31:33]
    gram, cross, turned, x = refs[33:37]
    o_own, l_own = refs[37:39]
    send, by_block, by_head, by_pair, at_end, own, own_end = refs[39:46]
    q, k, v, mk, mq = bufs
    att, out = homes
    rows, size = ins[0].shape[0], ridge_in.shape[1]
    per_device = rates.shape[0]
    planes = n // g
    group, me = lax.axis_index("groups"), lax.axis_index("seq")
    plane, place = me // g, lax.rem(me, g)

    def head_col(ref, j):
        return ref.at[:, pl.ds(pl.multiple_of(j * size, size), size)]

    def cell(ref, s, j):
        return ref.at[
            pl.ds(pl.multiple_of(s * rows, rows), rows),
            pl.ds(pl.multiple_of(j * size, size), size),
        ]

    def ends(a, j, source, target):
        if a in (Q, K, V, MK, MQ):
            return head_col(ins[a], target * per_device + j), cell(bufs[a], source, j)
        if a == RATES:
            return rates_in.at[pl.ds(target * per_device, per_device)], rates.at[:, source]
        return cell(homes[a - ATT], target, j), head_col(results[a - ATT], source * per_device + j)

    def arrival(a, j, i):
        if a in (Q, QX):
            return by_block.at[(Q, QX).index(a), j, i]
        if a in BY_HEAD:
            return by_head.at[BY_HEAD.index(a), j]
        if a >= PART:
            return by_pair.at[a - PART, j, i // 2]
        return at_end.at[a - RATES]

    def copy_to(src, dst, a, j, i, peer):
        return pltpu.make_async_remote_copy(
            src_ref=src,
            dst_ref=dst,
            send_sem=send.at[a],
            recv_sem=arrival(a, j, i),
            device_id=(group, peer),
            device_id_type=pl.DeviceIdType.MESH,
        )

    def bytes_of(ref, a, j=0, i=0):
        return copy_to(ref, ref, a, j, i, me)

    def home(e):
        return plane * g + e

    def remote(a, j, source, target, peer):
        src, dst = ends(a, j, source, target)
        return copy_to(src, dst, a, j, source, home(peer))

    def local(a, j):
        src, dst = ends(a, j, place, place)
        sem = own_end.at[a - RATES] if a in (RATES, ATT, OUT) else own.at[a, j]
        return pltpu.make_async_copy(src, dst, sem)

    def back(d, j, e):
        return copy_to(
            cell(later[d - 1], e, j), cell(later[d], e, j), QX + d - 1, j, e, me - g
        )

    def onward(a, d, j, i):
        if a == PART:
            src, dst = cell(o_out[d], i, j), cell(o_in[d], i, j)
        else:
            src, dst = l_out[d].at[j, i], l_in[d].at[j, i]
        return copy_to(src, dst, a + d - 1, j, i, me + g)

    def pass_on(d, j, i):
        onward(PART, d, j, i).start()
        onward(LEVEL, d, j, i).start()

    def take(d, j, t):
        @pl.when(has_previous)
        def _():
            both = pl.ds(pl.multiple_of(2 * t * rows, rows), 2 * rows)
            sums = head_col(o_in[d], j).at[both, :]
            bytes_of(sums, PART + d - 1, j, 2 * t).wait_recv()
            bytes_of(l_in[d].at[j, pl.ds(2 * t, 2)], LEVEL + d - 1, j, 2 * t).wait_recv()

    def state(a, j):
        return copy_to(first_out[a].at[j], first_in[a].at[j], a, j, 0, me + g)

    def loop(first, last, act):
        def one(t, carry):
            act(t)
            return carry

        lax.fori_loop(first, last, one, 0)

    def others(act):
        loop(1, g, lambda t: act(lax.rem(place + t, g)))

    def signal(peer):
        pl.semaphore_signal(
            barrier, inc=1, device_id=(group, peer), device_id_type=pl.DeviceIdType.MESH
        )

    def push(a, j):
        others(lambda e: remote(a, j, place, e, e).start())
        local(a, j).start()

    def arrive(a, j):
        if a == RATES:
            bytes_of(rates.at[:, : g - 1], a).wait_recv()
        else:
            bytes_of(head_col(bufs[a], j).at[: (g - 1) * rows, :], a, j).wait_recv()
        local(a, j).wait()

    def give(a, j, e):
        @pl.when(e != place)
        def _():
            remote(a, j, place, e, e).start()

        @pl.when(e == place)
        def _():
            local(a, j).start()

    def reaches(d):
        return plane + d < planes

    has_previous = plane > 0

    barrier = pltpu.get_barrier_semaphore()
    others(lambda e: signal(home(e)))

    @pl.when(has_previous)
    def _():
        signal(me - g)

    @pl.when(reaches(1))
    def _():
        signal(me + g)

    neighbours = has_previous.astype(jnp.int32) + reaches(1).astype(jnp.int32)
    pl.semaphore_wait(barrier, g - 1 + neighbours)

    push(RATES, 0)
    for a, j in push_order(per_device):
        push(a, j)

    @pl.when(jnp.logical_not(has_previous))
    def _():
        for d in range(1, REACH + 1):
            o_in[d][...] = jnp.zeros_like(o_in[d])
            l_in[d][...] = jnp.full_like(l_in[d], masked_score)
        for a in (GRAM, CROSS):
            first_in[a][...] = jnp.zeros_like(first_in[a])

    def near_first(act):
        loop(0, g, lambda t: act(place ^ t))

    def forward(j):
        def one(e):
            @pl.when(e == place)
            def _():
                local(Q, j).wait()

            @pl.when(e != place)
            def _():
                remote(Q, j, e, place, e).wait_recv()

            @pl.when(has_previous)
            def _():
                back(1, j, e).start()

        near_first(one)

    def relay(j):
        @pl.when(reaches(1))
        def _():
            def one(e):
                back(1, j, e).wait_recv()

                @pl.when(has_previous)
                def _():
                    back(2, j, e).start()

            near_first(one)

    arrive(RATES, 0)

    def head_totals(a, j, others_ref):
        return state_totals(
            turned.at[j], head_col(others_ref, j), rates.at[j], zero.at[a - GRAM, j]
        )

    def hand_on(a, j):
        @pl.when(has_previous)
        def _():
            state(a, j).wait_recv()

        @pl.when(reaches(1))
        def _():
            first = first_in[a][j].astype(F32)
            following = decays[pl.ds(j, 1), :] * first + zero[a - GRAM, j, zero.shape[2] - 1]
            first_out[a][j] = following.astype(BF16)
            state(a, j).start()

    def head_starts(a, j, starts_ref):
        state_starts(rates.at[j], zero.at[a - GRAM, j], first_in[a].at[j], starts_ref.at[j])

    def total_head(j):
        arrive(MK, j)
        turn_keys(head_col(mk, j), turned.at[j])
        decay = head_totals(GRAM, j, mk)
        decays[pl.ds(j, 1), :] = jnp.broadcast_to(decay, (1, size))

        @pl.when(jnp.logical_not(has_previous))
        def _():
            hand_on(GRAM, j)

    def far_head(j):
        bytes_of(head_col(later[2], j), QX + 1, j).wait_recv()
        attend_far(
            head_col(later[2], j), head_col(k, j), head_col(v, j),
            head_col(o_out[2], j), l_out[2].at[j], rows, lambda i: pass_on(2, j, i),
        )

    def merge_head(j):
        attend_last(
            head_col(o_own, j), l_own.at[j], head_col(o_in[1], j), l_in[1].at[j],
            head_col(att, j), rows, lambda i: take(1, j, i), lambda i: give(ATT, j, i),
        )
        head_totals(CROSS, j, att)

        @pl.when(jnp.logical_not(has_previous))
        def _():
            hand_on(CROSS, j)

    def step(s):
        first, middle, near, last = s, s - 1, s - 2, s - 3

        @pl.when(s == 0)
        def _():
            total_head(0)
            forward(0)

        @pl.when(first < per_device)
        def _():
            j = first

            @pl.when(has_previous)
            def _():
                hand_on(GRAM, j)

            head_starts(GRAM, j, gram)
            arrive(MQ, j)
            solve_all(
                head_col(mq, j), head_col(mk, j), turned.at[j], rates.at[j],
                ridge_in[pl.ds(place * per_device + j, 1), :], gram.at[j], head_col(x, j),
            )

        @pl.when((last >= 0) & (plane == 1))
        def _():
            hand_on(CROSS, last)

        @pl.when((s < 2) & (s + 1 < per_device))
        def _():
            forward(s + 1)

        @pl.when((s == 1) & (s < per_device))
        def _():
            relay(1)

        @pl.when((middle >= 0) & (middle < per_device - 1) & reaches(2))
        def _():
            far_head(middle)

        @pl.when(first < per_device)
        def _():
            j = first
            arrive(K, j)
            arrive(V, j)
            attend_own(
                head_col(q, j), head_col(k, j), head_col(v, j), head_col(o_own, j), l_own.at[j],
                rows,
            )

        @pl.when(s == 0)
        def _():
            relay(0)

        @pl.when((s > 0) & (s + 2 < per_device))
        def _():
            forward(s + 2)

        @pl.when((s > 0) & (s + 1 < per_device))
        def _():
            relay(s + 1)

        @pl.when(s + 1 < per_device)
        def _():
            total_head(s + 1)

        @pl.when((first == per_device - 1) & reaches(2))
        def _():
            far_head(first)

        @pl.when((near >= 0) & (near < per_device) & (plane == 0))
        def _():
            merge_head(near)

        @pl.when((middle >= 0) & (middle < per_device) & reaches(1))
        def _():
            j = middle
            attend_middle(
                head_col(later[1], j), head_col(k, j), head_col(v, j),
                head_col(o_in[2], j), l_in[2].at[j],
                head_col(o_out[1], j), l_out[1].at[j], rows,
                lambda i: take(2, j, i), lambda i: pass_on(1, j, i),
            )

        @pl.when((near >= 0) & (near < per_device) & has_previous)
        def _():
            merge_head(near)

        @pl.when(last >= 0)
        def _():
            j = last

            @pl.when(plane > 1)
            def _():
                hand_on(CROSS, j)

            head_starts(CROSS, j, cross)

            def slab_out(i):
                read_out(
                    head_col(mk, j), head_col(att, j), rates.at[j], cross.at[j], head_col(x, j),
                    head_col(out, j), i,
                )
                give(OUT, j, i)

            loop(0, g, slab_out)

    loop(0, per_device + 3, step)

    def finish():
        for a in (ATT, OUT):
            result = results[a - ATT]
            bytes_of(result.at[:, : (g - 1) * per_device * size], a).wait_recv()
            part = result.at[:, : per_device * size]
            pltpu.make_async_copy(part, part, own_end.at[a - RATES]).wait()
            bytes_of(homes[a - ATT].at[: (g - 1) * rows, :], a).wait_send()
        for a in (Q, K, V, MK, MQ):
            bytes_of(bufs[a].at[: (g - 1) * rows, :], a).wait_send()
        bytes_of(rates.at[:, : g - 1], RATES).wait_send()

        @pl.when(has_previous)
        def _():
            bytes_of(later[0], QX).wait_send()

            @pl.when(reaches(1))
            def _():
                bytes_of(later[1], QX + 1).wait_send()

        for d in range(1, REACH + 1):

            @pl.when(reaches(d))
            def _(d=d):
                bytes_of(o_out[d], PART + d - 1).wait_send()
                bytes_of(l_out[d], LEVEL + d - 1).wait_send()

        @pl.when(reaches(1))
        def _():
            for a in (GRAM, CROSS):
                bytes_of(first_out[a], a).wait_send()

    finish()


def plane_body(
    attn_query, attn_key, attn_value, mesa_query, mesa_key, log_decay, input_gate, regularizer
):
    rows = attn_query.shape[0]
    heads, size = regularizer.shape
    devices = lax.axis_size("seq")
    g = WINDOW // (REACH * rows)
    per_device, tokens = heads // g, g * rows
    per, chunks = rows // CHUNK, tokens // CHUNK
    cum = jnp.cumsum(log_decay.reshape(per, CHUNK, heads), axis=1)
    rates = jnp.concatenate([cum, input_gate.reshape(per, CHUNK, heads)] * 2, axis=0)
    rates = jnp.transpose(rates, (2, 0, 1))
    slab = jax.ShapeDtypeStruct((rows, heads * size), BF16)
    vmem = pl.BlockSpec(memory_space=pltpu.VMEM)
    anywhere = pl.BlockSpec(memory_space=pl.ANY)
    tall = pltpu.VMEM((tokens, per_device * size), BF16)
    levels = pltpu.VMEM((per_device, g, 1, rows), F32)
    first = pltpu.VMEM((per_device, size, size), BF16)
    states = pltpu.VMEM((per_device, chunks, size, size), BF16)
    return pl.pallas_call(
        functools.partial(plane_kernel, devices, g),
        out_shape=(slab, slab),
        in_specs=[anywhere] * 5 + [vmem] * 2,
        out_specs=(anywhere, anywhere),
        scratch_shapes=[tall] * 5
        + [pltpu.VMEM((per_device, g, 4 * per, CHUNK), F32)]
        + [tall] * (2 + REACH + 2 * REACH)
        + [levels] * (2 * REACH)
        + [first] * 4
        + [
            pltpu.VMEM((8, size), F32),
            pltpu.VMEM((2, per_device, chunks + 1, size, size), F32),
        ]
        + [states] * 3
        + [
            tall,
            pltpu.VMEM((tokens, per_device * size), F32),
            levels,
            pltpu.SemaphoreType.DMA((KINDS,)),
            pltpu.SemaphoreType.DMA((2, per_device, g)),
            pltpu.SemaphoreType.DMA((len(BY_HEAD), per_device)),
            pltpu.SemaphoreType.DMA((2 * REACH, per_device, g // 2)),
            pltpu.SemaphoreType.DMA((3,)),
            pltpu.SemaphoreType.DMA((5, per_device)),
            pltpu.SemaphoreType.DMA((3,)),
        ],
        compiler_params=pltpu.CompilerParams(
            collective_id=0, has_side_effects=True, vmem_limit_bytes=56 * 1024 * 1024
        ),
    )(attn_query, attn_key, attn_value, mesa_key, mesa_query, rates, regularizer)


def fits_planes(mesh, rows, heads, size):
    if WINDOW % (REACH * rows):
        return False
    g = WINDOW // (REACH * rows)
    return (
        size == CHUNK
        and g & (g - 1) == 0
        and mesh.shape["seq"] % g == 0
        and heads % g == 0
        and 2 <= heads // g <= 8
        and g % 2 == 0
        and rows % CHUNK == 0
        and WAYS % (rows // CHUNK) == 0
        and g * rows % (CHUNK * WAYS) == 0
    )


def solution(mesh):
    spec = P(("groups", "seq"), None)

    def body(*args):
        heads, size = args[7].shape
        fits = fits_planes(mesh, args[0].shape[0], heads, size)
        return (plane_body if fits else slab_body)(*args)

    return jax.shard_map(
        body,
        mesh=mesh,
        in_specs=(spec,) * 7 + (P(),),
        out_specs=(spec, spec),
        check_vma=False,
    )
```
